32 devices in a mesh: dp: 4 (over y, core), tensor: 8 (over z, x).
Axes of the slice: x: 2, y: 2, z: 4, core: 2. Of those that a mesh axis runs over, the one named last changes fastest.
Arguments:
- blocks: bfloat16 [8192, 768], P(('dp', 'tensor')), may hold values from -6 to 6
- counts: int32 [8, 2], P('dp'), may hold values from 1 to 896, as said below
- cotangent: bfloat16 [8192, 768], P(('dp', 'tensor')), may hold values from -6 to 6
- w_query: bfloat16 [768, 768], replicated, may hold values from -0.21875 to 0.21875
- w_key: bfloat16 [768, 768], replicated, may hold values from -0.21875 to 0.21875
- w_value: bfloat16 [768, 768], replicated, may hold values from -0.21875 to 0.21875
- w_out: bfloat16 [768, 768], replicated, may hold values from -3.5 to 3.5
- b_query: bfloat16 [768], replicated, may hold values from -3 to 3
- b_value: bfloat16 [768], replicated, may hold values from -0.29882812 to 0.29882812
- b_out: bfloat16 [768], replicated, may hold values from -3 to 3
- norm1_gain: bfloat16 [768], replicated, may hold values from 0.5 to 1.5
- norm1_bias: bfloat16 [768], replicated, may hold values from -0.29882812 to 0.29882812
- norm2_gain: bfloat16 [768], replicated, may hold values from 0.5 to 1.5
- norm2_bias: bfloat16 [768], replicated, may hold values from -3 to 3
- gate_logits: bfloat16 [2, 768], replicated, may hold values from -6 to 6
- w_up: bfloat16 [768, 3072], P(None, 'tensor'), may hold values from -0.21875 to 0.21875
- b_up: bfloat16 [3072], P('tensor'), may hold values from -3 to 3
- w_down: bfloat16 [3072, 768], P('tensor'), may hold values from -0.109375 to 0.109375
- b_down: bfloat16 [768], replicated, may hold values from -3 to 3
Outputs:
- joined: bfloat16 [8192, 768], P(('dp', 'tensor'))
- grad_blocks: float32 [8192, 768], P(('dp', 'tensor'))
- grad_w_query: float32 [768, 768], replicated
- grad_w_key: float32 [768, 768], replicated
- grad_w_value: float32 [768, 768], replicated
- grad_w_out: float32 [768, 768], replicated
- grad_b_query: float32 [768], replicated
- grad_b_value: float32 [768], replicated
- grad_b_out: float32 [768], replicated
- grad_norm1_gain: float32 [768], replicated
- grad_norm1_bias: float32 [768], replicated
- grad_norm2_gain: float32 [768], replicated
- grad_norm2_bias: float32 [768], replicated
- grad_gate_logits: float32 [2, 768], replicated
- grad_w_up: float32 [768, 3072], P(None, 'tensor')
- grad_b_up: float32 [3072], P('tensor')
- grad_w_down: float32 [3072, 768], P('tensor')
- grad_b_down: float32 [768], replicated
The draws below stay inside these ranges and needn't reach their ends.
Inputs may be any that keep to these rules, and one draw needn't show every extreme that they name: counts[d, 0] is the number of text blocks of document d, 448 or more, counts[d, 1] its visual blocks, 1 or more; some document has all 896 text and all 128 visual slots filled.
All inputs are finite; a program needn't handle non-finite values.
Results may differ from the reference program's by a relative error of at most 0.013.
Values may be sent and summed in bfloat16 or wider, within the bound.
A program may use at most 192 MiB of HBM per device.

```python
import jax
import jax.numpy as jnp
from jax import lax

D = 768
HEADS = 12
HEAD_DIM = 64
FF = 3072
TEXT_SLOTS = 896
VISUAL_SLOTS = 128
SEQ = 1024
DOCS = 8
ROWS = 8192


def draw_blocks(key, part):
    result = jax.random.truncated_normal(key, -6.0, 6.0, (ROWS, D), jnp.float32)
    return result.astype(jnp.bfloat16)


def draw_counts(key, part):
    text_key, image_key, extra_key = jax.random.split(key, 3)
    text_count = jax.random.randint(text_key, (DOCS,), TEXT_SLOTS // 2, TEXT_SLOTS + 1)
    image_first = jax.random.randint(image_key, (DOCS,), 1, VISUAL_SLOTS + 1)
    image_second = jax.random.randint(extra_key, (DOCS,), 1, VISUAL_SLOTS + 1)
    image_count = jnp.minimum(image_first, image_second)
    text_count = text_count.at[0].set(TEXT_SLOTS)
    image_count = image_count.at[0].set(VISUAL_SLOTS)
    return jnp.stack([text_count, image_count], axis=1).astype(jnp.int32)


def shard_levels(key, extent, cuts, low, top_value):
    loudness, own = 1.0, jax.random.fold_in(key, 6)
    for dim, parts in cuts:
        draws = jnp.exp(jax.random.uniform(jax.random.fold_in(own, dim), (parts,), jnp.float32, low / len(cuts), top_value / len(cuts)))
        loudness = loudness * jnp.repeat(draws, extent[dim] // parts).reshape([-1 if axis == dim else 1 for axis in range(len(extent))])
    return loudness


def normal_values(own_key, extent, scale, bound, shards=(), held_as=jnp.bfloat16):
    values = jax.random.normal(own_key, extent, jnp.float32) * scale
    if len(shards) > 0:
        values = shard_levels(own_key, extent, shards, -0.22, 0.18) * values
    return jnp.clip(values, min=-bound, max=bound).astype(held_as)


def setup_inputs(seed: int = 0) -> dict:
    streams_of = jax.random.split(jax.random.key(seed), 20)
    return {
        "blocks": draw_blocks(jax.random.fold_in(streams_of[19], 71), 0),
        "counts": draw_counts(jax.random.fold_in(streams_of[19], 71), 0),
        "cotangent": normal_values(streams_of[2], (ROWS, D), 1.0, 6.0, ((0, 32),)),
        "w_query": normal_values(streams_of[3], (D, D), D ** -0.5, 0.21875),
        "w_key": normal_values(streams_of[4], (D, D), D ** -0.5, 0.21875),
        "w_value": normal_values(streams_of[5], (D, D), D ** -0.5, 0.21875),
        "w_out": normal_values(streams_of[6], (D, D), (max(D // 256, 2)) ** -0.5, 3.5),
        "b_query": normal_values(streams_of[7], (D,), 0.5, 3.0),
        "b_value": normal_values(streams_of[8], (D,), 0.05, 0.29882812),
        "b_out": normal_values(streams_of[9], (D,), 0.5, 3.0),
        "norm1_gain": jnp.clip(1.0 + 0.1 * jax.random.normal(streams_of[10], (D,), jnp.float32), 0.5, 1.5).astype(jnp.bfloat16),
        "norm1_bias": normal_values(streams_of[11], (D,), 0.05, 0.29882812),
        "norm2_gain": jnp.clip(1.0 + 0.1 * jax.random.normal(streams_of[12], (D,), jnp.float32), 0.5, 1.5).astype(jnp.bfloat16),
        "norm2_bias": normal_values(streams_of[13], (D,), 0.5, 3.0),
        "gate_logits": normal_values(streams_of[14], (2, D), 1.5, 6.0),
        "w_up": normal_values(streams_of[15], (D, FF), D ** -0.5, 0.21875, ((1, 8),)),
        "b_up": normal_values(streams_of[16], (FF,), 0.5, 3.0, ((0, 8),)),
        "w_down": normal_values(streams_of[17], (FF, D), FF ** -0.5, 0.109375, ((0, 8),)),
        "b_down": normal_values(streams_of[18], (D,), 0.5, 3.0),
    }


@jax.custom_vjp
def low(v):
    return lax.optimization_barrier(v.astype(jnp.bfloat16)).astype(jnp.float32)

@jax.custom_vjp
def low_back(v):
    return v

def low_keep(v):
    return (low(v), None)

def low_pass(kept, grad):
    return (grad,)

def back_keep(v):
    return (v, None)

def back_low(kept, grad):
    return (low(grad),)
low.defvjp(low_keep, low_pass)
low_back.defvjp(back_keep, back_low)
EPSILON = 1e-05

def normalize(values, gain, shift):
    centre = values - lax.optimization_barrier(jnp.mean(values, axis=-1, keepdims=True))
    spread = lax.optimization_barrier(jnp.mean(centre * centre, axis=-1, keepdims=True))
    return centre * lax.rsqrt(spread + EPSILON) * gain + shift

def matmul_high(left, right):
    return jnp.dot(left, right, precision=lax.Precision.HIGHEST)

def cross_layer(inputs, params, doc_counts):
    w_query, w_key, w_value, w_out, b_query, b_value, b_out, gain_one, shift_one, gain_two, shift_two, gate_logits, w_up, b_up, w_down, b_down = params
    position = jnp.arange(SEQ, dtype=jnp.int32)
    visual = position >= TEXT_SLOTS
    valid = jnp.where(visual, position - TEXT_SLOTS < doc_counts[1], position < doc_counts[0])
    normed = low(normalize(inputs, gain_one, shift_one))
    queries = low(low_back(matmul_high(normed, w_query) + b_query)).reshape(SEQ, HEADS, HEAD_DIM)
    keyed = low(low_back(matmul_high(normed, w_key))).reshape(SEQ, HEADS, HEAD_DIM)
    valued = low(low_back(matmul_high(normed, w_value) + b_value)).reshape(SEQ, HEADS, HEAD_DIM)
    raw = low_back(jnp.einsum('qhd,khd->hqk', queries, keyed, precision=lax.Precision.HIGHEST))
    scores = raw * HEAD_DIM ** (-0.5) + jnp.where(valid, 0.0, -1e+30)[None, None, :]
    probs = low(jax.nn.softmax(scores, axis=-1))
    mixed = jnp.einsum('hqk,khd->qhd', probs, valued, precision=lax.Precision.HIGHEST)
    attended = low(low_back(mixed.reshape(SEQ, D)))
    branch = low_back(matmul_high(attended, w_out) + b_out)
    gate = jax.nn.sigmoid(jnp.where(visual[:, None], gate_logits[1][None, :], gate_logits[0][None, :]))
    middle = inputs + gate * branch
    second = low(normalize(middle, gain_two, shift_two))
    pre = low_back(matmul_high(second, w_up) + b_up)
    hidden = low(jax.nn.gelu(pre, approximate=False))
    lowered = low_back(matmul_high(hidden, w_down))
    return middle + lowered + b_down

def reference(blocks, counts, cotangent, w_query, w_key, w_value, w_out, b_query, b_value, b_out, norm1_gain, norm1_bias, norm2_gain, norm2_bias, gate_logits, w_up, b_up, w_down, b_down):
    params = tuple((p.astype(jnp.float32) for p in (w_query, w_key, w_value, w_out, b_query, b_value, b_out, norm1_gain, norm1_bias, norm2_gain, norm2_bias, gate_logits, w_up, b_up, w_down, b_down)))
    inputs_all = blocks.astype(jnp.float32).reshape(DOCS, SEQ, D)
    cot_all = cotangent.astype(jnp.float32).reshape(DOCS, SEQ, D)

    def doc_step(totals, item):
        doc_inputs, doc_cot, doc_counts = item
        result, pull = jax.vjp(lambda vals, prm: cross_layer(vals, prm, doc_counts), doc_inputs, params)
        grad_inputs, grad_params = pull(doc_cot)
        totals = jax.tree.map(jnp.add, totals, grad_params)
        return (totals, (result.astype(jnp.bfloat16), grad_inputs))
    zeros = jax.tree.map(jnp.zeros_like, params)
    grads, (joined_all, grad_rows) = lax.scan(doc_step, zeros, (inputs_all, cot_all, counts))
    joined = joined_all.reshape(ROWS, D)
    grad_blocks = grad_rows.reshape(ROWS, D)
    return (joined, grad_blocks, grads[0], grads[1], grads[2], grads[3], grads[4], grads[5], grads[6], grads[7], grads[8], grads[9], grads[10], grads[11], grads[12], grads[13], grads[14], grads[15])
```

```python
import functools

import jax
import jax.numpy as jnp
from jax import lax
from jax.experimental import pallas as pl
from jax.experimental.pallas import tpu as pltpu
from jax.sharding import PartitionSpec as P

HEADS = 12
HEAD_DIM = 64
TEXT_SLOTS = 896
SEQ = 1024
EPSILON = 1e-05
BF = jnp.bfloat16
F32 = jnp.float32


def normalize(values, gain, shift):
    centre = values - jnp.mean(values, axis=-1, keepdims=True)
    spread = jnp.mean(centre * centre, axis=-1, keepdims=True)
    return centre * lax.rsqrt(spread + EPSILON) * gain + shift


def gelu_exact(values):
    return jax.nn.gelu(values, approximate=False)


def gelu_grad(values, upstream):
    return jax.vjp(gelu_exact, values)[1](upstream)[0]


def dot_nn(left, right):
    return lax.dot_general(left, right, (((1,), (0,)), ((), ())), preferred_element_type=F32)


def dot_tn(left, right):
    return lax.dot_general(left, right, (((0,), (0,)), ((), ())), preferred_element_type=F32)


def dot_nt(left, right):
    return lax.dot_general(left, right, (((1,), (1,)), ((), ())), preferred_element_type=F32)


def pick(array, index):
    return lax.dynamic_index_in_dim(array, index, 0, keepdims=False)


def low(value):
    return value.astype(BF)


def wide(value):
    return value.astype(F32)


def flip(value, axis, mask):
    size = lax.axis_size(axis)
    return lax.ppermute(value, axis, [(i, i ^ mask) for i in range(size)])


def bits_of(size):
    found = []
    mask = 1
    while mask < size:
        found.append(mask)
        mask *= 2
    return found


def sum_everywhere(value):
    for axis in ("dp", "tensor"):
        for mask in bits_of(lax.axis_size(axis)):
            value = value + flip(value, axis, mask)
    return value


def exchange_sum(value, stages):
    for axis, mask in stages:
        sent = low(value)
        value = wide(sent) + wide(flip(sent, axis, mask))
    return value


def head_mask(lanes, head):
    return (lanes >= head * HEAD_DIM) & (lanes < (head + 1) * HEAD_DIM)


def attention_forward_kernel(
    heads, rows, n_ref, wq_ref, wk_ref, wv_ref, b_ref, tail_ref, o_ref, q_ref, k_ref, v_ref, l_ref
):
    total_rows = n_ref.shape[0]
    wide_span = q_ref.shape[1]
    count = total_rows // rows
    scale = HEAD_DIM ** (-0.5)
    extra = heads * HEAD_DIM

    @pl.loop(0, count)
    def _(block):
        at = pl.ds(pl.multiple_of(block * rows, rows), rows)
        part = n_ref[at, :]
        q_ref[at, :] = low(low(dot_nn(part, wq_ref[...]) + b_ref[0:1, :]) * scale)
        k_ref[at, :] = low(dot_nn(part, wk_ref[...]) + tail_ref[at, :])
        v_ref[at, :] = low(dot_nn(part, wv_ref[...]) + b_ref[1:2, :])

    lanes = lax.broadcasted_iota(jnp.int32, (rows, wide_span), 1)
    unit = low(jnp.where(lanes == extra, 1.0, 0.0))
    side = lax.broadcasted_iota(jnp.int32, (rows, 128), 1)

    @pl.loop(0, count)
    def _(block):
        at = pl.ds(pl.multiple_of(block * rows, rows), rows)
        query = q_ref[at, :]
        mixed = jnp.zeros((rows, wide_span), F32)
        logs = jnp.zeros((rows, 128), F32)
        for head in range(heads):
            chosen = head_mask(lanes, head)
            left = jnp.where(chosen, query, unit)
            scores = dot_nt(left, k_ref[...])
            peak = jnp.max(scores, axis=-1, keepdims=True)
            expo = jnp.exp(scores - peak)
            total = jnp.sum(expo, axis=-1, keepdims=True)
            out = dot_nn(low(expo), v_ref[...]) / total
            mixed = jnp.where(chosen, out, mixed)
            logs = jnp.where(side == head, peak + jnp.log(total), logs)
        o_ref[at, :] = low(mixed)
        l_ref[at, :] = logs


def attention_backward_kernel(
    heads, rows, q_ref, k_ref, v_ref, l_ref, g_ref, dq_ref, dk_ref, dv_ref, sum_k, sum_v
):
    total_rows, wide_span = q_ref.shape
    count = total_rows // rows
    scale = HEAD_DIM ** (-0.5)
    extra = heads * HEAD_DIM
    lanes = lax.broadcasted_iota(jnp.int32, (rows, wide_span), 1)
    sum_k[...] = jnp.zeros_like(sum_k)
    sum_v[...] = jnp.zeros_like(sum_v)

    @pl.loop(0, count)
    def _(block):
        at = pl.ds(pl.multiple_of(block * rows, rows), rows)
        query = q_ref[at, :]
        grad = g_ref[at, :]
        grad_q = jnp.zeros((rows, wide_span), F32)
        for head in range(heads):
            chosen = head_mask(lanes, head)
            log_total = l_ref[at, head : head + 1]
            high = low(log_total)
            rest = log_total - wide(high)
            middle = low(rest)
            last = low(rest - wide(middle))
            fill = jnp.where(lanes == extra, 1.0, 0.0)
            fill = jnp.where(lanes == extra + 1, -wide(high), fill)
            fill = jnp.where(lanes == extra + 2, -wide(middle), fill)
            fill = jnp.where(lanes == extra + 3, -wide(last), fill)
            left = jnp.where(chosen, query, low(fill))
            upstream = jnp.where(chosen, grad, jnp.zeros_like(grad))
            probs = jnp.exp(dot_nt(k_ref[...], left))
            grad_probs = dot_nt(v_ref[...], upstream)
            centred = jnp.sum(probs * grad_probs, axis=0, keepdims=True)
            grad_scores = low(probs * (grad_probs - centred))
            sum_k[...] += dot_nn(grad_scores, left)
            sum_v[...] += dot_nn(low(probs), upstream)
            out = dot_tn(grad_scores, k_ref[...]) * scale
            grad_q = jnp.where(chosen, out, grad_q)
        dq_ref[at, :] = low(grad_q)

    keep = lax.broadcasted_iota(jnp.int32, (total_rows, wide_span), 1) < extra
    dk_ref[...] = low(jnp.where(keep, sum_k[...], 0.0))
    dv_ref[...] = low(sum_v[...])


def attention_forward(heads, rows, normed_all, w_q, w_k, w_v, bias, tail):
    total_rows = normed_all.shape[0]
    wide_span = w_q.shape[1]
    square = jax.ShapeDtypeStruct((total_rows, wide_span), BF)
    return pl.pallas_call(
        functools.partial(attention_forward_kernel, heads, rows),
        out_shape=(square, square, square, square, jax.ShapeDtypeStruct((total_rows, 128), F32)),
        compiler_params=pltpu.CompilerParams(vmem_limit_bytes=48 << 20),
        cost_estimate=pl.CostEstimate(
            flops=20_000_000_000, bytes_accessed=6_000_000, transcendentals=3_000_000
        ),
    )(normed_all, w_q, w_k, w_v, bias, tail)


def attention_backward(heads, rows, queries, keys, values, logs, grad_mixed):
    total_rows, wide_span = queries.shape
    square = jax.ShapeDtypeStruct((total_rows, wide_span), BF)
    return pl.pallas_call(
        functools.partial(attention_backward_kernel, heads, rows),
        out_shape=(square, square, square),
        scratch_shapes=[
            pltpu.VMEM((total_rows, wide_span), F32),
            pltpu.VMEM((total_rows, wide_span), F32),
        ],
        compiler_params=pltpu.CompilerParams(vmem_limit_bytes=48 << 20),
        cost_estimate=pl.CostEstimate(
            flops=30_000_000_000, bytes_accessed=6_000_000, transcendentals=3_000_000
        ),
    )(queries, keys, values, logs, grad_mixed)


def local(
    blocks,
    counts,
    cotangent,
    w_query,
    w_key,
    w_value,
    w_out,
    b_query,
    b_value,
    b_out,
    norm1_gain,
    norm1_bias,
    norm2_gain,
    norm2_bias,
    gate_logits,
    w_up,
    b_up,
    w_down,
    b_down,
):
    rows, width = blocks.shape
    tensor_size = lax.axis_size("tensor")
    dp_size = lax.axis_size("dp")
    t_pos = lax.axis_index("tensor")
    d_pos = lax.axis_index("dp")
    members = SEQ // rows
    member = t_pos % members
    per_head = -(-HEADS // members)
    span = per_head * HEAD_DIM
    ring = 4
    line = tensor_size // ring
    z_pos = t_pos // line
    x_pos = t_pos % line
    core = d_pos % 2
    side = (d_pos // 2) % 2
    shard = w_up.shape[1]
    quarter = shard // 4
    hidden_total = shard * tensor_size
    dp_rest = [("dp", mask) for mask in bits_of(dp_size)[2:]]
    member_masks = bits_of(members)
    tensor_rest = [("tensor", mask) for mask in bits_of(tensor_size)[len(member_masks):]]

    def z_shift(value, step):
        pairs = [
            (i, ((i // line + step) % ring) * line + i % line) for i in range(tensor_size)
        ]
        return lax.ppermute(value, "tensor", pairs)

    def x_shift(value, step):
        pairs = [
            (i, (i // line) * line + (i % line + step) % line) for i in range(tensor_size)
        ]
        return lax.ppermute(value, "tensor", pairs)

    gain_one = wide(norm1_gain)
    shift_one = wide(norm1_bias)
    gain_two = wide(norm2_gain)
    shift_two = wide(norm2_bias)
    logits_gate = wide(gate_logits)
    inputs = wide(blocks)

    normed = low(normalize(inputs, gain_one, shift_one))
    row_slots = [normed] + [flip(normed, "tensor", j) for j in range(1, members)]
    cot_all = jnp.concatenate([cotangent, flip(cotangent, "dp", 1)], 0)

    doc_counts = pick(counts, t_pos // members)
    slot_ids = member ^ jnp.arange(members, dtype=jnp.int32)
    slot_pos = (slot_ids[:, None] * rows + jnp.arange(rows, dtype=jnp.int32)[None, :]).reshape(SEQ)
    valid = jnp.where(
        slot_pos >= TEXT_SLOTS, slot_pos - TEXT_SLOTS < doc_counts[1], slot_pos < doc_counts[0]
    )
    key_mask = jnp.where(valid, 0.0, -1e30).astype(F32)
    own_pos = member * rows + jnp.arange(rows, dtype=jnp.int32)
    visual = own_pos >= TEXT_SLOTS

    begin = core * (2 * quarter) + side * quarter
    up_part = lax.dynamic_slice_in_dim(w_up.T, begin, quarter, 0)
    down_part = lax.dynamic_slice_in_dim(w_down, begin, quarter, 0)
    piece = jnp.concatenate([up_part, down_part], 0)
    pieces = [piece]
    for _ in range(ring - 1):
        pieces.append(z_shift(pieces[-1], 1))
    ups, downs = [], []
    for held in pieces:
        for step in range(line):
            moved = held if step == 0 else x_shift(held, step)
            for got in (moved, flip(moved, "dp", 2)):
                ups.append(got[:quarter])
                downs.append(got[quarter:])
    up_t = jnp.concatenate(ups, 0)
    down = jnp.concatenate(downs, 0)
    biases = b_up[None, :]
    for mask in bits_of(tensor_size):
        biases = jnp.concatenate([biases, flip(biases, "tensor", mask)], 0)
    slot_z = (z_pos - jnp.arange(ring, dtype=jnp.int32)) % ring
    slot_x = (x_pos - jnp.arange(line, dtype=jnp.int32)) % line
    slot_t = (slot_z[:, None] * line + slot_x[None, :]).reshape(-1)
    biases = wide(biases).reshape(tensor_size, 2, 2, quarter)
    biases = jnp.take(biases, slot_t ^ t_pos, axis=0)
    biases = lax.dynamic_index_in_dim(biases, core, 1, keepdims=False)
    biases = jnp.where(side == 0, biases, biases[:, ::-1]).reshape(-1)

    def head_part(weight):
        extra = per_head * HEAD_DIM * members - width
        if extra:
            weight = jnp.pad(weight, ((0, 0),) * (weight.ndim - 1) + ((0, extra),))
        return lax.dynamic_slice_in_dim(weight, member * span, span, weight.ndim - 1)

    wide_span = -(-(span + 4) // 128) * 128

    def widen(array):
        return jnp.pad(array, ((0, 0),) * (array.ndim - 1) + ((0, wide_span - array.shape[-1]),))

    w_q = widen(head_part(w_query))
    w_k = widen(head_part(w_key))
    w_v = widen(head_part(w_value))
    bias = wide(jnp.stack([widen(head_part(b_query)), widen(head_part(b_value))], 0))
    lane = jnp.arange(wide_span, dtype=jnp.int32)[None, :]
    tail = jnp.where(lane == span, key_mask[:, None], 0.0)
    tail = jnp.where((lane > span) & (lane < span + 4), 1.0, tail)
    normed_all = jnp.concatenate(row_slots, 0)
    mixed, queries, keys, values, logs = attention_forward(
        per_head, rows, normed_all, w_q, w_k, w_v, bias, tail
    )
    mixed = mixed[:, :span].reshape(members, rows, span)
    mixed_slots = [mixed[0]] + [flip(mixed[j], "tensor", j) for j in range(1, members)]
    attended = jnp.take(jnp.stack(mixed_slots, 0), slot_ids, axis=0)
    attended = attended.transpose(1, 0, 2).reshape(rows, members * span)[:, :width]

    branch = dot_nn(attended, w_out) + wide(b_out)
    gate = jax.nn.sigmoid(
        jnp.where(visual[:, None], logits_gate[1][None, :], logits_gate[0][None, :])
    )
    middle = inputs + gate * branch
    second = low(normalize(middle, gain_two, shift_two))
    second_all = jnp.concatenate([second, flip(second, "dp", 1)], 0)

    pre = dot_nt(second_all, up_t) + biases
    hidden = low(gelu_exact(pre))
    grad_down = dot_tn(hidden, cot_all)
    spread = dot_nt(cot_all, down)
    dpre = low(gelu_grad(pre, spread))
    second_part = dot_nn(dpre, up_t)
    grad_second = second_part[:rows] + flip(second_part[rows:], "dp", 1)
    lowered_part = dot_nn(hidden, down)
    lowered = lowered_part[:rows] + flip(lowered_part[rows:], "dp", 1)
    grad_up = dot_tn(dpre, second_all)
    grad_up_bias = jnp.sum(wide(dpre), axis=0)
    joined = low(middle + lowered + wide(b_down))

    upstream = wide(cotangent)
    pull_two = jax.vjp(normalize, middle, gain_two, shift_two)[1]
    grad_middle_norm, grad_gain_two, grad_shift_two = pull_two(grad_second)
    grad_middle = upstream + grad_middle_norm
    grad_branch = low(gate * grad_middle)
    gate_term = grad_middle * branch * gate * (1.0 - gate)
    grad_gate = jnp.stack(
        [
            jnp.sum(jnp.where(visual[:, None], 0.0, gate_term), axis=0),
            jnp.sum(jnp.where(visual[:, None], gate_term, 0.0), axis=0),
        ]
    )
    grad_out_bias = jnp.sum(wide(grad_branch), axis=0)
    grad_attended = low(dot_nt(grad_branch, w_out))
    extra = members * span - width
    if extra:
        grad_attended = jnp.pad(grad_attended, ((0, 0), (0, extra)))
    grad_slots = grad_attended.reshape(rows, members, span).transpose(1, 0, 2)
    grad_slots = jnp.take(grad_slots, slot_ids, axis=0)
    grad_mixed = jnp.stack(
        [grad_slots[0]] + [flip(grad_slots[j], "tensor", j) for j in range(1, members)], 0
    )
    grad_out = dot_tn(attended, grad_branch)

    grad_q, grad_k, grad_v = attention_backward(
        per_head,
        rows,
        queries,
        keys,
        values,
        logs,
        widen(grad_mixed.reshape(SEQ, span)),
    )
    normed_part = dot_nt(grad_q, w_q) + dot_nt(grad_k, w_k) + dot_nt(grad_v, w_v)
    normed_part = normed_part.reshape(members, rows, width)
    grad_normed = normed_part[0]
    for j in range(1, members):
        grad_normed = grad_normed + wide(flip(low(normed_part[j]), "tensor", j))
    pull_one = jax.vjp(normalize, inputs, gain_one, shift_one)[1]
    grad_inputs_norm, grad_gain_one, grad_shift_one = pull_one(grad_normed)
    grad_blocks = grad_middle + grad_inputs_norm

    def z_reduce(value):
        total = value[ring - 1]
        for slot in range(ring - 2, -1, -1):
            total = wide(z_shift(low(total), -1)) + value[slot]
        return total

    def x_reduce(value):
        total = value[:, 0]
        for step in range(1, line):
            total = total + wide(x_shift(low(value[:, step]), -step))
        return total

    grad_down = grad_down.reshape(ring, line, 2, quarter, width)
    grad_down = grad_down[:, :, 0] + wide(flip(low(grad_down[:, :, 1]), "dp", 2))
    grad_down = low(exchange_sum(z_reduce(x_reduce(grad_down)), dp_rest))
    grad_down = jnp.stack([grad_down, flip(grad_down, "dp", 2)], 0)
    grad_up = grad_up.reshape(ring, line, 2, quarter, width)
    grad_up = z_reduce(x_reduce(grad_up))
    sent_up = low(grad_up)
    grad_up = wide(sent_up) + wide(flip(sent_up[::-1], "dp", 2))
    grad_up = low(exchange_sum(grad_up, dp_rest))
    ffn = jnp.stack([grad_down, grad_up], 0)
    ffn = jnp.stack([ffn, flip(ffn, "dp", 1)], 0)
    ffn = jnp.where(side == 0, ffn, ffn[:, :, ::-1])
    ffn = jnp.where(core == 0, ffn, ffn[::-1])
    grad_down_out = wide(ffn[:, 0].reshape(shard, width))
    grad_up_out = wide(ffn[:, 1].reshape(shard, width)).T

    halvings = [("dp", 1, core), ("dp", 2, side)]
    for mask in (1, 2):
        halvings.append(("tensor", mask, (t_pos // mask) % 2))
    rest = [("tensor", mask) for mask in bits_of(tensor_size)[2:]] + dp_rest
    total = grad_out
    for axis, mask, bit in halvings:
        total = total.reshape((2, total.shape[0] // 2, width))
        total = pick(total, bit) + wide(flip(low(pick(total, 1 - bit)), axis, mask))
    gathered = low(exchange_sum(total, rest))[None]
    for axis, mask, bit in halvings[::-1]:
        gathered = jnp.concatenate([gathered, flip(gathered, axis, mask)], 0)
    code = core * 8 + side * 4 + (t_pos % 2) * 2 + (t_pos // 2) % 2
    order = jnp.arange(16, dtype=jnp.int32) ^ code
    grad_out_full = wide(jnp.take(gathered, order, axis=0).reshape(width, width))

    grad_w = jnp.stack(
        [dot_tn(grad, normed_all)[:span] for grad in (grad_q, grad_k, grad_v)], 0
    ).reshape(3, 2, span // 2, width)
    grad_w = jnp.moveaxis(grad_w, 1, 0)
    grad_w = pick(grad_w, core) + wide(flip(low(pick(grad_w, 1 - core)), "dp", 1))
    grad_w = jnp.moveaxis(grad_w.reshape(3, 2, span // 4, width), 1, 0)
    grad_w = pick(grad_w, side) + wide(flip(low(pick(grad_w, 1 - side)), "dp", 2))
    grad_w = low(exchange_sum(grad_w, tensor_rest + dp_rest))
    moves = [("tensor", mask) for mask in member_masks] + [("dp", 2)]
    weight_grads = []
    for which in range(3):
        shiftby = which % len(moves)
        turns = moves[shiftby:] + moves[:shiftby] + [("dp", 1)]
        have = {(): grad_w[which]}
        box = grad_w[which][None]
        for axis, mask in turns:
            box = jnp.stack([box, flip(box, axis, mask)], 0).reshape(
                (2 * box.shape[0],) + box.shape[1:]
            )
        box = box.reshape((2,) * len(turns) + (span // 4, width))
        held = turns[::-1]
        wanted = [("tensor", mask) for mask in member_masks[::-1]] + [("dp", 1), ("dp", 2)]
        box = box.transpose([held.index(name) for name in wanted] + [len(held), len(held) + 1])
        box = box.reshape(members * 4, span // 4, width)
        order = jnp.arange(members * 4, dtype=jnp.int32) ^ (member * 4 + core * 2 + side)
        full = jnp.take(box, order, axis=0).reshape(members * span, width)[:width]
        weight_grads.append(wide(full).T)

    def place(vector):
        base = jnp.zeros((members * span,), F32)
        return lax.dynamic_update_slice_in_dim(base, vector, member * span, 0)[:width]

    abs_t = jnp.arange(tensor_size, dtype=jnp.int32)
    slot_of = ((z_pos - abs_t // line) % ring) * line + (x_pos - abs_t % line) % line
    bias_sum = jnp.take(grad_up_bias.reshape(tensor_size, 2, quarter), slot_of, axis=0)
    bias_sum = jnp.where(side == 0, bias_sum, bias_sum[:, ::-1]).reshape(tensor_size, 1, 2 * quarter)
    both = jnp.arange(2, dtype=jnp.int32)[None, :, None]
    bias_sum = jnp.where(both == core, bias_sum, 0.0).reshape(hidden_total // width, width)
    early = jnp.concatenate(
        [
            jnp.stack([grad_out_bias, grad_gain_two, grad_shift_two, jnp.sum(upstream, axis=0)], 0),
            grad_gate,
            bias_sum,
        ],
        0,
    )
    early = sum_everywhere(early)
    late = jnp.stack(
        [
            place(jnp.sum(wide(grad_q), axis=0)[:span]),
            place(jnp.sum(wide(grad_v), axis=0)[:span]),
            grad_gain_one,
            grad_shift_one,
        ],
        0,
    )
    late = sum_everywhere(late)
    bias_out = lax.dynamic_slice_in_dim(early[6:].reshape(hidden_total), t_pos * shard, shard, 0)
    return (
        joined,
        grad_blocks,
        weight_grads[0],
        weight_grads[1],
        weight_grads[2],
        grad_out_full,
        late[0],
        late[1],
        early[0],
        late[2],
        late[3],
        early[1],
        early[2],
        early[4:6],
        grad_up_out,
        bias_out,
        grad_down_out,
        early[3],
    )


def solution(mesh):
    rows = P(("dp", "tensor"), None)
    in_specs = (rows, P("dp", None), rows) + (P(),) * 12 + (
        P(None, "tensor"),
        P("tensor"),
        P("tensor", None),
        P(),
    )
    out_specs = (rows, rows) + (P(),) * 12 + (
        P(None, "tensor"),
        P("tensor"),
        P("tensor", None),
        P(),
    )
    return jax.shard_map(local, mesh=mesh, in_specs=in_specs, out_specs=out_specs, check_vma=False)
```

```python
import functools

import jax
import jax.numpy as jnp
from jax import lax
from jax.experimental import pallas as pl
from jax.experimental.pallas import tpu as pltpu
from jax.sharding import PartitionSpec as P

HEADS = 12
HEAD_DIM = 64
TEXT_SLOTS = 896
SEQ = 1024
EPSILON = 1e-05
BF = jnp.bfloat16
F32 = jnp.float32


def normalize(values, gain, shift):
    centre = values - jnp.mean(values, axis=-1, keepdims=True)
    spread = jnp.mean(centre * centre, axis=-1, keepdims=True)
    return centre * lax.rsqrt(spread + EPSILON) * gain + shift


def gelu_exact(values):
    return jax.nn.gelu(values, approximate=False)


def gelu_grad(values, upstream):
    return jax.vjp(gelu_exact, values)[1](upstream)[0]


def dot_nn(left, right):
    return lax.dot_general(left, right, (((1,), (0,)), ((), ())), preferred_element_type=F32)


def dot_tn(left, right):
    return lax.dot_general(left, right, (((0,), (0,)), ((), ())), preferred_element_type=F32)


def dot_nt(left, right):
    return lax.dot_general(left, right, (((1,), (1,)), ((), ())), preferred_element_type=F32)


def pick(array, index):
    return lax.dynamic_index_in_dim(array, index, 0, keepdims=False)


def low(value):
    return value.astype(BF)


def wide(value):
    return value.astype(F32)


def flip(value, axis, mask):
    size = lax.axis_size(axis)
    return lax.ppermute(value, axis, [(i, i ^ mask) for i in range(size)])


def bits_of(size):
    found = []
    mask = 1
    while mask < size:
        found.append(mask)
        mask *= 2
    return found


def sum_everywhere(value):
    for axis in ("dp", "tensor"):
        for mask in bits_of(lax.axis_size(axis)):
            value = value + flip(value, axis, mask)
    return value


def exchange_sum(value, stages):
    for axis, mask in stages:
        sent = low(value)
        value = wide(sent) + wide(flip(sent, axis, mask))
    return value


def head_mask(lanes, head):
    return (lanes >= head * HEAD_DIM) & (lanes < (head + 1) * HEAD_DIM)


def bit(index, mask):
    return (index // mask) % 2


def turned(index, mask):
    return index + mask - 2 * mask * bit(index, mask)


def place_of(masks, gathered, index):
    return tuple(slice(None) if mask in gathered else bit(index, mask) for mask in masks)


class Copies:
    def __init__(self, send, recv):
        self.send, self.recv, self.used, self.open = send, recv, 0, []

    def make(self, source, target, device, at=None):
        if at is None:
            at = self.used
            self.used += 1
        return pltpu.make_async_remote_copy(
            src_ref=source,
            dst_ref=target,
            send_sem=self.send.at[at],
            recv_sem=self.recv.at[at],
            device_id=device,
            device_id_type=pl.DeviceIdType.MESH,
        )

    def start(self, source, target, device):
        copy = self.make(source, target, device)
        copy.start()
        self.open.append(copy)
        return copy

    def drain(self):
        for copy in self.open:
            copy.wait_send()
        self.open = []


def greet(devices):
    barrier = pltpu.get_barrier_semaphore()
    for device in devices:
        pl.semaphore_signal(
            barrier, inc=1, device_id=device, device_id_type=pl.DeviceIdType.MESH
        )
    return barrier


def weight_parts(tensor_masks, width):
    unit = width // 6
    low_masks, high = tensor_masks[:2], tensor_masks[2:][::-1]
    one, other = high + low_masks, high + low_masks[::-1]
    return (
        (0, 2 * unit, True, one),
        (2 * unit, 2 * unit, True, other),
        (4 * unit, unit, True, other),
        (5 * unit, unit, False, other),
    )


def front_copies(tensor_size, members, width):
    masks, inner = bits_of(tensor_size), bits_of(members)
    parts = weight_parts(masks, width)
    forwards = sum(1 for part in parts if part[2])
    return 2 * len(inner) + len(masks) * (len(parts) + forwards + 1) + 1 + members


def front_kernel(
    heads,
    members,
    tensor_size,
    blocks_ref,
    norm_ref,
    wq_ref,
    wk_ref,
    wv_ref,
    b_ref,
    counts_ref,
    cot_ref,
    piece_ref,
    up_bias_ref,
    q_ref,
    k_ref,
    v_ref,
    l_ref,
    normed_out,
    att_out,
    cot_out,
    up_out,
    down_out,
    bias_out,
    normed,
    mixed,
    att,
    cots,
    weights,
    biases,
    send,
    recv,
    here,
):
    t_pos = lax.axis_index("tensor")
    d_pos = lax.axis_index("dp")
    member = t_pos % members
    side = bit(d_pos, 2)
    rows, width = blocks_ref.shape
    wide_span = q_ref.shape[1]
    masks, inner = bits_of(tensor_size), bits_of(members)
    outer_first, inner_first = masks[::-1], inner[::-1]
    scale = HEAD_DIM ** (-0.5)
    extra = heads * HEAD_DIM
    copies = Copies(send, recv)

    def along(mask):
        return {"tensor": turned(t_pos, mask)}

    def slot(index):
        return tuple(bit(index, mask) for mask in inner_first)

    diagonals = [j for j in range(1, members) if j not in inner]

    def xor_member(j):
        return sum(mask * ((bit(member, mask) + bit(j, mask)) % 2) for mask in inner)

    peers = [along(mask) for mask in masks]
    peers += [{"tensor": t_pos - member + xor_member(j)} for j in diagonals]
    peers += [{"dp": turned(d_pos, 1)}, {"dp": turned(d_pos, 2)}]
    barrier = greet(peers)

    own = place_of(outer_first, (), t_pos)
    local = [
        pltpu.make_async_copy(piece_ref, weights.at[(slice(None),) + own], here.at[0]),
        pltpu.make_async_copy(cot_ref, cots.at[0], here.at[1]),
        pltpu.make_async_copy(up_bias_ref, biases.at[own], here.at[2]),
    ]
    for copy in local:
        copy.start()
    mine = slot(member)
    step = rows // 2
    for start in range(0, rows, step):
        at = pl.ds(start, step)
        normed[mine + (at, slice(None))] = low(
            normalize(wide(blocks_ref[at, :]), norm_ref[0:1, :], norm_ref[1:2, :])
        )
    for copy in local:
        copy.wait()
    pl.semaphore_wait(barrier, len(peers))

    half = width // 2
    halves = ((pl.ds(0, half), inner), (pl.ds(half, half), inner[::-1]))

    def send_rows(stage):
        sent = []
        for columns, order in halves:
            block = normed.at[place_of(inner_first, order[:stage], member) + (slice(None), columns)]
            sent.append(copies.start(block, block, along(order[stage])))
        return sent

    parts = weight_parts(masks, width)

    def send_weights(stage):
        sent = []
        for start, size, split, order in parts:
            rest = (side if split else slice(None), slice(None), pl.ds(start, size))
            block = weights.at[(slice(None),) + place_of(outer_first, order[:stage], t_pos) + rest]
            sent.append(copies.start(block, block, along(order[stage])))
        block = biases.at[place_of(outer_first, masks[:stage], t_pos)]
        sent.append(copies.start(block, block, along(masks[stage])))
        return sent

    def pass_weights(stage):
        sent = []
        for start, size, split, order in parts:
            if split:
                other = turned(t_pos, order[stage])
                rest = (side, slice(None), pl.ds(start, size))
                block = weights.at[(slice(None),) + place_of(outer_first, order[:stage], other) + rest]
                sent.append(copies.start(block, block, {"dp": turned(d_pos, 2)}))
        return sent

    def project(block):
        at = pl.ds(pl.multiple_of(block * rows, rows), rows)
        part = normed[slot(block) + (slice(None), slice(None))]
        position = block * rows + lax.broadcasted_iota(jnp.int32, (rows, wide_span), 0)
        lane = lax.broadcasted_iota(jnp.int32, (rows, wide_span), 1)
        text, visual = counts_ref[0:1, 0:1], counts_ref[1:2, 0:1]
        bound = jnp.where(position >= TEXT_SLOTS, visual + TEXT_SLOTS, text)
        tail = jnp.where((lane > extra) & (lane < extra + 4), 1.0, 0.0)
        tail = jnp.where((lane == extra) & (position >= bound), -1e30, tail)
        q_ref[at, :] = low(low(dot_nn(part, wq_ref[...]) + b_ref[0:1, :]) * scale)
        k_ref[at, :] = low(dot_nn(part, wk_ref[...]) + tail)
        v_ref[at, :] = low(dot_nn(part, wv_ref[...]) + b_ref[1:2, :])

    arriving = send_rows(0)
    other_cots = copies.start(cot_ref, cots.at[1], {"dp": turned(d_pos, 1)})
    for stage in range(1, len(inner)):
        for copy in arriving:
            copy.wait_recv()
        arriving = send_rows(stage)
    flows = send_weights(0)
    forwards = []
    for copy in arriving:
        copy.wait_recv()

    @pl.loop(0, members)
    def _(block):
        project(block)

    lanes = lax.broadcasted_iota(jnp.int32, (rows, wide_span), 1)
    unit = low(jnp.where(lanes == extra, 1.0, 0.0))
    side_lanes = lax.broadcasted_iota(jnp.int32, (rows, 128), 1)
    base = copies.used
    copies.used += members
    lane_block = pl.ds(pl.multiple_of(member * wide_span, wide_span), wide_span)

    def att_copy(j, block):
        return copies.make(
            mixed.at[block], att.at[:, lane_block], {"tensor": t_pos - member + block}, base + j
        )

    def attend(j):
        block = xor_member(j)
        at = pl.ds(pl.multiple_of(block * rows, rows), rows)
        query = q_ref[at, :]
        total_mix = jnp.zeros((rows, wide_span), F32)
        logs = jnp.zeros((rows, 128), F32)
        for head in range(heads):
            chosen = head_mask(lanes, head)
            left = jnp.where(chosen, query, unit)
            scores = dot_nt(left, k_ref[...])
            peak = jnp.max(scores, axis=-1, keepdims=True)
            expo = jnp.exp(scores - peak)
            total = jnp.sum(expo, axis=-1, keepdims=True)
            out = dot_nn(low(expo), v_ref[...]) / total
            total_mix = jnp.where(chosen, out, total_mix)
            logs = jnp.where(side_lanes == head, peak + jnp.log(total), logs)
        mixed[block] = low(total_mix)
        l_ref[at, :] = logs

    @pl.loop(0, members - 1)
    def _(turn):
        j = members - 1 - turn
        attend(j)
        att_copy(j, xor_member(j)).start()

    attend(0)
    own_att = pltpu.make_async_copy(mixed.at[member], att.at[:, lane_block], here.at[0])
    own_att.start()

    for stage in range(1, len(masks)):
        for copy in flows:
            copy.wait_recv()
        flows = send_weights(stage)
        forwards += pass_weights(stage - 1)
    normed_copy = pltpu.make_async_copy(normed, normed_out, here.at[1])
    normed_copy.start()
    other_cots.wait_recv()
    cot_copy = pltpu.make_async_copy(cots, cot_out, here.at[2])
    cot_copy.start()
    own_att.wait()
    for j in range(1, members):
        att_copy(j, xor_member(j)).wait()
    att_copy_out = pltpu.make_async_copy(att, att_out, here.at[3])
    att_copy_out.start()
    for copy in flows:
        copy.wait_recv()
    forwards += pass_weights(len(masks) - 1)
    bias_copy = pltpu.make_async_copy(biases, bias_out, here.at[4])
    bias_copy.start()
    for copy in forwards:
        copy.wait_recv()
    up_copy = pltpu.make_async_copy(weights.at[0], up_out, here.at[5])
    up_copy.start()
    down_copy = pltpu.make_async_copy(weights.at[1], down_out, here.at[0])
    down_copy.start()
    for copy in (normed_copy, cot_copy, att_copy_out, bias_copy, up_copy, down_copy):
        copy.wait()
    copies.drain()


def front(
    heads, members, tensor_size, blocks, norm, w_q, w_k, w_v, bias, counts, cotangent, piece, up_bias
):
    rows, width = blocks.shape
    wide_span = w_q.shape[1]
    total = members * rows
    inner, outer = len(bits_of(members)), len(bits_of(tensor_size))
    square = jax.ShapeDtypeStruct((total, wide_span), BF)
    normed = jax.ShapeDtypeStruct((2,) * inner + (rows, width), BF)
    att = jax.ShapeDtypeStruct((rows, members * wide_span), BF)
    cots = jax.ShapeDtypeStruct((2, rows, width), BF)
    weights = jax.ShapeDtypeStruct((2,) * outer + piece.shape[1:], BF)
    biases = jax.ShapeDtypeStruct((2,) * outer + up_bias.shape, F32)
    number = front_copies(tensor_size, members, width)
    vmem = pl.BlockSpec(memory_space=pltpu.VMEM)
    away = pl.BlockSpec(memory_space=pl.ANY)
    held = (normed, att, cots, weights, weights, biases)
    return pl.pallas_call(
        functools.partial(front_kernel, heads, members, tensor_size),
        out_shape=(square, square, square, jax.ShapeDtypeStruct((total, 128), F32)) + held,
        in_specs=[vmem] * 10,
        out_specs=(vmem,) * 4 + (away,) * 6,
        scratch_shapes=[
            pltpu.VMEM(normed.shape, BF),
            pltpu.VMEM((members, rows, wide_span), BF),
            pltpu.VMEM(att.shape, BF),
            pltpu.VMEM(cots.shape, BF),
            pltpu.VMEM((2,) + weights.shape, BF),
            pltpu.VMEM(biases.shape, F32),
            pltpu.SemaphoreType.DMA((number,)),
            pltpu.SemaphoreType.DMA((number,)),
            pltpu.SemaphoreType.DMA((6,)),
        ],
        compiler_params=pltpu.CompilerParams(
            vmem_limit_bytes=48 << 20, collective_id=0, has_side_effects=True
        ),
        cost_estimate=pl.CostEstimate(
            flops=20_000_000_000, bytes_accessed=20_000_000, transcendentals=3_000_000
        ),
    )(blocks, norm, w_q, w_k, w_v, bias, counts, cotangent, piece, up_bias)


def attention_backward_kernel(
    heads, rows, q_ref, k_ref, v_ref, l_ref, g_ref, dq_ref, dk_ref, dv_ref, sum_k, sum_v
):
    total_rows, wide_span = q_ref.shape
    count = total_rows // rows
    scale = HEAD_DIM ** (-0.5)
    extra = heads * HEAD_DIM
    lanes = lax.broadcasted_iota(jnp.int32, (rows, wide_span), 1)
    sum_k[...] = jnp.zeros_like(sum_k)
    sum_v[...] = jnp.zeros_like(sum_v)

    @pl.loop(0, count)
    def _(block):
        at = pl.ds(pl.multiple_of(block * rows, rows), rows)
        query = q_ref[at, :]
        grad = g_ref[at, :]
        grad_q = jnp.zeros((rows, wide_span), F32)
        for head in range(heads):
            chosen = head_mask(lanes, head)
            log_total = l_ref[at, head : head + 1]
            high = low(log_total)
            rest = log_total - wide(high)
            middle = low(rest)
            last = low(rest - wide(middle))
            fill = jnp.where(lanes == extra, 1.0, 0.0)
            fill = jnp.where(lanes == extra + 1, -wide(high), fill)
            fill = jnp.where(lanes == extra + 2, -wide(middle), fill)
            fill = jnp.where(lanes == extra + 3, -wide(last), fill)
            left = jnp.where(chosen, query, low(fill))
            upstream = jnp.where(chosen, grad, jnp.zeros_like(grad))
            probs = jnp.exp(dot_nt(k_ref[...], left))
            grad_probs = dot_nt(v_ref[...], upstream)
            centred = jnp.sum(probs * grad_probs, axis=0, keepdims=True)
            grad_scores = low(probs * (grad_probs - centred))
            sum_k[...] += dot_nn(grad_scores, left)
            sum_v[...] += dot_nn(low(probs), upstream)
            out = dot_tn(grad_scores, k_ref[...]) * scale
            grad_q = jnp.where(chosen, out, grad_q)
        dq_ref[at, :] = low(grad_q)

    keep = lax.broadcasted_iota(jnp.int32, (total_rows, wide_span), 1) < extra
    dk_ref[...] = low(jnp.where(keep, sum_k[...], 0.0))
    dv_ref[...] = low(sum_v[...])


def attention_backward(heads, rows, queries, keys, values, logs, grad_mixed):
    total_rows, wide_span = queries.shape
    square = jax.ShapeDtypeStruct((total_rows, wide_span), BF)
    return pl.pallas_call(
        functools.partial(attention_backward_kernel, heads, rows),
        out_shape=(square, square, square),
        scratch_shapes=[
            pltpu.VMEM((total_rows, wide_span), F32),
            pltpu.VMEM((total_rows, wide_span), F32),
        ],
        compiler_params=pltpu.CompilerParams(vmem_limit_bytes=48 << 20),
        cost_estimate=pl.CostEstimate(
            flops=30_000_000_000, bytes_accessed=6_000_000, transcendentals=3_000_000
        ),
    )(queries, keys, values, logs, grad_mixed)


def local(
    blocks,
    counts,
    cotangent,
    w_query,
    w_key,
    w_value,
    w_out,
    b_query,
    b_value,
    b_out,
    norm1_gain,
    norm1_bias,
    norm2_gain,
    norm2_bias,
    gate_logits,
    w_up,
    b_up,
    w_down,
    b_down,
):
    rows, width = blocks.shape
    tensor_size = lax.axis_size("tensor")
    dp_size = lax.axis_size("dp")
    t_pos = lax.axis_index("tensor")
    d_pos = lax.axis_index("dp")
    members = SEQ // rows
    member = t_pos % members
    per_head = -(-HEADS // members)
    span = per_head * HEAD_DIM
    ring = 4
    line = tensor_size // ring
    z_pos = t_pos // line
    x_pos = t_pos % line
    core = d_pos % 2
    side = (d_pos // 2) % 2
    shard = w_up.shape[1]
    quarter = shard // 4
    hidden_total = shard * tensor_size
    dp_rest = [("dp", mask) for mask in bits_of(dp_size)[2:]]
    member_masks = bits_of(members)
    tensor_rest = [("tensor", mask) for mask in bits_of(tensor_size)[len(member_masks):]]

    def z_shift(value, step):
        pairs = [
            (i, ((i // line + step) % ring) * line + i % line) for i in range(tensor_size)
        ]
        return lax.ppermute(value, "tensor", pairs)

    def x_shift(value, step):
        pairs = [
            (i, (i // line) * line + (i % line + step) % line) for i in range(tensor_size)
        ]
        return lax.ppermute(value, "tensor", pairs)

    gain_one = wide(norm1_gain)
    shift_one = wide(norm1_bias)
    gain_two = wide(norm2_gain)
    shift_two = wide(norm2_bias)
    logits_gate = wide(gate_logits)
    inputs = wide(blocks)

    doc_counts = pick(counts, t_pos // members)
    slot_ids = member ^ jnp.arange(members, dtype=jnp.int32)
    own_pos = member * rows + jnp.arange(rows, dtype=jnp.int32)
    visual = own_pos >= TEXT_SLOTS

    def head_part(weight):
        extra = per_head * HEAD_DIM * members - width
        if extra:
            weight = jnp.pad(weight, ((0, 0),) * (weight.ndim - 1) + ((0, extra),))
        return lax.dynamic_slice_in_dim(weight, member * span, span, weight.ndim - 1)

    wide_span = -(-(span + 4) // 128) * 128

    def widen(array):
        return jnp.pad(array, ((0, 0),) * (array.ndim - 1) + ((0, wide_span - array.shape[-1]),))

    w_q = widen(head_part(w_query))
    w_k = widen(head_part(w_key))
    w_v = widen(head_part(w_value))
    bias = wide(jnp.stack([widen(head_part(b_query)), widen(head_part(b_value))], 0))
    halves = (2, 2, quarter, width)
    piece = jnp.stack(
        [pick(w_up.T.reshape(halves), core), pick(w_down.reshape(halves), core)], 0
    )
    queries, keys, values, logs, normed_all, attended, cot_all, up_t, down, biases = front(
        per_head,
        members,
        tensor_size,
        blocks,
        jnp.stack([gain_one, shift_one], 0),
        w_q,
        w_k,
        w_v,
        bias,
        jnp.broadcast_to(doc_counts[:, None], (2, 128)),
        cotangent,
        piece,
        wide(b_up)[None, :],
    )
    normed_all = normed_all.reshape(SEQ, width)
    cot_all = cot_all.reshape(2 * rows, width)
    up_t = up_t.reshape(-1, width)
    down = down.reshape(-1, width)
    biases = biases.reshape(tensor_size, shard)
    biases = lax.dynamic_slice_in_dim(biases, core * (2 * quarter), 2 * quarter, 1).reshape(-1)
    extra_rows = members * span - width
    out_rows = jnp.pad(w_out, ((0, extra_rows), (0, 0))) if extra_rows else w_out
    out_rows = jnp.pad(out_rows.reshape(members, span, width), ((0, 0), (0, wide_span - span), (0, 0)))
    out_rows = out_rows.reshape(members * wide_span, width)

    branch = dot_nn(attended, out_rows) + wide(b_out)
    gate = jax.nn.sigmoid(
        jnp.where(visual[:, None], logits_gate[1][None, :], logits_gate[0][None, :])
    )
    middle = inputs + gate * branch
    second = low(normalize(middle, gain_two, shift_two))
    second_all = jnp.concatenate([second, flip(second, "dp", 1)], 0)

    pre = dot_nt(second_all, up_t) + biases
    hidden = low(gelu_exact(pre))
    grad_down = dot_tn(hidden, cot_all)
    spread = dot_nt(cot_all, down)
    dpre = low(gelu_grad(pre, spread))
    second_part = dot_nn(dpre, up_t)
    grad_second = second_part[:rows] + flip(second_part[rows:], "dp", 1)
    lowered_part = dot_nn(hidden, down)
    lowered = lowered_part[:rows] + flip(lowered_part[rows:], "dp", 1)
    grad_up = dot_tn(dpre, second_all)
    grad_up_bias = jnp.sum(wide(dpre), axis=0)
    joined = low(middle + lowered + wide(b_down))

    upstream = wide(cotangent)
    pull_two = jax.vjp(normalize, middle, gain_two, shift_two)[1]
    grad_middle_norm, grad_gain_two, grad_shift_two = pull_two(grad_second)
    grad_middle = upstream + grad_middle_norm
    grad_branch = low(gate * grad_middle)
    gate_term = grad_middle * branch * gate * (1.0 - gate)
    grad_gate = jnp.stack(
        [
            jnp.sum(jnp.where(visual[:, None], 0.0, gate_term), axis=0),
            jnp.sum(jnp.where(visual[:, None], gate_term, 0.0), axis=0),
        ]
    )
    grad_out_bias = jnp.sum(wide(grad_branch), axis=0)
    grad_attended = low(dot_nt(grad_branch, out_rows))
    grad_slots = grad_attended.reshape(rows, members, wide_span).transpose(1, 0, 2)
    grad_slots = jnp.take(grad_slots, slot_ids, axis=0)
    grad_mixed = jnp.stack(
        [grad_slots[0]] + [flip(grad_slots[j], "tensor", j) for j in range(1, members)], 0
    )
    grad_mixed = jnp.take(grad_mixed, slot_ids, axis=0)
    grad_out = dot_tn(attended, grad_branch)
    grad_out = grad_out.reshape(members, wide_span, width)[:, :span].reshape(-1, width)[:width]

    grad_q, grad_k, grad_v = attention_backward(
        per_head,
        rows,
        queries,
        keys,
        values,
        logs,
        grad_mixed.reshape(SEQ, wide_span),
    )
    normed_part = dot_nt(grad_q, w_q) + dot_nt(grad_k, w_k) + dot_nt(grad_v, w_v)
    normed_part = jnp.take(normed_part.reshape(members, rows, width), slot_ids, axis=0)
    grad_normed = normed_part[0]
    for j in range(1, members):
        grad_normed = grad_normed + wide(flip(low(normed_part[j]), "tensor", j))
    pull_one = jax.vjp(normalize, inputs, gain_one, shift_one)[1]
    grad_inputs_norm, grad_gain_one, grad_shift_one = pull_one(grad_normed)
    grad_blocks = grad_middle + grad_inputs_norm

    def z_reduce(value):
        total = value[ring - 1]
        for slot in range(ring - 2, -1, -1):
            total = wide(z_shift(low(total), -1)) + value[slot]
        return total

    def x_reduce(value):
        total = value[:, 0]
        for step in range(1, line):
            total = total + wide(x_shift(low(value[:, step]), -step))
        return total

    slot_z = (z_pos - jnp.arange(ring, dtype=jnp.int32)) % ring
    slot_x = (x_pos - jnp.arange(line, dtype=jnp.int32)) % line
    slot_t = (slot_z[:, None] * line + slot_x[None, :]).reshape(-1)

    def relative(value):
        value = jnp.take(value.reshape(tensor_size, 2, quarter, width), slot_t, axis=0)
        value = jnp.where(side == 0, value, value[:, ::-1])
        return value.reshape(ring, line, 2, quarter, width)

    grad_down = relative(grad_down)
    grad_down = grad_down[:, :, 0] + wide(flip(low(grad_down[:, :, 1]), "dp", 2))
    grad_down = low(exchange_sum(z_reduce(x_reduce(grad_down)), dp_rest))
    grad_down = jnp.stack([grad_down, flip(grad_down, "dp", 2)], 0)
    grad_up = relative(grad_up)
    grad_up = z_reduce(x_reduce(grad_up))
    sent_up = low(grad_up)
    grad_up = wide(sent_up) + wide(flip(sent_up[::-1], "dp", 2))
    grad_up = low(exchange_sum(grad_up, dp_rest))
    ffn = jnp.stack([grad_down, grad_up], 0)
    ffn = jnp.stack([ffn, flip(ffn, "dp", 1)], 0)
    ffn = jnp.where(side == 0, ffn, ffn[:, :, ::-1])
    ffn = jnp.where(core == 0, ffn, ffn[::-1])
    grad_down_out = wide(ffn[:, 0].reshape(shard, width))
    grad_up_out = wide(ffn[:, 1].reshape(shard, width)).T

    halvings = [("dp", 1, core), ("dp", 2, side)]
    for mask in (1, 2):
        halvings.append(("tensor", mask, (t_pos // mask) % 2))
    rest = [("tensor", mask) for mask in bits_of(tensor_size)[2:]] + dp_rest
    total = grad_out
    for axis, mask, bit in halvings:
        total = total.reshape((2, total.shape[0] // 2, width))
        total = pick(total, bit) + wide(flip(low(pick(total, 1 - bit)), axis, mask))
    gathered = low(exchange_sum(total, rest))[None]
    for axis, mask, bit in halvings[::-1]:
        gathered = jnp.concatenate([gathered, flip(gathered, axis, mask)], 0)
    code = core * 8 + side * 4 + (t_pos % 2) * 2 + (t_pos // 2) % 2
    order = jnp.arange(16, dtype=jnp.int32) ^ code
    grad_out_full = wide(jnp.take(gathered, order, axis=0).reshape(width, width))

    grad_w = jnp.stack(
        [dot_tn(grad, normed_all)[:span] for grad in (grad_q, grad_k, grad_v)], 0
    ).reshape(3, 2, span // 2, width)
    grad_w = jnp.moveaxis(grad_w, 1, 0)
    grad_w = pick(grad_w, core) + wide(flip(low(pick(grad_w, 1 - core)), "dp", 1))
    grad_w = jnp.moveaxis(grad_w.reshape(3, 2, span // 4, width), 1, 0)
    grad_w = pick(grad_w, side) + wide(flip(low(pick(grad_w, 1 - side)), "dp", 2))
    grad_w = low(exchange_sum(grad_w, tensor_rest + dp_rest))
    moves = [("tensor", mask) for mask in member_masks] + [("dp", 2)]
    weight_grads = []
    for which in range(3):
        shiftby = which % len(moves)
        turns = moves[shiftby:] + moves[:shiftby] + [("dp", 1)]
        have = {(): grad_w[which]}
        box = grad_w[which][None]
        for axis, mask in turns:
            box = jnp.stack([box, flip(box, axis, mask)], 0).reshape(
                (2 * box.shape[0],) + box.shape[1:]
            )
        box = box.reshape((2,) * len(turns) + (span // 4, width))
        held = turns[::-1]
        wanted = [("tensor", mask) for mask in member_masks[::-1]] + [("dp", 1), ("dp", 2)]
        box = box.transpose([held.index(name) for name in wanted] + [len(held), len(held) + 1])
        box = box.reshape(members * 4, span // 4, width)
        order = jnp.arange(members * 4, dtype=jnp.int32) ^ (member * 4 + core * 2 + side)
        full = jnp.take(box, order, axis=0).reshape(members * span, width)[:width]
        weight_grads.append(wide(full).T)

    def place(vector):
        base = jnp.zeros((members * span,), F32)
        return lax.dynamic_update_slice_in_dim(base, vector, member * span, 0)[:width]

    bias_sum = grad_up_bias.reshape(tensor_size, 1, 2 * quarter)
    both = jnp.arange(2, dtype=jnp.int32)[None, :, None]
    bias_sum = jnp.where(both == core, bias_sum, 0.0).reshape(hidden_total // width, width)
    early = jnp.concatenate(
        [
            jnp.stack([grad_out_bias, grad_gain_two, grad_shift_two, jnp.sum(upstream, axis=0)], 0),
            grad_gate,
            bias_sum,
        ],
        0,
    )
    early = sum_everywhere(early)
    late = jnp.stack(
        [
            place(jnp.sum(wide(grad_q), axis=0)[:span]),
            place(jnp.sum(wide(grad_v), axis=0)[:span]),
            grad_gain_one,
            grad_shift_one,
        ],
        0,
    )
    late = sum_everywhere(late)
    bias_out = lax.dynamic_slice_in_dim(early[6:].reshape(hidden_total), t_pos * shard, shard, 0)
    return (
        joined,
        grad_blocks,
        weight_grads[0],
        weight_grads[1],
        weight_grads[2],
        grad_out_full,
        late[0],
        late[1],
        early[0],
        late[2],
        late[3],
        early[1],
        early[2],
        early[4:6],
        grad_up_out,
        bias_out,
        grad_down_out,
        early[3],
    )


def solution(mesh):
    rows = P(("dp", "tensor"), None)
    in_specs = (rows, P("dp", None), rows) + (P(),) * 12 + (
        P(None, "tensor"),
        P("tensor"),
        P("tensor", None),
        P(),
    )
    out_specs = (rows, rows) + (P(),) * 12 + (
        P(None, "tensor"),
        P("tensor"),
        P("tensor", None),
        P(),
    )
    return jax.shard_map(local, mesh=mesh, in_specs=in_specs, out_specs=out_specs, check_vma=False)
```

```python
import functools

import jax
import jax.numpy as jnp
from jax import lax
from jax.experimental import pallas as pl
from jax.experimental.pallas import tpu as pltpu
from jax.sharding import PartitionSpec as P

HEADS = 12
HEAD_DIM = 64
TEXT_SLOTS = 896
SEQ = 1024
EPSILON = 1e-05
PARTS = 3
HIDDEN_ORDERS = (("x", "y", "z1", "z0"), ("z0", "y", "x", "z1"), ("y", "x", "z0", "z1"))
OUT_ORDER = ("x", "y", "z0")
BACK_PROGRAM = (
    ("out", "h2", "h1", "*block0", "out", "h0", "*block1", "out", "*square", "square", "out"),
    ("*rows", "rows", "early", "h2", "out", "early", "square", "early", "h0", "square", "h1"),
    ("rows", "out", "h0", "early", "square", "h2", "out", "h1", "rows", "early", "*norm", "late"),
    ("square", "late", "out", "h1", "h0", "h2", "late", "early", "square", "h0", "out", "late"),
    ("h1", "out", "h2", "h0", "h0", "h1", "square", "late", "h1", "h2", "square", "h2"),
)
FRONT_CUTS = (16, 18, 19)
FRONT_FIRST = True
BF = jnp.bfloat16
F32 = jnp.float32


def normalize(values, gain, shift):
    centre = values - jnp.mean(values, axis=-1, keepdims=True)
    spread = jnp.mean(centre * centre, axis=-1, keepdims=True)
    return centre * lax.rsqrt(spread + EPSILON) * gain + shift


def gelu_exact(values):
    return jax.nn.gelu(values, approximate=False)


def gelu_grad(values, upstream):
    return jax.vjp(gelu_exact, values)[1](upstream)[0]


def dot_nn(left, right):
    return lax.dot_general(left, right, (((1,), (0,)), ((), ())), preferred_element_type=F32)


def dot_tn(left, right):
    return lax.dot_general(left, right, (((0,), (0,)), ((), ())), preferred_element_type=F32)


def dot_nt(left, right):
    return lax.dot_general(left, right, (((1,), (1,)), ((), ())), preferred_element_type=F32)


def pick(array, index):
    return lax.dynamic_index_in_dim(array, index, 0, keepdims=False)


def low(value):
    return value.astype(BF)


def wide(value):
    return value.astype(F32)


def flip(value, axis, mask):
    size = lax.axis_size(axis)
    return lax.ppermute(value, axis, [(i, i ^ mask) for i in range(size)])


def bits_of(size):
    found = []
    mask = 1
    while mask < size:
        found.append(mask)
        mask *= 2
    return found


def sum_everywhere(value):
    for axis in ("dp", "tensor"):
        for mask in bits_of(lax.axis_size(axis)):
            value = value + flip(value, axis, mask)
    return value


def exchange_sum(value, stages):
    for axis, mask in stages:
        sent = low(value)
        value = wide(sent) + wide(flip(sent, axis, mask))
    return value


def head_mask(lanes, head):
    return (lanes >= head * HEAD_DIM) & (lanes < (head + 1) * HEAD_DIM)


def bit(index, mask):
    return (index // mask) % 2


def turned(index, mask):
    return index + mask - 2 * mask * bit(index, mask)


def place_of(masks, gathered, index):
    return tuple(slice(None) if mask in gathered else bit(index, mask) for mask in masks)


class Copies:
    def __init__(self, send, recv):
        self.send, self.recv, self.used, self.open = send, recv, 0, []

    def make(self, source, target, device, at=None):
        if at is None:
            at = self.used
            self.used += 1
        return pltpu.make_async_remote_copy(
            src_ref=source,
            dst_ref=target,
            send_sem=self.send.at[at],
            recv_sem=self.recv.at[at],
            device_id=device,
            device_id_type=pl.DeviceIdType.MESH,
        )

    def start(self, source, target, device):
        copy = self.make(source, target, device)
        copy.start()
        self.open.append(copy)
        return copy

    def drain(self):
        for copy in self.open:
            copy.wait_send()
        self.open = []


def greet(devices):
    barrier = pltpu.get_barrier_semaphore()
    for device in devices:
        pl.semaphore_signal(
            barrier, inc=1, device_id=device, device_id_type=pl.DeviceIdType.MESH
        )
    return barrier


def weight_parts(tensor_masks, width):
    unit = width // 6
    low_masks, high = tensor_masks[:2], tensor_masks[2:][::-1]
    one, other = high + low_masks, high + low_masks[::-1]
    return (
        (0, 2 * unit, True, other),
        (2 * unit, 2 * unit, True, other),
        (4 * unit, unit, True, one),
        (5 * unit, unit, False, one),
    )


def subsets(masks):
    found = [()]
    for mask in masks:
        found += [kept + (mask,) for kept in found]
    return found


def front_copies(tensor_size, members, width):
    masks, inner = bits_of(tensor_size), bits_of(members)
    parts = weight_parts(masks, width)
    forwards = sum(1 for part in parts if part[2])
    pieces = tensor_size - 1
    return 2 * len(inner) + pieces * (len(parts) + forwards) + len(masks) + 1 + members


def front_kernel(
    heads,
    members,
    tensor_size,
    blocks_ref,
    norm_ref,
    wq_ref,
    wk_ref,
    wv_ref,
    b_ref,
    counts_ref,
    cot_ref,
    piece_ref,
    up_bias_ref,
    q_ref,
    k_ref,
    v_ref,
    l_ref,
    normed_out,
    att_out,
    cot_out,
    up_out,
    down_out,
    bias_out,
    normed,
    mixed,
    att,
    cots,
    weights,
    biases,
    send,
    recv,
    here,
):
    t_pos = lax.axis_index("tensor")
    d_pos = lax.axis_index("dp")
    member = t_pos % members
    side = bit(d_pos, 2)
    rows, width = blocks_ref.shape
    wide_span = q_ref.shape[1]
    masks, inner = bits_of(tensor_size), bits_of(members)
    outer_first, inner_first = masks[::-1], inner[::-1]
    scale = HEAD_DIM ** (-0.5)
    extra = heads * HEAD_DIM
    copies = Copies(send, recv)

    def along(mask):
        return {"tensor": turned(t_pos, mask)}

    def slot(index):
        return tuple(bit(index, mask) for mask in inner_first)

    def slot_of(index):
        return tuple(bit(index, mask) for mask in outer_first)

    diagonals = [j for j in range(1, members) if j not in inner]

    def xor_member(j):
        return sum(mask * ((bit(member, mask) + bit(j, mask)) % 2) for mask in inner)

    peers = [along(mask) for mask in masks]
    peers += [{"tensor": t_pos - member + xor_member(j)} for j in diagonals]
    peers += [{"dp": turned(d_pos, 1)}, {"dp": turned(d_pos, 2)}]
    barrier = greet(peers)

    own = place_of(outer_first, (), t_pos)
    local = [
        pltpu.make_async_copy(piece_ref, weights.at[(slice(None),) + own], here.at[0]),
        pltpu.make_async_copy(cot_ref, cots.at[0], here.at[1]),
        pltpu.make_async_copy(up_bias_ref, biases.at[own], here.at[2]),
    ]
    for copy in local:
        copy.start()
    mine = slot(member)
    step = rows // 2
    for start in range(0, rows, step):
        at = pl.ds(start, step)
        normed[mine + (at, slice(None))] = low(
            normalize(wide(blocks_ref[at, :]), norm_ref[0:1, :], norm_ref[1:2, :])
        )
    for copy in local:
        copy.wait()
    pl.semaphore_wait(barrier, len(peers))

    half = width // 2
    halves = ((pl.ds(0, half), inner), (pl.ds(half, half), inner[::-1]))

    def send_rows(stage):
        sent = []
        for columns, order in halves:
            block = normed.at[place_of(inner_first, order[:stage], member) + (slice(None), columns)]
            sent.append(copies.start(block, block, along(order[stage])))
        return sent

    parts = weight_parts(masks, width)

    def device_of(kept):
        index = t_pos
        for mask in kept:
            index = turned(index, mask)
        return index

    arrivals = {}

    def send_piece(number, kept):
        start, size, split, order = parts[number]
        rest = (side if split else slice(None), slice(None), pl.ds(start, size))
        block = weights.at[(slice(None),) + slot_of(device_of(kept)) + rest]
        after = order.index(kept[-1]) + 1 if kept else 0
        for mask in order[after:]:
            arrivals[number, kept + (mask,)] = copies.start(block, block, along(mask))
        if split and kept:
            forwards.append(copies.start(block, block, {"dp": turned(d_pos, 2)}))

    def receive_piece(number, kept):
        arrivals[number, kept].wait_recv()
        send_piece(number, kept)

    def send_bias(stage):
        block = biases.at[place_of(outer_first, masks[:stage], t_pos)]
        return copies.start(block, block, along(masks[stage]))

    def project(block):
        at = pl.ds(pl.multiple_of(block * rows, rows), rows)
        part = normed[slot(block) + (slice(None), slice(None))]
        position = block * rows + lax.broadcasted_iota(jnp.int32, (rows, wide_span), 0)
        lane = lax.broadcasted_iota(jnp.int32, (rows, wide_span), 1)
        text, visual = counts_ref[0:1, 0:1], counts_ref[1:2, 0:1]
        bound = jnp.where(position >= TEXT_SLOTS, visual + TEXT_SLOTS, text)
        tail = jnp.where((lane > extra) & (lane < extra + 4), 1.0, 0.0)
        tail = jnp.where((lane == extra) & (position >= bound), -1e30, tail)
        q_ref[at, :] = low(low(dot_nn(part, wq_ref[...]) + b_ref[0:1, :]) * scale)
        k_ref[at, :] = low(dot_nn(part, wk_ref[...]) + tail)
        v_ref[at, :] = low(dot_nn(part, wv_ref[...]) + b_ref[1:2, :])

    forwards = []

    def send_own():
        for number in range(len(parts)):
            send_piece(number, ())

    arriving = send_rows(0)
    other_cots = copies.start(cot_ref, cots.at[1], {"dp": turned(d_pos, 1)})
    for stage in range(1, len(inner)):
        if stage == 1 and FRONT_FIRST:
            send_own()
        for copy in arriving:
            copy.wait_recv()
        arriving = send_rows(stage)
    if not (FRONT_FIRST and len(inner) > 1):
        send_own()
    bias_flow = send_bias(0)

    coming = []
    for number in range(len(parts)):
        order = parts[number][3]
        for kept in subsets(order)[1:]:
            coming.append((len(kept), masks.index(kept[-1]), number, kept))
    coming = [(number, kept) for _, _, number, kept in sorted(coming)]
    cuts = [0] + [len(coming) * cut // 21 for cut in FRONT_CUTS] + [len(coming)]

    def receive(wave):
        for number, kept in coming[cuts[wave] : cuts[wave + 1]]:
            receive_piece(number, kept)

    receive(0)
    for copy in arriving:
        copy.wait_recv()

    @pl.loop(0, members)
    def _(block):
        project(block)

    receive(1)
    lanes = lax.broadcasted_iota(jnp.int32, (rows, wide_span), 1)
    unit = low(jnp.where(lanes == extra, 1.0, 0.0))
    side_lanes = lax.broadcasted_iota(jnp.int32, (rows, 128), 1)
    base = copies.used
    copies.used += members
    lane_block = pl.ds(pl.multiple_of(member * wide_span, wide_span), wide_span)

    def att_copy(j, block):
        return copies.make(
            mixed.at[block], att.at[:, lane_block], {"tensor": t_pos - member + block}, base + j
        )

    def attend(j):
        block = xor_member(j)
        at = pl.ds(pl.multiple_of(block * rows, rows), rows)
        query = q_ref[at, :]
        total_mix = jnp.zeros((rows, wide_span), F32)
        logs = jnp.zeros((rows, 128), F32)
        for head in range(heads):
            chosen = head_mask(lanes, head)
            left = jnp.where(chosen, query, unit)
            scores = dot_nt(left, k_ref[...])
            peak = jnp.max(scores, axis=-1, keepdims=True)
            expo = jnp.exp(scores - peak)
            total = jnp.sum(expo, axis=-1, keepdims=True)
            out = dot_nn(low(expo), v_ref[...]) / total
            total_mix = jnp.where(chosen, out, total_mix)
            logs = jnp.where(side_lanes == head, peak + jnp.log(total), logs)
        mixed[block] = low(total_mix)
        l_ref[at, :] = logs

    half_turns = members // 2

    @pl.loop(0, half_turns)
    def _(turn):
        j = members - 1 - turn
        attend(j)
        att_copy(j, xor_member(j)).start()

    receive(2)

    @pl.loop(half_turns, members)
    def _(turn):
        j = members - 1 - turn
        attend(j)

        @pl.when(j > 0)
        def _():
            att_copy(j, xor_member(j)).start()

    own_att = pltpu.make_async_copy(mixed.at[member], att.at[:, lane_block], here.at[0])
    own_att.start()
    for stage in range(1, len(masks)):
        bias_flow.wait_recv()
        bias_flow = send_bias(stage)
    normed_copy = pltpu.make_async_copy(normed, normed_out, here.at[1])
    normed_copy.start()
    other_cots.wait_recv()
    cot_copy = pltpu.make_async_copy(cots, cot_out, here.at[2])
    cot_copy.start()
    own_att.wait()
    for j in range(1, members):
        att_copy(j, xor_member(j)).wait()
    att_copy_out = pltpu.make_async_copy(att, att_out, here.at[3])
    att_copy_out.start()
    receive(3)
    bias_flow.wait_recv()
    bias_copy = pltpu.make_async_copy(biases, bias_out, here.at[4])
    bias_copy.start()
    for copy in forwards:
        copy.wait_recv()
    up_copy = pltpu.make_async_copy(weights.at[0], up_out, here.at[5])
    up_copy.start()
    down_copy = pltpu.make_async_copy(weights.at[1], down_out, here.at[0])
    down_copy.start()
    for copy in (normed_copy, cot_copy, att_copy_out, bias_copy, up_copy, down_copy):
        copy.wait()
    copies.drain()


def front(
    heads, members, tensor_size, blocks, norm, w_q, w_k, w_v, bias, counts, cotangent, piece, up_bias
):
    rows, width = blocks.shape
    wide_span = w_q.shape[1]
    total = members * rows
    inner, outer = len(bits_of(members)), len(bits_of(tensor_size))
    square = jax.ShapeDtypeStruct((total, wide_span), BF)
    normed = jax.ShapeDtypeStruct((2,) * inner + (rows, width), BF)
    att = jax.ShapeDtypeStruct((rows, members * wide_span), BF)
    cots = jax.ShapeDtypeStruct((2, rows, width), BF)
    weights = jax.ShapeDtypeStruct((2,) * outer + piece.shape[1:], BF)
    biases = jax.ShapeDtypeStruct((2,) * outer + up_bias.shape, F32)
    number = front_copies(tensor_size, members, width)
    vmem = pl.BlockSpec(memory_space=pltpu.VMEM)
    away = pl.BlockSpec(memory_space=pl.ANY)
    held = (normed, att, cots, weights, weights, biases)
    return pl.pallas_call(
        functools.partial(front_kernel, heads, members, tensor_size),
        out_shape=(square, square, square, jax.ShapeDtypeStruct((total, 128), F32)) + held,
        in_specs=[vmem] * 10,
        out_specs=(vmem,) * 4 + (away,) * 6,
        scratch_shapes=[
            pltpu.VMEM(normed.shape, BF),
            pltpu.VMEM((members, rows, wide_span), BF),
            pltpu.VMEM(att.shape, BF),
            pltpu.VMEM(cots.shape, BF),
            pltpu.VMEM((2,) + weights.shape, BF),
            pltpu.VMEM(biases.shape, F32),
            pltpu.SemaphoreType.DMA((number,)),
            pltpu.SemaphoreType.DMA((number,)),
            pltpu.SemaphoreType.DMA((6,)),
        ],
        compiler_params=pltpu.CompilerParams(
            vmem_limit_bytes=48 << 20, collective_id=0, has_side_effects=True
        ),
        cost_estimate=pl.CostEstimate(
            flops=20_000_000_000, bytes_accessed=20_000_000, transcendentals=3_000_000
        ),
    )(blocks, norm, w_q, w_k, w_v, bias, counts, cotangent, piece, up_bias)


def back_shapes(members, rows, width, wide_span, span, tensor_size, dp_size, quarter):
    inner, outer = len(bits_of(members)), len(bits_of(tensor_size))
    third = width // PARTS
    half = width // 2
    split_bits = outer + 1
    four = span // 4
    sixteenth = members * span // 16
    shapes = {
        "grad_mixed": ((members, rows, wide_span), BF),
        "grads": ((3, members * rows, wide_span), BF),
        "sum_k": ((members * rows, wide_span), F32),
        "sum_v": ((members * rows, wide_span), F32),
        "rows_part": ((2,) * inner + (rows, width), BF),
        "grad_rows": ((rows, width), F32),
        "whole": ((2, 2, 2, quarter, width), BF),
        "out_full": ((2, 2, 2, 2, sixteenth, width), BF),
        "square": ((3, 2, 2, four, width), BF),
        "square_one": ((3, 2, four, width), BF),
        "square_two": ((3, four, width), BF),
        "square_full": ((3,) + (2,) * inner + (2, 2, four, width), BF),
        "late": ((8, width), F32),
        "early_sum": ((16, width), F32),
        "out_part": ((2, 2, 2, 2, sixteenth, width), BF),
        "heads_sum": ((2, members, 1, wide_span), F32),
    }
    for part in range(PARTS):
        for stage in range(split_bits):
            left = (2,) * (split_bits - 1 - stage)
            shapes[f"hidden{part}_{stage}"] = ((2,) + left + (quarter, third), BF)
        for stage in range(len(bits_of(dp_size)) - 2):
            shapes[f"hidden{part}_more{stage}"] = ((2, quarter, third), BF)
    for part in range(2):
        for stage in range(inner):
            shapes[f"rows{part}_{stage}"] = ((2,) * (inner - 1 - stage) + (rows, half), BF)
    for stage in range(4):
        shapes[f"out{stage}"] = ((2,) * (3 - stage) + (sixteenth, width), BF)
    every = len(bits_of(tensor_size)) + len(bits_of(dp_size))
    for stage in range(every - 4):
        shapes[f"out_more{stage}"] = ((sixteenth, width), BF)
    for stage in range(every - 2 - inner):
        shapes[f"square_more{stage}"] = ((3, four, width), BF)
    for stage in range(every):
        shapes[f"early{stage}"] = ((16, width), F32)
        shapes[f"late{stage}"] = ((8, width), F32)
        shapes[f"heads{stage}"] = ((2, members, 1, wide_span), F32)
    return shapes


def tiles(count):
    if count == 0:
        return [()]
    return [(value,) + rest for value in range(2) for rest in tiles(count - 1)]


def back_kernel(
    heads,
    members,
    tensor_size,
    dp_size,
    names,
    number,
    q_ref,
    k_ref,
    v_ref,
    l_ref,
    datt_ref,
    normed_ref,
    weight_ref,
    down_ref,
    up_ref,
    att_ref,
    branch_ref,
    blocks_ref,
    norm_ref,
    middle_ref,
    hidden_bias_ref,
    early0_ref,
    early1_ref,
    early2_ref,
    early3_ref,
    early4_ref,
    early5_ref,
    blocks_out,
    square_out,
    out_out,
    whole_out,
    early_out,
    late_out,
    heads_out,
    *scratch,
):
    held = dict(zip(names, scratch))
    early_refs = (early0_ref, early1_ref, early2_ref, early3_ref, early4_ref, early5_ref)
    send, recv, here = scratch[len(names):]
    copies = Copies(send, recv)
    t_pos = lax.axis_index("tensor")
    d_pos = lax.axis_index("dp")
    member = t_pos % members
    core, side = bit(d_pos, 1), bit(d_pos, 2)
    total_rows, wide_span = q_ref.shape
    rows, width = blocks_ref.shape
    masks, inner, dp_masks = bits_of(tensor_size), bits_of(members), bits_of(dp_size)
    outer_first, inner_first = masks[::-1], inner[::-1]
    scale = HEAD_DIM ** (-0.5)
    extra = heads * HEAD_DIM
    position = {"tensor": t_pos, "dp": d_pos}
    every = [("dp", mask) for mask in dp_masks] + [("tensor", mask) for mask in masks]
    rest_dp = [("dp", mask) for mask in dp_masks[2:]]
    rest_tensor = [("tensor", mask) for mask in masks[len(inner):]]

    named = {
        "x": ("tensor", masks[0]),
        "z0": ("tensor", masks[1]),
        "z1": ("tensor", masks[2]),
        "y": ("dp", 2),
    }

    def to(move):
        axis, mask = move
        return {axis: turned(position[axis], mask)}

    def mine(move):
        axis, mask = move
        return bit(position[axis], mask)

    def xor_member(j):
        return sum(mask * ((bit(member, mask) + bit(j, mask)) % 2) for mask in inner)

    def slot(index):
        return tuple(bit(index, mask) for mask in inner_first)

    peers = [to(move) for move in every]
    peers += [
        {"tensor": t_pos - member + xor_member(j)} for j in range(1, members) if j not in inner
    ]
    barrier = greet(peers)
    grad_mixed, grads = held["grad_mixed"], held["grads"]
    sum_k, sum_v = held["sum_k"], held["sum_v"]
    own_lanes = pl.ds(pl.multiple_of(member * wide_span, wide_span), wide_span)
    own_copy = pltpu.make_async_copy(datt_ref.at[:, own_lanes], grad_mixed.at[member], here.at[0])
    own_copy.start()
    sum_k[...] = jnp.zeros_like(sum_k)
    sum_v[...] = jnp.zeros_like(sum_v)
    pl.semaphore_wait(barrier, len(peers))

    base = copies.used
    copies.used += members

    def datt_copy(j):
        block = xor_member(j)
        there = pl.ds(pl.multiple_of(block * wide_span, wide_span), wide_span)
        return copies.make(
            datt_ref.at[:, there],
            grad_mixed.at[member],
            {"tensor": t_pos - member + block},
            base + j,
        )

    for j in range(1, members):
        datt_copy(j).start()

    def add(target, at, source, source_at):
        target[at] = low(wide(target[at]) + wide(source[source_at]))

    def hidden_chain(part):
        third = width // PARTS
        columns = pl.ds(part * third, third)
        dims = [("tensor", mask) for mask in outer_first] + [("dp", 2)]
        order = [named[name] for name in HIDDEN_ORDERS[part]]
        order += [("tensor", mask) for mask in masks[3:]]
        full = slice(None)
        current = None
        for stage, move in enumerate(order):
            landing = held[f"hidden{part}_{stage}"]
            where = dims.index(move)
            away = (full,) * where + (1 - mine(move),) + (full,) * (len(dims) - 1 - where)
            sent = []
            if current is None:
                for which, source in enumerate((down_ref, up_ref)):
                    sent.append(
                        copies.start(
                            source.at[away + (full, columns)], landing.at[which], to(move)
                        )
                    )
            else:
                sent.append(copies.start(current.at[(full,) + away], landing, to(move)))
            yield
            for copy in sent:
                copy.wait_recv()
            for tile in tiles(len(dims) - 1):
                kept = tile[:where] + (mine(move),) + tile[where:]
                for which in range(2):
                    if current is None:
                        source = (down_ref, up_ref)[which]
                        add(landing, (which,) + tile, source, kept + (full, columns))
                    else:
                        add(landing, (which,) + tile, current, (which,) + kept)
            current = landing
            dims = dims[:where] + dims[where + 1 :]
        for stage, move in enumerate(rest_dp):
            landing = held[f"hidden{part}_more{stage}"]
            copy = copies.start(current, landing, to(move))
            yield
            copy.wait_recv()
            for which in range(2):
                add(landing, which, current, which)
            current = landing
        whole = held["whole"]
        for which in range(2):
            whole[which, core, side, :, columns] = current[which]
        block = whole.at[:, core, side, :, columns]
        copy = copies.start(block, block, to(("dp", 2)))
        yield
        copy.wait_recv()
        block = whole.at[:, core, :, :, columns]
        copy = copies.start(block, block, to(("dp", 1)))
        yield
        copy.wait_recv()

    def out_chain():
        halvings = [("dp", 1)] + [named[name] for name in OUT_ORDER]
        current = out_part
        for stage, move in enumerate(halvings):
            landing = held[f"out{stage}"]
            copy = copies.start(current.at[1 - mine(move)], landing, to(move))
            yield
            copy.wait_recv()
            for tile in tiles(3 - stage):
                add(landing, tile + (slice(None),), current, (mine(move),) + tile)
            current = landing
        for stage, move in enumerate([move for move in every if move not in halvings]):
            landing = held[f"out_more{stage}"]
            copy = copies.start(current, landing, to(move))
            yield
            copy.wait_recv()
            add(landing, slice(None), current, slice(None))
            current = landing
        out_full = held["out_full"]
        own = tuple(mine(move) for move in halvings)
        out_full[own] = current[...]
        for stage in range(3, -1, -1):
            block = out_full.at[own[: stage + 1]]
            copy = copies.start(block, block, to(halvings[stage]))
            yield
            copy.wait_recv()

    def square_chain():
        square, one, two = held["square"], held["square_one"], held["square_two"]
        copy = copies.start(square.at[:, 1 - core], one, to(("dp", 1)))
        yield
        copy.wait_recv()
        for which in range(3):
            for tile in tiles(1):
                add(one, (which,) + tile, square, (which, core) + tile)
        copy = copies.start(one.at[:, 1 - side], two, to(("dp", 2)))
        yield
        copy.wait_recv()
        for which in range(3):
            add(two, which, one, (which, side))
        current = two
        for stage, move in enumerate(rest_tensor + rest_dp):
            landing = held[f"square_more{stage}"]
            copy = copies.start(current, landing, to(move))
            yield
            copy.wait_recv()
            for which in range(3):
                add(landing, which, current, which)
            current = landing
        full = held["square_full"]
        dims = [("tensor", mask) for mask in inner_first] + [("dp", 1), ("dp", 2)]
        own = tuple(mine(move) for move in dims)
        for which in range(3):
            full[(which,) + own] = current[which]
        moves = [("tensor", mask) for mask in inner] + [("dp", 2)]
        for stage in range(len(moves) + 1):
            sent = []
            for which in range(3):
                turn = which % len(moves)
                order = moves[turn:] + moves[:turn] + [("dp", 1)]
                done = order[:stage]
                at = tuple(slice(None) if move in done else mine(move) for move in dims)
                block = full.at[(which,) + at]
                sent.append(copies.start(block, block, to(order[stage])))
            yield
            for copy in sent:
                copy.wait_recv()

    def rows_chain():
        half = width // 2
        part_ref = held["rows_part"]
        state = []
        for part in range(2):
            state.append([part_ref, list(inner_first), (pl.ds(part * half, half),)])
        orders = (inner, inner[::-1])
        for stage in range(len(inner)):
            sent = []
            for part in range(2):
                current, dims, columns = state[part]
                mask = orders[part][stage]
                where = dims.index(mask)
                away = (slice(None),) * where + (1 - bit(member, mask),)
                away += (slice(None),) * (len(dims) - 1 - where)
                sent.append(
                    copies.start(
                        current.at[away + (slice(None),) + columns],
                        held[f"rows{part}_{stage}"],
                        to(("tensor", mask)),
                    )
                )
            yield
            for part in range(2):
                sent[part].wait_recv()
                current, dims, columns = state[part]
                mask = orders[part][stage]
                where = dims.index(mask)
                landing = held[f"rows{part}_{stage}"]
                for tile in tiles(len(dims) - 1):
                    kept = tile[:where] + (bit(member, mask),) + tile[where:]
                    kept += (slice(None),) + columns
                    if stage < len(inner) - 1:
                        add(landing, tile + (slice(None),), current, kept)
                    else:
                        held["grad_rows"][:, part * half : (part + 1) * half] = wide(
                            landing[...]
                        ) + wide(current[kept])
                state[part] = [landing, dims[:where] + dims[where + 1 :], ()]

    def small_chain(pairs):
        for stage, move in enumerate(every):
            sent = []
            for first, name, _ in pairs:
                source = first if stage == 0 else held[f"{name}{stage - 1}"]
                sent.append(copies.start(source, held[f"{name}{stage}"], to(move)))
            yield
            for copy, (first, name, result) in zip(sent, pairs):
                copy.wait_recv()
                source = first if stage == 0 else held[f"{name}{stage - 1}"]
                value = held[f"{name}{stage}"][...] + source[...]
                if stage == len(every) - 1:
                    result[...] = value
                else:
                    held[f"{name}{stage}"][...] = value

    chains = {
        "out": out_chain(),
        "early": small_chain([(held["early_sum"], "early", early_out)]),
        "rows": rows_chain(),
        "square": square_chain(),
        "late": small_chain(
            [(held["late"], "late", late_out), (held["heads_sum"], "heads", heads_out)]
        ),
    }
    for part in range(PARTS):
        chains[f"h{part}"] = hidden_chain(part)
    live = list(chains)

    def go(*wanted):
        for name in wanted:
            if name in live:
                if next(chains[name], True):
                    live.remove(name)

    span = heads * HEAD_DIM
    unit_rows = span // 4
    out_part = held["out_part"]
    for index in range(members):
        full = dot_tn(att_ref[:, index * wide_span : (index + 1) * wide_span], branch_ref[...])
        for quarter_index in range(4):
            at = index * 4 + quarter_index
            where = tuple((at * 16 // (members * 4)) // step % 2 for step in (8, 4, 2, 1))
            inner_row = (at * unit_rows) % out_part.shape[4]
            out_part[where + (slice(inner_row, inner_row + unit_rows), slice(None))] = low(
                full[quarter_index * unit_rows : (quarter_index + 1) * unit_rows]
            )
    early = held["early_sum"]
    early[...] = jnp.zeros_like(early)
    for index, row in enumerate(early_refs):
        early[index : index + 1, :] = row[...]
    early[6 : 6 + hidden_bias_ref.shape[0], :] = hidden_bias_ref[...]
    own_copy.wait()
    lanes = lax.broadcasted_iota(jnp.int32, (rows, wide_span), 1)

    def attend(block):
        at = pl.ds(pl.multiple_of(block * rows, rows), rows)
        query = q_ref[at, :]
        grad = grad_mixed[block]
        grad_q = jnp.zeros((rows, wide_span), F32)
        for head in range(heads):
            chosen = head_mask(lanes, head)
            log_total = l_ref[at, head : head + 1]
            high = low(log_total)
            rest = log_total - wide(high)
            middle = low(rest)
            last = low(rest - wide(middle))
            fill = jnp.where(lanes == extra, 1.0, 0.0)
            fill = jnp.where(lanes == extra + 1, -wide(high), fill)
            fill = jnp.where(lanes == extra + 2, -wide(middle), fill)
            fill = jnp.where(lanes == extra + 3, -wide(last), fill)
            left = jnp.where(chosen, query, low(fill))
            upstream = jnp.where(chosen, grad, jnp.zeros_like(grad))
            probs = jnp.exp(dot_nt(k_ref[...], left))
            grad_probs = dot_nt(v_ref[...], upstream)
            centred = jnp.sum(probs * grad_probs, axis=0, keepdims=True)
            grad_scores = low(probs * (grad_probs - centred))
            sum_k[...] += dot_nn(grad_scores, left)
            sum_v[...] += dot_nn(low(probs), upstream)
            out = dot_tn(grad_scores, k_ref[...]) * scale
            grad_q = jnp.where(chosen, out, grad_q)
        grads[0, at, :] = low(grad_q)

    def block(index):
        count = members // 2

        @pl.loop(index * count, (index + 1) * count)
        def _(j):
            @pl.when(j > 0)
            def _():
                datt_copy(j).wait_recv()

            attend(xor_member(j))

    def finish_attention():
        keep = lanes < extra

        @pl.loop(0, members)
        def _(block):
            at = pl.ds(pl.multiple_of(block * rows, rows), rows)
            grads[1, at, :] = low(jnp.where(keep, sum_k[at, :], 0.0))
            grads[2, at, :] = low(sum_v[at, :])

    def compute_rows():
        @pl.loop(0, members)
        def _(block):
            at = pl.ds(pl.multiple_of(block * rows, rows), rows)
            part = dot_nt(grads[0, at, :], weight_ref[0])
            part += dot_nt(grads[1, at, :], weight_ref[1])
            part += dot_nt(grads[2, at, :], weight_ref[2])
            held["rows_part"][slot(block) + (slice(None), slice(None))] = low(part)

    def compute_square():
        four = held["square"].shape[3]

        @pl.loop(0, 3)
        def _(which):
            full = dot_tn(grads[which], normed_ref[...])
            for tile in tiles(2):
                start = (tile[0] * 2 + tile[1]) * four
                held["square"][(which,) + tile] = low(full[start : start + four])

        heads_sum = held["heads_sum"]
        heads_sum[...] = jnp.zeros_like(heads_sum)
        heads_sum[0, member] = jnp.sum(wide(grads[0]), axis=0, keepdims=True)
        heads_sum[1, member] = jnp.sum(wide(grads[2]), axis=0, keepdims=True)

    def compute_norm():
        while "rows" in live:
            go("rows")
        gain = norm_ref[0:1, :]
        gain_sum = jnp.zeros((1, width), F32)
        shift_sum = jnp.zeros((1, width), F32)
        step = rows // 2
        for start in range(0, rows, step):
            at = pl.ds(start, step)
            grad = held["grad_rows"][at, :]
            values = wide(blocks_ref[at, :])
            centre = values - jnp.mean(values, axis=-1, keepdims=True)
            spread = jnp.mean(centre * centre, axis=-1, keepdims=True)
            factor = lax.rsqrt(spread + EPSILON)
            unit = centre * factor
            scaled = grad * gain
            pulled = scaled - jnp.mean(scaled, axis=-1, keepdims=True)
            pulled = pulled - unit * jnp.mean(scaled * unit, axis=-1, keepdims=True)
            blocks_out[at, :] = middle_ref[at, :] + factor * pulled
            gain_sum += jnp.sum(grad * unit, axis=0, keepdims=True)
            shift_sum += jnp.sum(grad, axis=0, keepdims=True)
        late = held["late"]
        late[...] = jnp.zeros_like(late)
        late[0:1, :] = gain_sum
        late[1:2, :] = shift_sum

    for token in sum(BACK_PROGRAM, ()):
        if token.startswith("*block"):
            block(int(token[6:]))
            if token == "*block1":
                finish_attention()
        elif token == "*rows":
            compute_rows()
        elif token == "*square":
            compute_square()
        elif token == "*norm":
            compute_norm()
        else:
            go(token)
    while live:
        go(*list(live))
    finals = []
    for index, (name, target) in enumerate(
        (("square_full", square_out), ("out_full", out_out), ("whole", whole_out))
    ):
        copy = pltpu.make_async_copy(held[name], target, here.at[index])
        copy.start()
        finals.append(copy)
    for copy in finals:
        copy.wait()
    for j in range(1, members):
        datt_copy(j).wait_send()
    copies.drain()


def back(
    heads,
    members,
    tensor_size,
    dp_size,
    span,
    quarter,
    queries,
    keys,
    values,
    logs,
    datt,
    normed,
    weights,
    grad_down,
    grad_up,
    attended,
    grad_branch,
    blocks,
    norm,
    middle,
    hidden_bias,
    early,
):
    rows, width = blocks.shape
    wide_span = queries.shape[1]
    shapes = back_shapes(members, rows, width, wide_span, span, tensor_size, dp_size, quarter)
    names = list(shapes)
    outer, inner = len(bits_of(tensor_size)), len(bits_of(members))
    every = outer + len(bits_of(dp_size))
    number = members + PARTS * (outer + 1 + 1 + 2 + len(bits_of(dp_size))) + every + 8
    number += 2 + every + 3 * (inner + 2) + 2 * inner + 3 * every
    vmem = pl.BlockSpec(memory_space=pltpu.VMEM)
    away = pl.BlockSpec(memory_space=pl.ANY)

    def shape_of(name):
        return jax.ShapeDtypeStruct(*shapes[name])

    return pl.pallas_call(
        functools.partial(back_kernel, heads, members, tensor_size, dp_size, names, number),
        out_shape=(
            jax.ShapeDtypeStruct((rows, width), F32),
            shape_of("square_full"),
            shape_of("out_full"),
            shape_of("whole"),
            jax.ShapeDtypeStruct((16, width), F32),
            shape_of("late"),
            shape_of("heads_sum"),
        ),
        in_specs=[vmem] * 21,
        out_specs=(vmem,) + (away,) * 3 + (vmem,) * 3,
        scratch_shapes=[pltpu.VMEM(*shapes[name]) for name in names]
        + [
            pltpu.SemaphoreType.DMA((number,)),
            pltpu.SemaphoreType.DMA((number,)),
            pltpu.SemaphoreType.DMA((3,)),
        ],
        compiler_params=pltpu.CompilerParams(
            vmem_limit_bytes=60 << 20, collective_id=1, has_side_effects=True
        ),
        cost_estimate=pl.CostEstimate(
            flops=40_000_000_000, bytes_accessed=40_000_000, transcendentals=3_000_000
        ),
    )(
        queries,
        keys,
        values,
        logs,
        datt,
        normed,
        weights,
        grad_down,
        grad_up,
        attended,
        grad_branch,
        blocks,
        norm,
        middle,
        hidden_bias,
        *early,
    )


def local(
    blocks,
    counts,
    cotangent,
    w_query,
    w_key,
    w_value,
    w_out,
    b_query,
    b_value,
    b_out,
    norm1_gain,
    norm1_bias,
    norm2_gain,
    norm2_bias,
    gate_logits,
    w_up,
    b_up,
    w_down,
    b_down,
):
    rows, width = blocks.shape
    tensor_size = lax.axis_size("tensor")
    dp_size = lax.axis_size("dp")
    t_pos = lax.axis_index("tensor")
    d_pos = lax.axis_index("dp")
    members = SEQ // rows
    member = t_pos % members
    per_head = -(-HEADS // members)
    span = per_head * HEAD_DIM
    ring = 4
    line = tensor_size // ring
    z_pos = t_pos // line
    x_pos = t_pos % line
    core = d_pos % 2
    side = (d_pos // 2) % 2
    shard = w_up.shape[1]
    quarter = shard // 4
    hidden_total = shard * tensor_size
    dp_rest = [("dp", mask) for mask in bits_of(dp_size)[2:]]
    member_masks = bits_of(members)
    tensor_rest = [("tensor", mask) for mask in bits_of(tensor_size)[len(member_masks):]]

    def z_shift(value, step):
        pairs = [
            (i, ((i // line + step) % ring) * line + i % line) for i in range(tensor_size)
        ]
        return lax.ppermute(value, "tensor", pairs)

    def x_shift(value, step):
        pairs = [
            (i, (i // line) * line + (i % line + step) % line) for i in range(tensor_size)
        ]
        return lax.ppermute(value, "tensor", pairs)

    gain_one = wide(norm1_gain)
    shift_one = wide(norm1_bias)
    gain_two = wide(norm2_gain)
    shift_two = wide(norm2_bias)
    logits_gate = wide(gate_logits)
    inputs = wide(blocks)

    doc_counts = pick(counts, t_pos // members)
    slot_ids = member ^ jnp.arange(members, dtype=jnp.int32)
    own_pos = member * rows + jnp.arange(rows, dtype=jnp.int32)
    visual = own_pos >= TEXT_SLOTS

    def head_part(weight):
        extra = per_head * HEAD_DIM * members - width
        if extra:
            weight = jnp.pad(weight, ((0, 0),) * (weight.ndim - 1) + ((0, extra),))
        return lax.dynamic_slice_in_dim(weight, member * span, span, weight.ndim - 1)

    wide_span = -(-(span + 4) // 128) * 128

    def widen(array):
        return jnp.pad(array, ((0, 0),) * (array.ndim - 1) + ((0, wide_span - array.shape[-1]),))

    w_q = widen(head_part(w_query))
    w_k = widen(head_part(w_key))
    w_v = widen(head_part(w_value))
    bias = wide(jnp.stack([widen(head_part(b_query)), widen(head_part(b_value))], 0))
    halves = (2, 2, quarter, width)
    piece = jnp.stack(
        [pick(w_up.T.reshape(halves), core), pick(w_down.reshape(halves), core)], 0
    )
    queries, keys, values, logs, normed_all, attended, cot_all, up_t, down, biases = front(
        per_head,
        members,
        tensor_size,
        blocks,
        jnp.stack([gain_one, shift_one], 0),
        w_q,
        w_k,
        w_v,
        bias,
        jnp.broadcast_to(doc_counts[:, None], (2, 128)),
        cotangent,
        piece,
        wide(b_up)[None, :],
    )
    normed_all = normed_all.reshape(SEQ, width)
    cot_all = cot_all.reshape(2 * rows, width)
    up_t = up_t.reshape(-1, width)
    down = down.reshape(-1, width)
    biases = biases.reshape(tensor_size, shard)
    biases = lax.dynamic_slice_in_dim(biases, core * (2 * quarter), 2 * quarter, 1).reshape(-1)
    extra_rows = members * span - width
    out_rows = jnp.pad(w_out, ((0, extra_rows), (0, 0))) if extra_rows else w_out
    out_rows = jnp.pad(out_rows.reshape(members, span, width), ((0, 0), (0, wide_span - span), (0, 0)))
    out_rows = out_rows.reshape(members * wide_span, width)

    branch = dot_nn(attended, out_rows) + wide(b_out)
    gate = jax.nn.sigmoid(
        jnp.where(visual[:, None], logits_gate[1][None, :], logits_gate[0][None, :])
    )
    middle = inputs + gate * branch
    second = low(normalize(middle, gain_two, shift_two))
    second_all = jnp.concatenate([second, flip(second, "dp", 1)], 0)

    pre = dot_nt(second_all, up_t) + biases
    hidden = low(gelu_exact(pre))
    grad_down = low(dot_tn(hidden, cot_all))
    spread = dot_nt(cot_all, down)
    dpre = low(gelu_grad(pre, spread))
    grad_second = dot_nn(dpre[:rows], up_t) + flip(dot_nn(dpre[rows:], up_t), "dp", 1)
    lowered = dot_nn(hidden[:rows], down) + flip(dot_nn(hidden[rows:], down), "dp", 1)
    grad_up = low(dot_tn(dpre, second_all))
    grad_up_bias = jnp.sum(wide(dpre), axis=0)
    joined = low(middle + lowered + wide(b_down))

    upstream = wide(cotangent)
    pull_two = jax.vjp(normalize, middle, gain_two, shift_two)[1]
    grad_middle_norm, grad_gain_two, grad_shift_two = pull_two(grad_second)
    grad_middle = upstream + grad_middle_norm
    grad_branch = low(gate * grad_middle)
    gate_term = grad_middle * branch * gate * (1.0 - gate)
    grad_gate = [
        jnp.sum(jnp.where(visual[:, None], 0.0, gate_term), axis=0),
        jnp.sum(jnp.where(visual[:, None], gate_term, 0.0), axis=0),
    ]
    grad_out_bias = jnp.sum(wide(grad_branch), axis=0)
    grad_attended = low(dot_nt(grad_branch, out_rows))
    bias_sum = grad_up_bias.reshape(tensor_size, 1, 2 * quarter)
    both = jnp.arange(2, dtype=jnp.int32)[None, :, None]
    bias_sum = jnp.where(both == core, bias_sum, 0.0).reshape(hidden_total // width, width)
    early = [grad_out_bias, grad_gain_two, grad_shift_two, jnp.sum(upstream, axis=0)] + grad_gate
    early = [row[None, :] for row in early]
    hidden_shape = (2,) * len(bits_of(tensor_size)) + (2, quarter, width)
    grad_blocks, squares, outs, wholes, early, late, head_sums = back(
        per_head,
        members,
        tensor_size,
        dp_size,
        span,
        quarter,
        queries,
        keys,
        values,
        logs,
        grad_attended,
        normed_all,
        jnp.stack([w_q, w_k, w_v], 0),
        grad_down.reshape(hidden_shape),
        grad_up.reshape(hidden_shape),
        attended,
        grad_branch,
        blocks,
        jnp.stack([gain_one, shift_one], 0),
        grad_middle,
        bias_sum,
        early,
    )
    squares = squares.reshape(3, members * span, width)[:, :width]
    outs = outs.reshape(members * span, width)[:width]
    wholes = wholes.reshape(2, shard, width)
    head_sums = head_sums.reshape(2, members, wide_span)[:, :, :span]
    head_sums = head_sums.reshape(2, members * span)[:, :width]
    bias_out = lax.dynamic_slice_in_dim(
        early[6 : 6 + hidden_total // width].reshape(hidden_total), t_pos * shard, shard, 0
    )
    return (
        joined,
        grad_blocks,
        wide(squares[0].T),
        wide(squares[1].T),
        wide(squares[2].T),
        wide(outs),
        head_sums[0],
        head_sums[1],
        early[0],
        late[0],
        late[1],
        early[1],
        early[2],
        early[4:6],
        wide(wholes[1].T),
        bias_out,
        wide(wholes[0]),
        early[3],
    )


def solution(mesh):
    rows = P(("dp", "tensor"), None)
    in_specs = (rows, P("dp", None), rows) + (P(),) * 12 + (
        P(None, "tensor"),
        P("tensor"),
        P("tensor", None),
        P(),
    )
    out_specs = (rows, rows) + (P(),) * 12 + (
        P(None, "tensor"),
        P("tensor"),
        P("tensor", None),
        P(),
    )
    return jax.shard_map(local, mesh=mesh, in_specs=in_specs, out_specs=out_specs, check_vma=False)
```

```python
import functools

import jax
import jax.numpy as jnp
from jax import lax
from jax.experimental import pallas as pl
from jax.experimental.pallas import tpu as pltpu
from jax.sharding import PartitionSpec as P

HEADS = 12
HEAD_DIM = 64
TEXT_SLOTS = 896
SEQ = 1024
EPSILON = 1e-05
PARTS = 3
HIDDEN_ORDERS = (("x", "y", "z1", "z0"), ("z0", "y", "x", "z1"), ("y", "x", "z0", "z1"))
OUT_ORDER = ("x", "y", "z0")
BACK_PROGRAM = (
    ("out", "h2", "h1", "*block0", "out", "h0", "*block1", "out", "*square", "square", "out"),
    ("*rows", "rows", "early", "h2", "out", "early", "square", "early", "h0", "square", "h1"),
    ("rows", "out", "h0", "early", "square", "h2", "out", "h1", "rows", "early", "*norm", "late"),
    ("square", "late", "out", "h1", "h0", "h2", "late", "early", "square", "h0", "out", "late"),
    ("h1", "out", "h2", "h0", "h0", "h1", "square", "late", "h1", "h2", "square", "h2"),
)
FRONT_CUTS = (16, 18, 19)
FRONT_FIRST = True
BF = jnp.bfloat16
TENSOR = "tensor"
DP = "dp"
F32 = jnp.float32


def normalize(values, gain, shift):
    centre = values - jnp.mean(values, axis=-1, keepdims=True)
    spread = jnp.mean(centre * centre, axis=-1, keepdims=True)
    return centre * lax.rsqrt(spread + EPSILON) * gain + shift


def gelu_exact(values):
    return jax.nn.gelu(values, approximate=False)


def gelu_grad(values, upstream):
    return jax.vjp(gelu_exact, values)[1](upstream)[0]


def dot_nn(left, right):
    return lax.dot_general(left, right, (((1,), (0,)), ((), ())), preferred_element_type=F32)


def dot_tn(left, right):
    return lax.dot_general(left, right, (((0,), (0,)), ((), ())), preferred_element_type=F32)


def dot_nt(left, right):
    return lax.dot_general(left, right, (((1,), (1,)), ((), ())), preferred_element_type=F32)


def pick(array, index):
    return lax.dynamic_index_in_dim(array, index, 0, keepdims=False)


def low(value):
    return value.astype(BF)


def wide(value):
    return value.astype(F32)


def flip(value, axis, mask):
    size = lax.axis_size(axis)
    return lax.ppermute(value, axis, [(i, i ^ mask) for i in range(size)])


def bits_of(size):
    found = []
    mask = 1
    while mask < size:
        found.append(mask)
        mask *= 2
    return found


def sum_everywhere(value):
    for axis in (DP, TENSOR):
        for mask in bits_of(lax.axis_size(axis)):
            value = value + flip(value, axis, mask)
    return value


def exchange_sum(value, stages):
    for axis, mask in stages:
        sent = low(value)
        value = wide(sent) + wide(flip(sent, axis, mask))
    return value


def head_mask(lanes, head):
    return (lanes >= head * HEAD_DIM) & (lanes < (head + 1) * HEAD_DIM)


def bit(index, mask):
    return (index // mask) % 2


def turned(index, mask):
    return index + mask - 2 * mask * bit(index, mask)


def place_of(masks, gathered, index):
    return tuple(slice(None) if mask in gathered else bit(index, mask) for mask in masks)


class Copies:
    def __init__(self, send, recv):
        self.send, self.recv, self.used, self.open = send, recv, 0, []

    def make(self, source, target, device, at=None):
        if at is None:
            at = self.used
            self.used += 1
        return pltpu.make_async_remote_copy(
            src_ref=source,
            dst_ref=target,
            send_sem=self.send.at[at],
            recv_sem=self.recv.at[at],
            device_id=device,
            device_id_type=pl.DeviceIdType.MESH,
        )

    def start(self, source, target, device):
        copy = self.make(source, target, device)
        copy.start()
        self.open.append(copy)
        return copy

    def drain(self):
        for copy in self.open:
            copy.wait_send()
        self.open = []


def greet(devices):
    barrier = pltpu.get_barrier_semaphore()
    for device in devices:
        pl.semaphore_signal(
            barrier, inc=1, device_id=device, device_id_type=pl.DeviceIdType.MESH
        )
    return barrier


def weight_parts(tensor_masks, width):
    unit = width // 6
    low_masks, high = tensor_masks[:2], tensor_masks[2:][::-1]
    one, other = high + low_masks, high + low_masks[::-1]
    return (
        (0, 2 * unit, True, other),
        (2 * unit, 2 * unit, True, other),
        (4 * unit, unit, True, one),
        (5 * unit, unit, False, one),
    )


def subsets(masks):
    found = [()]
    for mask in masks:
        found += [kept + (mask,) for kept in found]
    return found


def front_copies(tensor_size, members, width):
    masks, inner = bits_of(tensor_size), bits_of(members)
    parts = weight_parts(masks, width)
    forwards = sum(1 for part in parts if part[2])
    pieces = tensor_size - 1
    return 2 * len(inner) + pieces * (len(parts) + forwards) + len(masks) + 1 + members


def front_kernel(
    heads,
    members,
    tensor_size,
    blocks_ref,
    norm_ref,
    wq_ref,
    wk_ref,
    wv_ref,
    b_ref,
    counts_ref,
    cot_ref,
    piece_ref,
    up_bias_ref,
    q_ref,
    k_ref,
    v_ref,
    l_ref,
    normed_out,
    att_out,
    cot_out,
    up_out,
    down_out,
    bias_out,
    normed,
    mixed,
    att,
    cots,
    weights,
    biases,
    send,
    recv,
    here,
):
    t_pos = lax.axis_index(TENSOR)
    d_pos = lax.axis_index(DP)
    member = t_pos % members
    side = bit(d_pos, 2)
    rows, width = blocks_ref.shape
    wide_span = q_ref.shape[1]
    masks, inner = bits_of(tensor_size), bits_of(members)
    outer_first, inner_first = masks[::-1], inner[::-1]
    scale = HEAD_DIM ** (-0.5)
    extra = heads * HEAD_DIM
    copies = Copies(send, recv)

    def along(mask):
        return {TENSOR: turned(t_pos, mask)}

    def slot(index):
        return tuple(bit(index, mask) for mask in inner_first)

    def slot_of(index):
        return tuple(bit(index, mask) for mask in outer_first)

    diagonals = [j for j in range(1, members) if j not in inner]

    def xor_member(j):
        return sum(mask * ((bit(member, mask) + bit(j, mask)) % 2) for mask in inner)

    peers = [along(mask) for mask in masks]
    peers += [{TENSOR: t_pos - member + xor_member(j)} for j in diagonals]
    peers += [{DP: turned(d_pos, 1)}, {DP: turned(d_pos, 2)}]
    barrier = greet(peers)

    own = place_of(outer_first, (), t_pos)
    local = [
        pltpu.make_async_copy(piece_ref, weights.at[(slice(None),) + own], here.at[0]),
        pltpu.make_async_copy(cot_ref, cots.at[0], here.at[1]),
        pltpu.make_async_copy(up_bias_ref, biases.at[own], here.at[2]),
    ]
    for copy in local:
        copy.start()
    mine = slot(member)
    step = rows // 2
    for start in range(0, rows, step):
        at = pl.ds(start, step)
        normed[mine + (at, slice(None))] = low(
            normalize(wide(blocks_ref[at, :]), norm_ref[0:1, :], norm_ref[1:2, :])
        )
    for copy in local:
        copy.wait()
    pl.semaphore_wait(barrier, len(peers))

    half = width // 2
    halves = ((pl.ds(0, half), inner), (pl.ds(half, half), inner[::-1]))

    def send_rows(stage):
        sent = []
        for columns, order in halves:
            block = normed.at[place_of(inner_first, order[:stage], member) + (slice(None), columns)]
            sent.append(copies.start(block, block, along(order[stage])))
        return sent

    parts = weight_parts(masks, width)

    def device_of(kept):
        index = t_pos
        for mask in kept:
            index = turned(index, mask)
        return index

    arrivals = {}

    def send_piece(number, kept):
        start, size, split, order = parts[number]
        rest = (side if split else slice(None), slice(None), pl.ds(start, size))
        block = weights.at[(slice(None),) + slot_of(device_of(kept)) + rest]
        after = order.index(kept[-1]) + 1 if kept else 0
        for mask in order[after:]:
            arrivals[number, kept + (mask,)] = copies.start(block, block, along(mask))
        if split and kept:
            forwards.append(copies.start(block, block, {DP: turned(d_pos, 2)}))

    def receive_piece(number, kept):
        arrivals[number, kept].wait_recv()
        send_piece(number, kept)

    def send_bias(stage):
        block = biases.at[place_of(outer_first, masks[:stage], t_pos)]
        return copies.start(block, block, along(masks[stage]))

    def project(block):
        at = pl.ds(pl.multiple_of(block * rows, rows), rows)
        part = normed[slot(block) + (slice(None), slice(None))]
        position = block * rows + lax.broadcasted_iota(jnp.int32, (rows, wide_span), 0)
        lane = lax.broadcasted_iota(jnp.int32, (rows, wide_span), 1)
        text, visual = counts_ref[0:1, 0:1], counts_ref[1:2, 0:1]
        bound = jnp.where(position >= TEXT_SLOTS, visual + TEXT_SLOTS, text)
        tail = jnp.where((lane > extra) & (lane < extra + 4), 1.0, 0.0)
        tail = jnp.where((lane == extra) & (position >= bound), -1e30, tail)
        q_ref[at, :] = low(low(dot_nn(part, wq_ref[...]) + b_ref[0:1, :]) * scale)
        k_ref[at, :] = low(dot_nn(part, wk_ref[...]) + tail)
        v_ref[at, :] = low(dot_nn(part, wv_ref[...]) + b_ref[1:2, :])

    forwards = []

    def send_own():
        for number in range(len(parts)):
            send_piece(number, ())

    arriving = send_rows(0)
    other_cots = copies.start(cot_ref, cots.at[1], {DP: turned(d_pos, 1)})
    for stage in range(1, len(inner)):
        if stage == 1 and FRONT_FIRST:
            send_own()
        for copy in arriving:
            copy.wait_recv()
        arriving = send_rows(stage)
    if not (FRONT_FIRST and len(inner) > 1):
        send_own()
    bias_flow = send_bias(0)

    coming = []
    for number in range(len(parts)):
        order = parts[number][3]
        for kept in subsets(order)[1:]:
            coming.append((len(kept), masks.index(kept[-1]), number, kept))
    coming = [(number, kept) for _, _, number, kept in sorted(coming)]
    cuts = [0] + [len(coming) * cut // 21 for cut in FRONT_CUTS] + [len(coming)]

    def receive(wave):
        for number, kept in coming[cuts[wave] : cuts[wave + 1]]:
            receive_piece(number, kept)

    receive(0)
    for copy in arriving:
        copy.wait_recv()

    @pl.loop(0, members)
    def _(block):
        project(block)

    receive(1)
    lanes = lax.broadcasted_iota(jnp.int32, (rows, wide_span), 1)
    unit = low(jnp.where(lanes == extra, 1.0, 0.0))
    side_lanes = lax.broadcasted_iota(jnp.int32, (rows, 128), 1)
    base = copies.used
    copies.used += members
    lane_block = pl.ds(pl.multiple_of(member * wide_span, wide_span), wide_span)

    def att_copy(j, block):
        return copies.make(
            mixed.at[block], att.at[:, lane_block], {TENSOR: t_pos - member + block}, base + j
        )

    def attend(j):
        block = xor_member(j)
        at = pl.ds(pl.multiple_of(block * rows, rows), rows)
        query = q_ref[at, :]
        total_mix = jnp.zeros((rows, wide_span), F32)
        logs = jnp.zeros((rows, 128), F32)
        for head in range(heads):
            chosen = head_mask(lanes, head)
            left = jnp.where(chosen, query, unit)
            scores = dot_nt(left, k_ref[...])
            peak = jnp.max(scores, axis=-1, keepdims=True)
            expo = jnp.exp(scores - peak)
            total = jnp.sum(expo, axis=-1, keepdims=True)
            out = dot_nn(low(expo), v_ref[...]) / total
            total_mix = jnp.where(chosen, out, total_mix)
            logs = jnp.where(side_lanes == head, peak + jnp.log(total), logs)
        mixed[block] = low(total_mix)
        l_ref[at, :] = logs

    half_turns = members // 2

    @pl.loop(0, half_turns)
    def _(turn):
        j = members - 1 - turn
        attend(j)
        att_copy(j, xor_member(j)).start()

    receive(2)

    @pl.loop(half_turns, members)
    def _(turn):
        j = members - 1 - turn
        attend(j)

        @pl.when(j > 0)
        def _():
            att_copy(j, xor_member(j)).start()

    own_att = pltpu.make_async_copy(mixed.at[member], att.at[:, lane_block], here.at[0])
    own_att.start()
    for stage in range(1, len(masks)):
        bias_flow.wait_recv()
        bias_flow = send_bias(stage)
    normed_copy = pltpu.make_async_copy(normed, normed_out, here.at[1])
    normed_copy.start()
    other_cots.wait_recv()
    cot_copy = pltpu.make_async_copy(cots, cot_out, here.at[2])
    cot_copy.start()
    own_att.wait()
    for j in range(1, members):
        att_copy(j, xor_member(j)).wait()
    att_copy_out = pltpu.make_async_copy(att, att_out, here.at[3])
    att_copy_out.start()
    receive(3)
    bias_flow.wait_recv()
    bias_copy = pltpu.make_async_copy(biases, bias_out, here.at[4])
    bias_copy.start()
    for copy in forwards:
        copy.wait_recv()
    up_copy = pltpu.make_async_copy(weights.at[0], up_out, here.at[5])
    up_copy.start()
    down_copy = pltpu.make_async_copy(weights.at[1], down_out, here.at[0])
    down_copy.start()
    for copy in (normed_copy, cot_copy, att_copy_out, bias_copy, up_copy, down_copy):
        copy.wait()
    copies.drain()


def front(
    heads, members, tensor_size, blocks, norm, w_q, w_k, w_v, bias, counts, cotangent, piece, up_bias
):
    rows, width = blocks.shape
    wide_span = w_q.shape[1]
    total = members * rows
    inner, outer = len(bits_of(members)), len(bits_of(tensor_size))
    square = jax.ShapeDtypeStruct((total, wide_span), BF)
    normed = jax.ShapeDtypeStruct((2,) * inner + (rows, width), BF)
    att = jax.ShapeDtypeStruct((rows, members * wide_span), BF)
    cots = jax.ShapeDtypeStruct((2, rows, width), BF)
    weights = jax.ShapeDtypeStruct((2,) * outer + piece.shape[1:], BF)
    biases = jax.ShapeDtypeStruct((2,) * outer + up_bias.shape, F32)
    number = front_copies(tensor_size, members, width)
    vmem = pl.BlockSpec(memory_space=pltpu.VMEM)
    away = pl.BlockSpec(memory_space=pl.ANY)
    held = (normed, att, cots, weights, weights, biases)
    return pl.pallas_call(
        functools.partial(front_kernel, heads, members, tensor_size),
        out_shape=(square, square, square, jax.ShapeDtypeStruct((total, 128), F32)) + held,
        in_specs=[vmem] * 10,
        out_specs=(vmem,) * 4 + (away,) * 6,
        scratch_shapes=[
            pltpu.VMEM(normed.shape, BF),
            pltpu.VMEM((members, rows, wide_span), BF),
            pltpu.VMEM(att.shape, BF),
            pltpu.VMEM(cots.shape, BF),
            pltpu.VMEM((2,) + weights.shape, BF),
            pltpu.VMEM(biases.shape, F32),
            pltpu.SemaphoreType.DMA((number,)),
            pltpu.SemaphoreType.DMA((number,)),
            pltpu.SemaphoreType.DMA((6,)),
        ],
        compiler_params=pltpu.CompilerParams(
            vmem_limit_bytes=48 << 20, collective_id=0, has_side_effects=True
        ),
        cost_estimate=pl.CostEstimate(
            flops=20_000_000_000, bytes_accessed=20_000_000, transcendentals=3_000_000
        ),
    )(blocks, norm, w_q, w_k, w_v, bias, counts, cotangent, piece, up_bias)


def back_shapes(members, rows, width, wide_span, span, tensor_size, dp_size, quarter):
    inner, outer = len(bits_of(members)), len(bits_of(tensor_size))
    third = width // PARTS
    half = width // 2
    split_bits = outer + 1
    four = span // 4
    sixteenth = members * span // 16
    shapes = {
        "grad_mixed": ((members, rows, wide_span), BF),
        "grads": ((3, members * rows, wide_span), BF),
        "sum_k": ((members * rows, wide_span), F32),
        "sum_v": ((members * rows, wide_span), F32),
        "rows_part": ((2,) * inner + (rows, width), BF),
        "grad_rows": ((rows, width), F32),
        "whole": ((2, 2, 2, quarter, width), BF),
        "out_full": ((2, 2, 2, 2, sixteenth, width), BF),
        "square": ((3, 2, 2, four, width), BF),
        "square_one": ((3, 2, four, width), BF),
        "square_two": ((3, four, width), BF),
        "square_full": ((3,) + (2,) * inner + (2, 2, four, width), BF),
        "late": ((8, width), F32),
        "early_sum": ((16, width), F32),
        "out_part": ((2, 2, 2, 2, sixteenth, width), BF),
        "heads_sum": ((2, members, 1, wide_span), F32),
    }
    for part in range(PARTS):
        for stage in range(split_bits):
            left = (2,) * (split_bits - 1 - stage)
            shapes[f"hidden{part}_{stage}"] = ((2,) + left + (quarter, third), BF)
        for stage in range(len(bits_of(dp_size)) - 2):
            shapes[f"hidden{part}_more{stage}"] = ((2, quarter, third), BF)
    for part in range(2):
        for stage in range(inner):
            shapes[f"rows{part}_{stage}"] = ((2,) * (inner - 1 - stage) + (rows, half), BF)
    for stage in range(4):
        shapes[f"out{stage}"] = ((2,) * (3 - stage) + (sixteenth, width), BF)
    every = len(bits_of(tensor_size)) + len(bits_of(dp_size))
    for stage in range(every - 4):
        shapes[f"out_more{stage}"] = ((sixteenth, width), BF)
    for stage in range(every - 2 - inner):
        shapes[f"square_more{stage}"] = ((3, four, width), BF)
    for stage in range(every):
        shapes[f"early{stage}"] = ((16, width), F32)
        shapes[f"late{stage}"] = ((8, width), F32)
        shapes[f"heads{stage}"] = ((2, members, 1, wide_span), F32)
    return shapes


def tiles(count):
    if count == 0:
        return [()]
    return [(value,) + rest for value in range(2) for rest in tiles(count - 1)]


def back_kernel(
    heads,
    members,
    tensor_size,
    dp_size,
    names,
    number,
    q_ref,
    k_ref,
    v_ref,
    l_ref,
    datt_ref,
    normed_ref,
    weight_ref,
    down_ref,
    up_ref,
    att_ref,
    branch_ref,
    blocks_ref,
    norm_ref,
    middle_ref,
    hidden_bias_ref,
    early0_ref,
    early1_ref,
    early2_ref,
    early3_ref,
    early4_ref,
    early5_ref,
    blocks_out,
    query_out,
    key_out,
    value_out,
    out_out,
    down_out,
    up_out,
    early_out,
    late_out,
    heads_out,
    *scratch,
):
    held = dict(zip(names, scratch))
    early_refs = (early0_ref, early1_ref, early2_ref, early3_ref, early4_ref, early5_ref)
    send, recv, here = scratch[len(names):]
    copies = Copies(send, recv)
    t_pos = lax.axis_index(TENSOR)
    d_pos = lax.axis_index(DP)
    member = t_pos % members
    core, side = bit(d_pos, 1), bit(d_pos, 2)
    total_rows, wide_span = q_ref.shape
    rows, width = blocks_ref.shape
    masks, inner, dp_masks = bits_of(tensor_size), bits_of(members), bits_of(dp_size)
    outer_first, inner_first = masks[::-1], inner[::-1]
    scale = HEAD_DIM ** (-0.5)
    extra = heads * HEAD_DIM
    position = {TENSOR: t_pos, DP: d_pos}
    every = [(DP, mask) for mask in dp_masks] + [(TENSOR, mask) for mask in masks]
    rest_dp = [(DP, mask) for mask in dp_masks[2:]]
    rest_tensor = [(TENSOR, mask) for mask in masks[len(inner):]]

    named = {
        "x": (TENSOR, masks[0]),
        "z0": (TENSOR, masks[1]),
        "z1": (TENSOR, masks[2]),
        "y": (DP, 2),
    }

    def to(move):
        axis, mask = move
        return {axis: turned(position[axis], mask)}

    def mine(move):
        axis, mask = move
        return bit(position[axis], mask)

    def xor_member(j):
        return sum(mask * ((bit(member, mask) + bit(j, mask)) % 2) for mask in inner)

    def slot(index):
        return tuple(bit(index, mask) for mask in inner_first)

    peers = [to(move) for move in every]
    peers += [
        {TENSOR: t_pos - member + xor_member(j)} for j in range(1, members) if j not in inner
    ]
    barrier = greet(peers)
    grad_mixed, grads = held["grad_mixed"], held["grads"]
    sum_k, sum_v = held["sum_k"], held["sum_v"]
    own_lanes = pl.ds(pl.multiple_of(member * wide_span, wide_span), wide_span)
    own_copy = pltpu.make_async_copy(datt_ref.at[:, own_lanes], grad_mixed.at[member], here.at[0])
    own_copy.start()
    sum_k[...] = jnp.zeros_like(sum_k)
    sum_v[...] = jnp.zeros_like(sum_v)
    pl.semaphore_wait(barrier, len(peers))

    base = copies.used
    copies.used += members

    def datt_copy(j):
        block = xor_member(j)
        there = pl.ds(pl.multiple_of(block * wide_span, wide_span), wide_span)
        return copies.make(
            datt_ref.at[:, there],
            grad_mixed.at[member],
            {TENSOR: t_pos - member + block},
            base + j,
        )

    for j in range(1, members):
        datt_copy(j).start()

    def add(target, at, source, source_at):
        target[at] = low(wide(target[at]) + wide(source[source_at]))

    def hidden_chain(part):
        third = width // PARTS
        columns = pl.ds(part * third, third)
        dims = [(TENSOR, mask) for mask in outer_first] + [(DP, 2)]
        order = [named[name] for name in HIDDEN_ORDERS[part]]
        order += [(TENSOR, mask) for mask in masks[3:]]
        full = slice(None)
        current = None
        for stage, move in enumerate(order):
            landing = held[f"hidden{part}_{stage}"]
            where = dims.index(move)
            away = (full,) * where + (1 - mine(move),) + (full,) * (len(dims) - 1 - where)
            sent = []
            if current is None:
                for which, source in enumerate((down_ref, up_ref)):
                    sent.append(
                        copies.start(
                            source.at[away + (full, columns)], landing.at[which], to(move)
                        )
                    )
            else:
                sent.append(copies.start(current.at[(full,) + away], landing, to(move)))
            yield
            for copy in sent:
                copy.wait_recv()
            for tile in tiles(len(dims) - 1):
                kept = tile[:where] + (mine(move),) + tile[where:]
                for which in range(2):
                    if current is None:
                        source = (down_ref, up_ref)[which]
                        add(landing, (which,) + tile, source, kept + (full, columns))
                    else:
                        add(landing, (which,) + tile, current, (which,) + kept)
            current = landing
            dims = dims[:where] + dims[where + 1 :]
        for stage, move in enumerate(rest_dp):
            landing = held[f"hidden{part}_more{stage}"]
            copy = copies.start(current, landing, to(move))
            yield
            copy.wait_recv()
            for which in range(2):
                add(landing, which, current, which)
            current = landing
        whole = held["whole"]
        for which in range(2):
            whole[which, core, side, :, columns] = current[which]
        block = whole.at[:, core, side, :, columns]
        copy = copies.start(block, block, to((DP, 2)))
        yield
        copy.wait_recv()
        block = whole.at[:, core, :, :, columns]
        copy = copies.start(block, block, to((DP, 1)))
        yield
        copy.wait_recv()

    def out_chain():
        halvings = [(DP, 1)] + [named[name] for name in OUT_ORDER]
        current = out_part
        for stage, move in enumerate(halvings):
            landing = held[f"out{stage}"]
            copy = copies.start(current.at[1 - mine(move)], landing, to(move))
            yield
            copy.wait_recv()
            for tile in tiles(3 - stage):
                add(landing, tile + (slice(None),), current, (mine(move),) + tile)
            current = landing
        for stage, move in enumerate([move for move in every if move not in halvings]):
            landing = held[f"out_more{stage}"]
            copy = copies.start(current, landing, to(move))
            yield
            copy.wait_recv()
            add(landing, slice(None), current, slice(None))
            current = landing
        out_full = held["out_full"]
        own = tuple(mine(move) for move in halvings)
        out_full[own] = current[...]
        for stage in range(3, -1, -1):
            block = out_full.at[own[: stage + 1]]
            copy = copies.start(block, block, to(halvings[stage]))
            yield
            copy.wait_recv()

    def square_chain():
        square, one, two = held["square"], held["square_one"], held["square_two"]
        copy = copies.start(square.at[:, 1 - core], one, to((DP, 1)))
        yield
        copy.wait_recv()
        for which in range(3):
            for tile in tiles(1):
                add(one, (which,) + tile, square, (which, core) + tile)
        copy = copies.start(one.at[:, 1 - side], two, to((DP, 2)))
        yield
        copy.wait_recv()
        for which in range(3):
            add(two, which, one, (which, side))
        current = two
        for stage, move in enumerate(rest_tensor + rest_dp):
            landing = held[f"square_more{stage}"]
            copy = copies.start(current, landing, to(move))
            yield
            copy.wait_recv()
            for which in range(3):
                add(landing, which, current, which)
            current = landing
        full = held["square_full"]
        dims = [(TENSOR, mask) for mask in inner_first] + [(DP, 1), (DP, 2)]
        own = tuple(mine(move) for move in dims)
        for which in range(3):
            full[(which,) + own] = current[which]
        moves = [(TENSOR, mask) for mask in inner] + [(DP, 2)]
        for stage in range(len(moves) + 1):
            sent = []
            for which in range(3):
                turn = which % len(moves)
                order = moves[turn:] + moves[:turn] + [(DP, 1)]
                done = order[:stage]
                at = tuple(slice(None) if move in done else mine(move) for move in dims)
                block = full.at[(which,) + at]
                sent.append(copies.start(block, block, to(order[stage])))
            yield
            for copy in sent:
                copy.wait_recv()

    def rows_chain():
        half = width // 2
        part_ref = held["rows_part"]
        state = []
        for part in range(2):
            state.append([part_ref, list(inner_first), (pl.ds(part * half, half),)])
        orders = (inner, inner[::-1])
        for stage in range(len(inner)):
            sent = []
            for part in range(2):
                current, dims, columns = state[part]
                mask = orders[part][stage]
                where = dims.index(mask)
                away = (slice(None),) * where + (1 - bit(member, mask),)
                away += (slice(None),) * (len(dims) - 1 - where)
                sent.append(
                    copies.start(
                        current.at[away + (slice(None),) + columns],
                        held[f"rows{part}_{stage}"],
                        to((TENSOR, mask)),
                    )
                )
            yield
            for part in range(2):
                sent[part].wait_recv()
                current, dims, columns = state[part]
                mask = orders[part][stage]
                where = dims.index(mask)
                landing = held[f"rows{part}_{stage}"]
                for tile in tiles(len(dims) - 1):
                    kept = tile[:where] + (bit(member, mask),) + tile[where:]
                    kept += (slice(None),) + columns
                    if stage < len(inner) - 1:
                        add(landing, tile + (slice(None),), current, kept)
                    else:
                        held["grad_rows"][:, part * half : (part + 1) * half] = wide(
                            landing[...]
                        ) + wide(current[kept])
                state[part] = [landing, dims[:where] + dims[where + 1 :], ()]

    def small_chain(pairs):
        for stage, move in enumerate(every):
            sent = []
            for first, name, _ in pairs:
                source = first if stage == 0 else held[f"{name}{stage - 1}"]
                sent.append(copies.start(source, held[f"{name}{stage}"], to(move)))
            yield
            for copy, (first, name, result) in zip(sent, pairs):
                copy.wait_recv()
                source = first if stage == 0 else held[f"{name}{stage - 1}"]
                value = held[f"{name}{stage}"][...] + source[...]
                if stage == len(every) - 1:
                    result[...] = value
                else:
                    held[f"{name}{stage}"][...] = value

    chains = {
        "out": out_chain(),
        "early": small_chain([(held["early_sum"], "early", early_out)]),
        "rows": rows_chain(),
        "square": square_chain(),
        "late": small_chain(
            [(held["late"], "late", late_out), (held["heads_sum"], "heads", heads_out)]
        ),
    }
    for part in range(PARTS):
        chains[f"h{part}"] = hidden_chain(part)
    live = list(chains)

    def go(*wanted):
        for name in wanted:
            if name in live:
                if next(chains[name], True):
                    live.remove(name)

    span = heads * HEAD_DIM
    unit_rows = span // 4
    out_part = held["out_part"]
    for index in range(members):
        full = dot_tn(att_ref[:, index * wide_span : (index + 1) * wide_span], branch_ref[...])
        for quarter_index in range(4):
            at = index * 4 + quarter_index
            where = tuple((at * 16 // (members * 4)) // step % 2 for step in (8, 4, 2, 1))
            inner_row = (at * unit_rows) % out_part.shape[4]
            out_part[where + (slice(inner_row, inner_row + unit_rows), slice(None))] = low(
                full[quarter_index * unit_rows : (quarter_index + 1) * unit_rows]
            )
    early = held["early_sum"]
    early[...] = jnp.zeros_like(early)
    for index, row in enumerate(early_refs):
        early[index : index + 1, :] = row[...].reshape(1, width)
    early[6 : 6 + hidden_bias_ref.shape[0], :] = hidden_bias_ref[...]
    own_copy.wait()
    lanes = lax.broadcasted_iota(jnp.int32, (rows, wide_span), 1)

    def attend(block):
        at = pl.ds(pl.multiple_of(block * rows, rows), rows)
        query = q_ref[at, :]
        grad = grad_mixed[block]
        grad_q = jnp.zeros((rows, wide_span), F32)
        for head in range(heads):
            chosen = head_mask(lanes, head)
            log_total = l_ref[at, head : head + 1]
            high = low(log_total)
            rest = log_total - wide(high)
            middle = low(rest)
            last = low(rest - wide(middle))
            fill = jnp.where(lanes == extra, 1.0, 0.0)
            fill = jnp.where(lanes == extra + 1, -wide(high), fill)
            fill = jnp.where(lanes == extra + 2, -wide(middle), fill)
            fill = jnp.where(lanes == extra + 3, -wide(last), fill)
            left = jnp.where(chosen, query, low(fill))
            upstream = jnp.where(chosen, grad, jnp.zeros_like(grad))
            probs = jnp.exp(dot_nt(k_ref[...], left))
            grad_probs = dot_nt(v_ref[...], upstream)
            centred = jnp.sum(probs * grad_probs, axis=0, keepdims=True)
            grad_scores = low(probs * (grad_probs - centred))
            sum_k[...] += dot_nn(grad_scores, left)
            sum_v[...] += dot_nn(low(probs), upstream)
            out = dot_tn(grad_scores, k_ref[...]) * scale
            grad_q = jnp.where(chosen, out, grad_q)
        grads[0, at, :] = low(grad_q)

    def block(index):
        count = members // 2

        @pl.loop(index * count, (index + 1) * count)
        def _(j):
            @pl.when(j > 0)
            def _():
                datt_copy(j).wait_recv()

            attend(xor_member(j))

    def finish_attention():
        keep = lanes < extra

        @pl.loop(0, members)
        def _(block):
            at = pl.ds(pl.multiple_of(block * rows, rows), rows)
            grads[1, at, :] = low(jnp.where(keep, sum_k[at, :], 0.0))
            grads[2, at, :] = low(sum_v[at, :])

    def compute_rows():
        @pl.loop(0, members)
        def _(block):
            at = pl.ds(pl.multiple_of(block * rows, rows), rows)
            part = dot_nt(grads[0, at, :], weight_ref[0])
            part += dot_nt(grads[1, at, :], weight_ref[1])
            part += dot_nt(grads[2, at, :], weight_ref[2])
            held["rows_part"][slot(block) + (slice(None), slice(None))] = low(part)

    def compute_square():
        four = held["square"].shape[3]

        @pl.loop(0, 3)
        def _(which):
            full = dot_tn(grads[which], normed_ref[...])
            for tile in tiles(2):
                start = (tile[0] * 2 + tile[1]) * four
                held["square"][(which,) + tile] = low(full[start : start + four])

        heads_sum = held["heads_sum"]
        heads_sum[...] = jnp.zeros_like(heads_sum)
        heads_sum[0, member] = jnp.sum(wide(grads[0]), axis=0, keepdims=True)
        heads_sum[1, member] = jnp.sum(wide(grads[2]), axis=0, keepdims=True)

    def compute_norm():
        while "rows" in live:
            go("rows")
        gain = norm_ref[0:1, :]
        gain_sum = jnp.zeros((1, width), F32)
        shift_sum = jnp.zeros((1, width), F32)
        step = rows // 2
        for start in range(0, rows, step):
            at = pl.ds(start, step)
            grad = held["grad_rows"][at, :]
            values = wide(blocks_ref[at, :])
            centre = values - jnp.mean(values, axis=-1, keepdims=True)
            spread = jnp.mean(centre * centre, axis=-1, keepdims=True)
            factor = lax.rsqrt(spread + EPSILON)
            unit = centre * factor
            scaled = grad * gain
            pulled = scaled - jnp.mean(scaled, axis=-1, keepdims=True)
            pulled = pulled - unit * jnp.mean(scaled * unit, axis=-1, keepdims=True)
            blocks_out[at, :] = middle_ref[at, :] + factor * pulled
            gain_sum += jnp.sum(grad * unit, axis=0, keepdims=True)
            shift_sum += jnp.sum(grad, axis=0, keepdims=True)
        late = held["late"]
        late[...] = jnp.zeros_like(late)
        late[0:1, :] = gain_sum
        late[1:2, :] = shift_sum

    for token in sum(BACK_PROGRAM, ()):
        if token.startswith("*block"):
            block(int(token[6:]))
            if token == "*block1":
                finish_attention()
        elif token == "*rows":
            compute_rows()
        elif token == "*square":
            compute_square()
        elif token == "*norm":
            compute_norm()
        else:
            go(token)
    while live:
        go(*list(live))
    finals = []
    sources = [held["square_full"].at[which] for which in range(3)] + [held["out_full"]]
    sources += [held["whole"].at[which] for which in range(2)]
    targets = (query_out, key_out, value_out, out_out, down_out, up_out)
    for index, (source, target) in enumerate(zip(sources, targets)):
        copy = pltpu.make_async_copy(source, target, here.at[index])
        copy.start()
        finals.append(copy)
    for copy in finals:
        copy.wait()
    for j in range(1, members):
        datt_copy(j).wait_send()
    copies.drain()


def back(
    heads,
    members,
    tensor_size,
    dp_size,
    span,
    quarter,
    queries,
    keys,
    values,
    logs,
    datt,
    normed,
    weights,
    grad_down,
    grad_up,
    attended,
    grad_branch,
    blocks,
    norm,
    middle,
    hidden_bias,
    early,
):
    rows, width = blocks.shape
    wide_span = queries.shape[1]
    shapes = back_shapes(members, rows, width, wide_span, span, tensor_size, dp_size, quarter)
    names = list(shapes)
    outer, inner = len(bits_of(tensor_size)), len(bits_of(members))
    every = outer + len(bits_of(dp_size))
    number = members + PARTS * (outer + 1 + 1 + 2 + len(bits_of(dp_size))) + every + 8
    number += 2 + every + 3 * (inner + 2) + 2 * inner + 3 * every
    vmem = pl.BlockSpec(memory_space=pltpu.VMEM)
    away = pl.BlockSpec(memory_space=pl.ANY)

    def shape_of(name):
        return jax.ShapeDtypeStruct(*shapes[name])

    def part_of(name):
        shape, kind = shapes[name]
        return jax.ShapeDtypeStruct(shape[1:], kind)

    return pl.pallas_call(
        functools.partial(back_kernel, heads, members, tensor_size, dp_size, names, number),
        out_shape=(
            jax.ShapeDtypeStruct((rows, width), F32),
            part_of("square_full"),
            part_of("square_full"),
            part_of("square_full"),
            shape_of("out_full"),
            part_of("whole"),
            part_of("whole"),
            jax.ShapeDtypeStruct((16, width), F32),
            shape_of("late"),
            shape_of("heads_sum"),
        ),
        in_specs=[vmem] * 21,
        out_specs=(vmem,) + (away,) * 6 + (vmem,) * 3,
        scratch_shapes=[pltpu.VMEM(*shapes[name]) for name in names]
        + [
            pltpu.SemaphoreType.DMA((number,)),
            pltpu.SemaphoreType.DMA((number,)),
            pltpu.SemaphoreType.DMA((6,)),
        ],
        compiler_params=pltpu.CompilerParams(
            vmem_limit_bytes=60 << 20, collective_id=1, has_side_effects=True
        ),
        cost_estimate=pl.CostEstimate(
            flops=40_000_000_000, bytes_accessed=40_000_000, transcendentals=3_000_000
        ),
    )(
        queries,
        keys,
        values,
        logs,
        datt,
        normed,
        weights,
        grad_down,
        grad_up,
        attended,
        grad_branch,
        blocks,
        norm,
        middle,
        hidden_bias,
        *early,
    )


def heads_where(heads, members, wide_span):
    return [index * heads * HEAD_DIM for index in range(members)]


def vectors_kernel(
    starts,
    early_ref,
    late_ref,
    heads_ref,
    query_ref,
    value_ref,
    out_ref,
    gain1_ref,
    shift1_ref,
    gain2_ref,
    shift2_ref,
    down_ref,
    gates_ref,
):
    width = out_ref.shape[0]
    span = starts[1]
    for which, target in ((0, query_ref), (1, value_ref)):
        pieces = [
            heads_ref[which, index, :, : min(span, width - start)]
            for index, start in enumerate(starts)
            if start < width
        ]
        target[...] = jnp.concatenate(pieces, axis=1).reshape(width)
    rows = ((early_ref, 0, out_ref), (late_ref, 0, gain1_ref), (late_ref, 1, shift1_ref))
    rows += ((early_ref, 1, gain2_ref), (early_ref, 2, shift2_ref), (early_ref, 3, down_ref))
    for source, row, target in rows:
        target[...] = source[row : row + 1, :].reshape(width)
    gates_ref[...] = early_ref[4:6, :]


def vectors(starts, width, early, late, head_sums):
    line = jax.ShapeDtypeStruct((width,), F32)
    return pl.pallas_call(
        functools.partial(vectors_kernel, starts),
        out_shape=(line,) * 8 + (jax.ShapeDtypeStruct((2, width), F32),),
        compiler_params=pltpu.CompilerParams(vmem_limit_bytes=4 << 20),
    )(early, late, head_sums)


def local(
    blocks,
    counts,
    cotangent,
    w_query,
    w_key,
    w_value,
    w_out,
    b_query,
    b_value,
    b_out,
    norm1_gain,
    norm1_bias,
    norm2_gain,
    norm2_bias,
    gate_logits,
    w_up,
    b_up,
    w_down,
    b_down,
):
    rows, width = blocks.shape
    tensor_size = lax.axis_size(TENSOR)
    dp_size = lax.axis_size(DP)
    t_pos = lax.axis_index(TENSOR)
    d_pos = lax.axis_index(DP)
    members = SEQ // rows
    member = t_pos % members
    per_head = -(-HEADS // members)
    span = per_head * HEAD_DIM
    ring = 4
    line = tensor_size // ring
    z_pos = t_pos // line
    x_pos = t_pos % line
    core = d_pos % 2
    side = (d_pos // 2) % 2
    shard = w_up.shape[1]
    quarter = shard // 4
    hidden_total = shard * tensor_size
    dp_rest = [(DP, mask) for mask in bits_of(dp_size)[2:]]
    member_masks = bits_of(members)
    tensor_rest = [(TENSOR, mask) for mask in bits_of(tensor_size)[len(member_masks):]]

    def z_shift(value, step):
        pairs = [
            (i, ((i // line + step) % ring) * line + i % line) for i in range(tensor_size)
        ]
        return lax.ppermute(value, TENSOR, pairs)

    def x_shift(value, step):
        pairs = [
            (i, (i // line) * line + (i % line + step) % line) for i in range(tensor_size)
        ]
        return lax.ppermute(value, TENSOR, pairs)

    gain_one = wide(norm1_gain)
    shift_one = wide(norm1_bias)
    gain_two = wide(norm2_gain)
    shift_two = wide(norm2_bias)
    logits_gate = wide(gate_logits)
    inputs = wide(blocks)

    doc_counts = pick(counts, t_pos // members)
    slot_ids = member ^ jnp.arange(members, dtype=jnp.int32)
    own_pos = member * rows + jnp.arange(rows, dtype=jnp.int32)
    visual = own_pos >= TEXT_SLOTS

    def head_part(weight):
        extra = per_head * HEAD_DIM * members - width
        if extra:
            weight = jnp.pad(weight, ((0, 0),) * (weight.ndim - 1) + ((0, extra),))
        return lax.dynamic_slice_in_dim(weight, member * span, span, weight.ndim - 1)

    wide_span = -(-(span + 4) // 128) * 128

    def widen(array):
        return jnp.pad(array, ((0, 0),) * (array.ndim - 1) + ((0, wide_span - array.shape[-1]),))

    w_q = widen(head_part(w_query))
    w_k = widen(head_part(w_key))
    w_v = widen(head_part(w_value))
    bias = wide(jnp.stack([widen(head_part(b_query)), widen(head_part(b_value))], 0))
    halves = (2, 2, quarter, width)
    piece = jnp.stack(
        [pick(w_up.T.reshape(halves), core), pick(w_down.reshape(halves), core)], 0
    )
    queries, keys, values, logs, normed_all, attended, cot_all, up_t, down, biases = front(
        per_head,
        members,
        tensor_size,
        blocks,
        jnp.stack([gain_one, shift_one], 0),
        w_q,
        w_k,
        w_v,
        bias,
        jnp.broadcast_to(doc_counts[:, None], (2, 128)),
        cotangent,
        piece,
        wide(b_up)[None, :],
    )
    normed_all = normed_all.reshape(SEQ, width)
    cot_all = cot_all.reshape(2 * rows, width)
    up_t = up_t.reshape(-1, width)
    down = down.reshape(-1, width)
    biases = biases.reshape(tensor_size, shard)
    biases = lax.dynamic_slice_in_dim(biases, core * (2 * quarter), 2 * quarter, 1).reshape(-1)
    extra_rows = members * span - width
    out_rows = jnp.pad(w_out, ((0, extra_rows), (0, 0))) if extra_rows else w_out
    out_rows = jnp.pad(out_rows.reshape(members, span, width), ((0, 0), (0, wide_span - span), (0, 0)))
    out_rows = out_rows.reshape(members * wide_span, width)

    branch = dot_nn(attended, out_rows) + wide(b_out)
    gate = jax.nn.sigmoid(
        jnp.where(visual[:, None], logits_gate[1][None, :], logits_gate[0][None, :])
    )
    middle = inputs + gate * branch
    second = low(normalize(middle, gain_two, shift_two))
    second_all = jnp.concatenate([second, flip(second, DP, 1)], 0)

    pre = dot_nt(second_all, up_t) + biases
    hidden = low(gelu_exact(pre))
    grad_down = low(dot_tn(hidden, cot_all))
    spread = dot_nt(cot_all, down)
    dpre = low(gelu_grad(pre, spread))
    grad_second = dot_nn(dpre[:rows], up_t) + flip(dot_nn(dpre[rows:], up_t), DP, 1)
    lowered = dot_nn(hidden[:rows], down) + flip(dot_nn(hidden[rows:], down), DP, 1)
    grad_up = low(dot_tn(dpre, second_all))
    grad_up_bias = jnp.sum(wide(dpre), axis=0)
    joined = low(middle + lowered + wide(b_down))

    upstream = wide(cotangent)
    pull_two = jax.vjp(normalize, middle, gain_two, shift_two)[1]
    grad_middle_norm, grad_gain_two, grad_shift_two = pull_two(grad_second)
    grad_middle = upstream + grad_middle_norm
    grad_branch = low(gate * grad_middle)
    gate_term = grad_middle * branch * gate * (1.0 - gate)
    grad_gate = [
        jnp.sum(jnp.where(visual[:, None], 0.0, gate_term), axis=0),
        jnp.sum(jnp.where(visual[:, None], gate_term, 0.0), axis=0),
    ]
    grad_out_bias = jnp.sum(wide(grad_branch), axis=0)
    grad_attended = low(dot_nt(grad_branch, out_rows))
    bias_sum = grad_up_bias.reshape(tensor_size, 1, 2 * quarter)
    both = jnp.arange(2, dtype=jnp.int32)[None, :, None]
    bias_sum = jnp.where(both == core, bias_sum, 0.0).reshape(hidden_total // width, width)
    early = [grad_out_bias, grad_gain_two, grad_shift_two, jnp.sum(upstream, axis=0)] + grad_gate
    hidden_shape = (2,) * len(bits_of(tensor_size)) + (2, quarter, width)
    grad_blocks, *squares, outs, down_sum, up_sum, early, late, head_sums = back(
        per_head,
        members,
        tensor_size,
        dp_size,
        span,
        quarter,
        queries,
        keys,
        values,
        logs,
        grad_attended,
        normed_all,
        jnp.stack([w_q, w_k, w_v], 0),
        grad_down.reshape(hidden_shape),
        grad_up.reshape(hidden_shape),
        attended,
        grad_branch,
        blocks,
        jnp.stack([gain_one, shift_one], 0),
        grad_middle,
        bias_sum,
        early,
    )
    outs = outs.reshape(members * span, width)[:width]
    query_bias, value_bias, out_bias, gain1, shift1, gain2, shift2, down_bias, gates = vectors(
        heads_where(per_head, members, wide_span), width, early, late, head_sums
    )
    bias_out = lax.dynamic_slice_in_dim(
        early[6 : 6 + hidden_total // width].reshape(hidden_total), t_pos * shard, shard, 0
    )

    def turned_over(value, size):
        identity = low(jnp.eye(size, dtype=F32))
        return dot_tn(value, identity)

    flipped = [
        turned_over(square.reshape(members * span, width)[:width], width) for square in squares
    ]
    return (
        joined,
        grad_blocks,
        flipped[0],
        flipped[1],
        flipped[2],
        wide(outs),
        query_bias,
        value_bias,
        out_bias,
        gain1,
        shift1,
        gain2,
        shift2,
        gates,
        turned_over(up_sum.reshape(shard, width), shard),
        bias_out,
        wide(down_sum.reshape(shard, width)),
        down_bias,
    )


def solution(mesh):
    rows = P((DP, TENSOR), None)
    in_specs = (rows, P(DP, None), rows) + (P(),) * 12 + (
        P(None, TENSOR),
        P(TENSOR),
        P(TENSOR, None),
        P(),
    )
    out_specs = (rows, rows) + (P(),) * 12 + (
        P(None, TENSOR),
        P(TENSOR),
        P(TENSOR, None),
        P(),
    )
    return jax.shard_map(local, mesh=mesh, in_specs=in_specs, out_specs=out_specs, check_vma=False)
```

```python
import functools

import jax
import jax.numpy as jnp
from jax import lax
from jax.experimental import pallas as pl
from jax.experimental.pallas import tpu as pltpu
from jax.sharding import PartitionSpec as P

HEADS = 12
HEAD_DIM = 64
TEXT_SLOTS = 896
SEQ = 1024
EPSILON = 1e-05
PARTS = 3
HIDDEN_ORDERS = (("z0", "y", "x", "z1"), ("x", "y", "z0", "z1"), ("y", "x", "z0", "z1"))
OUT_ORDER = ("x", "y", "z0")
BACK_PROGRAM = (
    ("h1", "*outs", "h2", "out", "h0", "*block0", "*block1", "out", "*square", "square", "*rows", "rows"),
    ("square", "out", "h1", "square", "out", "rows", "h0", "out", "h2", "h1", "square", "rows"),
    ("*norm", "late", "early", "late", "early", "out", "h1", "h0", "h2", "out", "late", "early"),
    ("square", "h0", "h1", "out", "late", "h2", "early", "square", "h1", "late", "h1", "h0"),
    ("early", "out", "out", "h2", "h0", "square", "h0", "h2", "late", "early", "square", "h2"),
)
FRONT_CUTS = (16, 18, 19)
FRONT_FIRST = True
BF = jnp.bfloat16
TENSOR = "tensor"
DP = "dp"
F32 = jnp.float32


def normalize(values, gain, shift):
    centre = values - jnp.mean(values, axis=-1, keepdims=True)
    spread = jnp.mean(centre * centre, axis=-1, keepdims=True)
    return centre * lax.rsqrt(spread + EPSILON) * gain + shift


def gelu_exact(values):
    return jax.nn.gelu(values, approximate=False)


def gelu_grad(values, upstream):
    return jax.vjp(gelu_exact, values)[1](upstream)[0]


def dot_nn(left, right):
    return lax.dot_general(left, right, (((1,), (0,)), ((), ())), preferred_element_type=F32)


def dot_tn(left, right):
    return lax.dot_general(left, right, (((0,), (0,)), ((), ())), preferred_element_type=F32)


def dot_nt(left, right):
    return lax.dot_general(left, right, (((1,), (1,)), ((), ())), preferred_element_type=F32)


def pick(array, index):
    return lax.dynamic_index_in_dim(array, index, 0, keepdims=False)


def low(value):
    return value.astype(BF)


def wide(value):
    return value.astype(F32)


def flip(value, axis, mask):
    size = lax.axis_size(axis)
    return lax.ppermute(value, axis, [(i, i ^ mask) for i in range(size)])


def bits_of(size):
    found = []
    mask = 1
    while mask < size:
        found.append(mask)
        mask *= 2
    return found


def sum_everywhere(value):
    for axis in (DP, TENSOR):
        for mask in bits_of(lax.axis_size(axis)):
            value = value + flip(value, axis, mask)
    return value


def exchange_sum(value, stages):
    for axis, mask in stages:
        sent = low(value)
        value = wide(sent) + wide(flip(sent, axis, mask))
    return value


def head_mask(lanes, head, offset):
    lanes = lanes - offset
    return (lanes >= head * HEAD_DIM) & (lanes < (head + 1) * HEAD_DIM)


def window(index, span, wide_span):
    start = (index * span) // 128 * 128
    offset = index * span - start
    return start, offset, (offset + span) % wide_span


def bit(index, mask):
    return (index // mask) % 2


def turned(index, mask):
    return index + mask - 2 * mask * bit(index, mask)


def place_of(masks, gathered, index):
    return tuple(slice(None) if mask in gathered else bit(index, mask) for mask in masks)


class Copies:
    def __init__(self, send, recv):
        self.send, self.recv, self.used, self.open = send, recv, 0, []

    def make(self, source, target, device, at=None):
        if at is None:
            at = self.used
            self.used += 1
        return pltpu.make_async_remote_copy(
            src_ref=source,
            dst_ref=target,
            send_sem=self.send.at[at],
            recv_sem=self.recv.at[at],
            device_id=device,
            device_id_type=pl.DeviceIdType.MESH,
        )

    def start(self, source, target, device):
        copy = self.make(source, target, device)
        copy.start()
        self.open.append(copy)
        return copy

    def drain(self):
        for copy in self.open:
            copy.wait_send()
        self.open = []


def greet(devices):
    barrier = pltpu.get_barrier_semaphore()
    for device in devices:
        pl.semaphore_signal(
            barrier, inc=1, device_id=device, device_id_type=pl.DeviceIdType.MESH
        )
    return barrier


def weight_parts(tensor_masks, width):
    unit = width // 6
    low_masks, high = tensor_masks[:2], tensor_masks[2:][::-1]
    one, other = high + low_masks, high + low_masks[::-1]
    return (
        (0, 2 * unit, True, other),
        (2 * unit, 2 * unit, True, other),
        (4 * unit, unit, True, one),
        (5 * unit, unit, False, one),
    )


def subsets(masks):
    found = [()]
    for mask in masks:
        found += [kept + (mask,) for kept in found]
    return found


def front_copies(tensor_size, members, width):
    masks, inner = bits_of(tensor_size), bits_of(members)
    parts = weight_parts(masks, width)
    forwards = sum(1 for part in parts if part[2])
    pieces = tensor_size - 1
    return 2 * len(inner) + pieces * (len(parts) + forwards) + len(masks) + 1 + members


def front_kernel(
    heads,
    members,
    tensor_size,
    blocks_ref,
    norm_ref,
    wq_ref,
    wk_ref,
    wv_ref,
    b_ref,
    counts_ref,
    cot_ref,
    piece_ref,
    up_bias_ref,
    q_ref,
    k_ref,
    v_ref,
    l_ref,
    normed_out,
    att_out,
    cot_out,
    up_out,
    down_out,
    bias_out,
    normed,
    mixed,
    att,
    cots,
    weights,
    biases,
    heads_weight,
    send,
    recv,
    here,
):
    t_pos = lax.axis_index(TENSOR)
    d_pos = lax.axis_index(DP)
    member = t_pos % members
    side = bit(d_pos, 2)
    rows, width = blocks_ref.shape
    wide_span = q_ref.shape[1]
    masks, inner = bits_of(tensor_size), bits_of(members)
    outer_first, inner_first = masks[::-1], inner[::-1]
    scale = HEAD_DIM ** (-0.5)
    span = heads * HEAD_DIM
    start, offset, extra = window(member, span, wide_span)
    lane_window = pl.ds(pl.multiple_of(start, 128), wide_span)
    copies = Copies(send, recv)

    def along(mask):
        return {TENSOR: turned(t_pos, mask)}

    def slot(index):
        return tuple(bit(index, mask) for mask in inner_first)

    def slot_of(index):
        return tuple(bit(index, mask) for mask in outer_first)

    diagonals = [j for j in range(1, members) if j not in inner]

    def xor_member(j):
        return sum(mask * ((bit(member, mask) + bit(j, mask)) % 2) for mask in inner)

    peers = [along(mask) for mask in masks]
    peers += [{TENSOR: t_pos - member + xor_member(j)} for j in diagonals]
    peers += [{DP: turned(d_pos, 1)}, {DP: turned(d_pos, 2)}]
    barrier = greet(peers)

    own = place_of(outer_first, (), t_pos)
    local = [
        pltpu.make_async_copy(piece_ref, weights.at[(slice(None),) + own], here.at[0]),
        pltpu.make_async_copy(cot_ref, cots.at[0], here.at[1]),
        pltpu.make_async_copy(up_bias_ref, biases.at[own], here.at[2]),
    ]
    for which, source in enumerate((wq_ref, wk_ref, wv_ref)):
        local.append(
            pltpu.make_async_copy(
                source.at[:, lane_window], heads_weight.at[which], here.at[3 + which]
            )
        )
    for copy in local:
        copy.start()
    mine = slot(member)
    step = rows // 2
    for start in range(0, rows, step):
        at = pl.ds(start, step)
        normed[mine + (at, slice(None))] = low(
            normalize(wide(blocks_ref[at, :]), norm_ref[0:1, :], norm_ref[1:2, :])
        )
    for copy in local:
        copy.wait()
    pl.semaphore_wait(barrier, len(peers))

    half = width // 2
    halves = ((pl.ds(0, half), inner), (pl.ds(half, half), inner[::-1]))

    def send_rows(stage):
        sent = []
        for columns, order in halves:
            block = normed.at[place_of(inner_first, order[:stage], member) + (slice(None), columns)]
            sent.append(copies.start(block, block, along(order[stage])))
        return sent

    parts = weight_parts(masks, width)

    def device_of(kept):
        index = t_pos
        for mask in kept:
            index = turned(index, mask)
        return index

    arrivals = {}

    def send_piece(number, kept):
        start, size, split, order = parts[number]
        rest = (side if split else slice(None), slice(None), pl.ds(start, size))
        block = weights.at[(slice(None),) + slot_of(device_of(kept)) + rest]
        after = order.index(kept[-1]) + 1 if kept else 0
        for mask in order[after:]:
            arrivals[number, kept + (mask,)] = copies.start(block, block, along(mask))
        if split and kept:
            forwards.append(copies.start(block, block, {DP: turned(d_pos, 2)}))

    def receive_piece(number, kept):
        arrivals[number, kept].wait_recv()
        send_piece(number, kept)

    def send_bias(stage):
        block = biases.at[place_of(outer_first, masks[:stage], t_pos)]
        return copies.start(block, block, along(masks[stage]))

    def project(block):
        at = pl.ds(pl.multiple_of(block * rows, rows), rows)
        part = normed[slot(block) + (slice(None), slice(None))]
        position = block * rows + lax.broadcasted_iota(jnp.int32, (rows, wide_span), 0)
        lane = lax.broadcasted_iota(jnp.int32, (rows, wide_span), 1)
        text, visual = counts_ref[0:1, 0:1], counts_ref[1:2, 0:1]
        bound = jnp.where(position >= TEXT_SLOTS, visual + TEXT_SLOTS, text)
        tail = jnp.where(lane > extra, 1.0, jnp.where(position >= bound, -1e30, 0.0))
        spare = (lane >= extra) & (lane < extra + 4)
        q_ref[at, :] = low(low(dot_nn(part, heads_weight[0]) + b_ref[0:1, lane_window]) * scale)
        k_ref[at, :] = low(jnp.where(spare, tail, dot_nn(part, heads_weight[1])))
        v_ref[at, :] = low(dot_nn(part, heads_weight[2]) + b_ref[1:2, lane_window])

    forwards = []

    def send_own():
        for number in range(len(parts)):
            send_piece(number, ())

    arriving = send_rows(0)
    other_cots = copies.start(cot_ref, cots.at[1], {DP: turned(d_pos, 1)})
    for stage in range(1, len(inner)):
        if stage == 1 and FRONT_FIRST:
            send_own()
        for copy in arriving:
            copy.wait_recv()
        arriving = send_rows(stage)
    if not (FRONT_FIRST and len(inner) > 1):
        send_own()
    bias_flow = send_bias(0)

    coming = []
    for number in range(len(parts)):
        order = parts[number][3]
        for kept in subsets(order)[1:]:
            coming.append((len(kept), masks.index(kept[-1]), number, kept))
    coming = [(number, kept) for _, _, number, kept in sorted(coming)]
    cuts = [0] + [len(coming) * cut // 21 for cut in FRONT_CUTS] + [len(coming)]

    def receive(wave):
        for number, kept in coming[cuts[wave] : cuts[wave + 1]]:
            receive_piece(number, kept)

    receive(0)
    for copy in arriving:
        copy.wait_recv()

    @pl.loop(0, members)
    def _(block):
        project(block)

    receive(1)
    lanes = lax.broadcasted_iota(jnp.int32, (rows, wide_span), 1)
    unit = low(jnp.where(lanes == extra, 1.0, 0.0))
    side_lanes = lax.broadcasted_iota(jnp.int32, (rows, 128), 1)
    base = copies.used
    copies.used += members
    lane_block = pl.ds(pl.multiple_of(member * wide_span, wide_span), wide_span)

    def att_copy(j, block):
        return copies.make(
            mixed.at[block], att.at[:, lane_block], {TENSOR: t_pos - member + block}, base + j
        )

    def attend(j):
        block = xor_member(j)
        at = pl.ds(pl.multiple_of(block * rows, rows), rows)
        query = q_ref[at, :]
        total_mix = jnp.zeros((rows, wide_span), F32)
        logs = jnp.zeros((rows, 128), F32)
        for head in range(heads):
            chosen = head_mask(lanes, head, offset)
            left = jnp.where(chosen, query, unit)
            scores = dot_nt(left, k_ref[...])
            peak = jnp.max(scores, axis=-1, keepdims=True)
            expo = jnp.exp(scores - peak)
            total = jnp.sum(expo, axis=-1, keepdims=True)
            out = dot_nn(low(expo), v_ref[...]) / total
            total_mix = jnp.where(chosen, out, total_mix)
            logs = jnp.where(side_lanes == head, peak + jnp.log(total), logs)
        mixed[block] = low(total_mix)
        l_ref[at, :] = logs

    half_turns = members // 2

    @pl.loop(0, half_turns)
    def _(turn):
        j = members - 1 - turn
        attend(j)
        att_copy(j, xor_member(j)).start()

    receive(2)

    @pl.loop(half_turns, members)
    def _(turn):
        j = members - 1 - turn
        attend(j)

        @pl.when(j > 0)
        def _():
            att_copy(j, xor_member(j)).start()

    own_att = pltpu.make_async_copy(mixed.at[member], att.at[:, lane_block], here.at[0])
    own_att.start()
    for stage in range(1, len(masks)):
        bias_flow.wait_recv()
        bias_flow = send_bias(stage)
    normed_copy = pltpu.make_async_copy(normed, normed_out, here.at[1])
    normed_copy.start()
    other_cots.wait_recv()
    cot_copy = pltpu.make_async_copy(cots, cot_out, here.at[2])
    cot_copy.start()
    own_att.wait()
    for j in range(1, members):
        att_copy(j, xor_member(j)).wait()
    att_copy_out = pltpu.make_async_copy(att, att_out, here.at[3])
    att_copy_out.start()
    receive(3)
    bias_flow.wait_recv()
    pieces = []
    core_bit = bit(d_pos, 1)
    for tile in tiles(len(masks)):
        row = biases[tile]
        half_lanes = row.shape[1] // 2
        pieces.append(jnp.where(core_bit == 0, row[:, :half_lanes], row[:, half_lanes:]))
    bias_out[...] = jnp.concatenate(pieces, axis=1).reshape(bias_out.shape)
    for copy in forwards:
        copy.wait_recv()
    up_copy = pltpu.make_async_copy(weights.at[0], up_out, here.at[5])
    up_copy.start()
    down_copy = pltpu.make_async_copy(weights.at[1], down_out, here.at[0])
    down_copy.start()
    for copy in (normed_copy, cot_copy, att_copy_out, up_copy, down_copy):
        copy.wait()
    copies.drain()


def front(
    heads, members, tensor_size, blocks, norm, w_q, w_k, w_v, bias, counts, cotangent, piece, up_bias
):
    rows, width = blocks.shape
    wide_span = -(-(heads * HEAD_DIM + 4) // 128) * 128
    total = members * rows
    inner, outer = len(bits_of(members)), len(bits_of(tensor_size))
    square = jax.ShapeDtypeStruct((total, wide_span), BF)
    normed = jax.ShapeDtypeStruct((2,) * inner + (rows, width), BF)
    att = jax.ShapeDtypeStruct((rows, members * wide_span), BF)
    cots = jax.ShapeDtypeStruct((2, rows, width), BF)
    weights = jax.ShapeDtypeStruct((2,) * outer + piece.shape[1:], BF)
    biases = jax.ShapeDtypeStruct((2,) * outer + up_bias.shape, F32)
    number = front_copies(tensor_size, members, width)
    vmem = pl.BlockSpec(memory_space=pltpu.VMEM)
    away = pl.BlockSpec(memory_space=pl.ANY)
    flat = jax.ShapeDtypeStruct((tensor_size * up_bias.shape[1] // 2,), F32)
    held = (normed, att, cots, weights, weights, flat)
    return pl.pallas_call(
        functools.partial(front_kernel, heads, members, tensor_size),
        out_shape=(square, square, square, jax.ShapeDtypeStruct((total, 128), F32)) + held,
        in_specs=[vmem] * 2 + [away] * 3 + [vmem] * 5,
        out_specs=(vmem,) * 4 + (away,) * 5 + (vmem,),
        scratch_shapes=[
            pltpu.VMEM(normed.shape, BF),
            pltpu.VMEM((members, rows, wide_span), BF),
            pltpu.VMEM(att.shape, BF),
            pltpu.VMEM(cots.shape, BF),
            pltpu.VMEM((2,) + weights.shape, BF),
            pltpu.VMEM(biases.shape, F32),
            pltpu.VMEM((3, width, wide_span), BF),
            pltpu.SemaphoreType.DMA((number,)),
            pltpu.SemaphoreType.DMA((number,)),
            pltpu.SemaphoreType.DMA((6,)),
        ],
        compiler_params=pltpu.CompilerParams(
            vmem_limit_bytes=48 << 20, collective_id=0, has_side_effects=True
        ),
        cost_estimate=pl.CostEstimate(
            flops=20_000_000_000, bytes_accessed=20_000_000, transcendentals=3_000_000
        ),
    )(blocks, norm, w_q, w_k, w_v, bias, counts, cotangent, piece, up_bias)


def back_shapes(members, rows, width, wide_span, span, tensor_size, dp_size, quarter):
    inner, outer = len(bits_of(members)), len(bits_of(tensor_size))
    third = width // PARTS
    half = width // 2
    split_bits = outer + 1
    four = span // 4
    sixteenth = members * span // 16
    shapes = {
        "grad_mixed": ((members, rows, wide_span), BF),
        "grads": ((3, members * rows, wide_span), BF),
        "heads_weight": ((3, width, wide_span), BF),
        "turned": ((wide_span, width), F32),
        "sum_k": ((members * rows, wide_span), F32),
        "sum_v": ((members * rows, wide_span), F32),
        "rows_part": ((2,) * inner + (rows, width), BF),
        "grad_rows": ((rows, width), F32),
        "whole": ((2, 2, 2, quarter, width), BF),
        "out_full": ((2, 2, 2, 2, sixteenth, width), BF),
        "square": ((3, 2, 2, four, width), BF),
        "square_one": ((3, 2, four, width), BF),
        "square_two": ((3, four, width), BF),
        "square_full": ((3,) + (2,) * inner + (2, 2, four, width), BF),
        "late": ((8, width), F32),
        "early_sum": ((16, width), F32),
        "out_part": ((2, 2, 2, 2, sixteenth, width), BF),
        "heads_sum": ((2, members, 1, wide_span), F32),
    }
    for part in range(PARTS):
        for stage in range(split_bits):
            left = (2,) * (split_bits - 1 - stage)
            shapes[f"hidden{part}_{stage}"] = ((2,) + left + (quarter, third), BF)
        for stage in range(len(bits_of(dp_size)) - 2):
            shapes[f"hidden{part}_more{stage}"] = ((2, quarter, third), BF)
    for part in range(2):
        for stage in range(inner):
            shapes[f"rows{part}_{stage}"] = ((2,) * (inner - 1 - stage) + (rows, half), BF)
    for stage in range(4):
        shapes[f"out{stage}"] = ((2,) * (3 - stage) + (sixteenth, width), BF)
    every = len(bits_of(tensor_size)) + len(bits_of(dp_size))
    for stage in range(every - 4):
        shapes[f"out_more{stage}"] = ((sixteenth, width), BF)
    for stage in range(every - 2 - inner):
        shapes[f"square_more{stage}"] = ((3, four, width), BF)
    for stage in range(every):
        shapes[f"early{stage}"] = ((16, width), F32)
        shapes[f"late{stage}"] = ((8, width), F32)
        shapes[f"heads{stage}"] = ((2, members, 1, wide_span), F32)
    return shapes


def tiles(count):
    if count == 0:
        return [()]
    return [(value,) + rest for value in range(2) for rest in tiles(count - 1)]


def back_kernel(
    heads,
    members,
    tensor_size,
    dp_size,
    names,
    number,
    q_ref,
    k_ref,
    v_ref,
    l_ref,
    datt_ref,
    normed_ref,
    wq_ref,
    wk_ref,
    wv_ref,
    down_ref,
    up_ref,
    att_ref,
    branch_ref,
    blocks_ref,
    norm_ref,
    middle_ref,
    hidden_bias_ref,
    early0_ref,
    early1_ref,
    early2_ref,
    early3_ref,
    early4_ref,
    early5_ref,
    blocks_out,
    query_out,
    key_out,
    value_out,
    out_out,
    down_out,
    up_out,
    early_out,
    late_out,
    heads_out,
    *scratch,
):
    held = dict(zip(names, scratch))
    early_refs = (early0_ref, early1_ref, early2_ref, early3_ref, early4_ref, early5_ref)
    send, recv, here = scratch[len(names):]
    copies = Copies(send, recv)
    t_pos = lax.axis_index(TENSOR)
    d_pos = lax.axis_index(DP)
    member = t_pos % members
    core, side = bit(d_pos, 1), bit(d_pos, 2)
    total_rows, wide_span = q_ref.shape
    rows, width = blocks_ref.shape
    masks, inner, dp_masks = bits_of(tensor_size), bits_of(members), bits_of(dp_size)
    outer_first, inner_first = masks[::-1], inner[::-1]
    scale = HEAD_DIM ** (-0.5)
    span = heads * HEAD_DIM
    start, offset, extra = window(member, span, wide_span)
    position = {TENSOR: t_pos, DP: d_pos}
    every = [(DP, mask) for mask in dp_masks] + [(TENSOR, mask) for mask in masks]
    rest_dp = [(DP, mask) for mask in dp_masks[2:]]
    rest_tensor = [(TENSOR, mask) for mask in masks[len(inner):]]

    named = {
        "x": (TENSOR, masks[0]),
        "z0": (TENSOR, masks[1]),
        "z1": (TENSOR, masks[2]),
        "y": (DP, 2),
    }

    def to(move):
        axis, mask = move
        return {axis: turned(position[axis], mask)}

    def mine(move):
        axis, mask = move
        return bit(position[axis], mask)

    def xor_member(j):
        return sum(mask * ((bit(member, mask) + bit(j, mask)) % 2) for mask in inner)

    def slot(index):
        return tuple(bit(index, mask) for mask in inner_first)

    peers = [to(move) for move in every]
    peers += [
        {TENSOR: t_pos - member + xor_member(j)} for j in range(1, members) if j not in inner
    ]
    barrier = greet(peers)
    grad_mixed, grads = held["grad_mixed"], held["grads"]
    sum_k, sum_v = held["sum_k"], held["sum_v"]
    own_lanes = pl.ds(pl.multiple_of(member * wide_span, wide_span), wide_span)
    own_copy = pltpu.make_async_copy(datt_ref.at[:, own_lanes], grad_mixed.at[member], here.at[0])
    own_copy.start()
    weight_ref = held["heads_weight"]
    weight_copies = []
    lane_window = pl.ds(pl.multiple_of(start, 128), wide_span)
    for which, source in enumerate((wq_ref, wk_ref, wv_ref)):
        weight_copies.append(
            pltpu.make_async_copy(
                source.at[:, lane_window], weight_ref.at[which], here.at[1 + which]
            )
        )
        weight_copies[-1].start()
    sum_k[...] = jnp.zeros_like(sum_k)
    sum_v[...] = jnp.zeros_like(sum_v)
    pl.semaphore_wait(barrier, len(peers))

    base = copies.used
    copies.used += members

    def datt_copy(j):
        block = xor_member(j)
        there = pl.ds(pl.multiple_of(block * wide_span, wide_span), wide_span)
        return copies.make(
            datt_ref.at[:, there],
            grad_mixed.at[member],
            {TENSOR: t_pos - member + block},
            base + j,
        )

    for j in range(1, members):
        datt_copy(j).start()

    def add(target, at, source, source_at):
        target[at] = low(wide(target[at]) + wide(source[source_at]))

    def hidden_chain(part):
        third = width // PARTS
        columns = pl.ds(part * third, third)
        dims = [(TENSOR, mask) for mask in outer_first] + [(DP, 2)]
        order = [named[name] for name in HIDDEN_ORDERS[part]]
        order += [(TENSOR, mask) for mask in masks[3:]]
        full = slice(None)
        current = None
        for stage, move in enumerate(order):
            landing = held[f"hidden{part}_{stage}"]
            where = dims.index(move)
            away = (full,) * where + (1 - mine(move),) + (full,) * (len(dims) - 1 - where)
            sent = []
            if current is None:
                for which, source in enumerate((down_ref, up_ref)):
                    sent.append(
                        copies.start(
                            source.at[away + (full, columns)], landing.at[which], to(move)
                        )
                    )
            else:
                sent.append(copies.start(current.at[(full,) + away], landing, to(move)))
            yield
            for copy in sent:
                copy.wait_recv()
            for tile in tiles(len(dims) - 1):
                kept = tile[:where] + (mine(move),) + tile[where:]
                for which in range(2):
                    if current is None:
                        source = (down_ref, up_ref)[which]
                        add(landing, (which,) + tile, source, kept + (full, columns))
                    else:
                        add(landing, (which,) + tile, current, (which,) + kept)
            current = landing
            dims = dims[:where] + dims[where + 1 :]
        for stage, move in enumerate(rest_dp):
            landing = held[f"hidden{part}_more{stage}"]
            copy = copies.start(current, landing, to(move))
            yield
            copy.wait_recv()
            for which in range(2):
                add(landing, which, current, which)
            current = landing
        whole = held["whole"]
        for which in range(2):
            whole[which, core, side, :, columns] = current[which]
        block = whole.at[:, core, side, :, columns]
        copy = copies.start(block, block, to((DP, 2)))
        yield
        copy.wait_recv()
        block = whole.at[:, core, :, :, columns]
        copy = copies.start(block, block, to((DP, 1)))
        yield
        copy.wait_recv()

    def out_chain():
        halvings = [(DP, 1)] + [named[name] for name in OUT_ORDER]
        current = held["out_part"]
        for stage, move in enumerate(halvings):
            landing = held[f"out{stage}"]
            copy = copies.start(current.at[1 - mine(move)], landing, to(move))
            yield
            copy.wait_recv()
            for tile in tiles(3 - stage):
                add(landing, tile + (slice(None),), current, (mine(move),) + tile)
            current = landing
        for stage, move in enumerate([move for move in every if move not in halvings]):
            landing = held[f"out_more{stage}"]
            copy = copies.start(current, landing, to(move))
            yield
            copy.wait_recv()
            add(landing, slice(None), current, slice(None))
            current = landing
        out_full = held["out_full"]
        own = tuple(mine(move) for move in halvings)
        out_full[own] = current[...]
        for stage in range(3, -1, -1):
            block = out_full.at[own[: stage + 1]]
            copy = copies.start(block, block, to(halvings[stage]))
            yield
            copy.wait_recv()

    def square_chain():
        square, one, two = held["square"], held["square_one"], held["square_two"]
        copy = copies.start(square.at[:, 1 - core], one, to((DP, 1)))
        yield
        copy.wait_recv()
        for which in range(3):
            for tile in tiles(1):
                add(one, (which,) + tile, square, (which, core) + tile)
        copy = copies.start(one.at[:, 1 - side], two, to((DP, 2)))
        yield
        copy.wait_recv()
        for which in range(3):
            add(two, which, one, (which, side))
        current = two
        for stage, move in enumerate(rest_tensor + rest_dp):
            landing = held[f"square_more{stage}"]
            copy = copies.start(current, landing, to(move))
            yield
            copy.wait_recv()
            for which in range(3):
                add(landing, which, current, which)
            current = landing
        full = held["square_full"]
        dims = [(TENSOR, mask) for mask in inner_first] + [(DP, 1), (DP, 2)]
        own = tuple(mine(move) for move in dims)
        for which in range(3):
            full[(which,) + own] = current[which]
        moves = [(TENSOR, mask) for mask in inner] + [(DP, 2)]
        for stage in range(len(moves) + 1):
            sent = []
            for which in range(3):
                turn = which % len(moves)
                order = moves[turn:] + moves[:turn] + [(DP, 1)]
                done = order[:stage]
                at = tuple(slice(None) if move in done else mine(move) for move in dims)
                block = full.at[(which,) + at]
                sent.append(copies.start(block, block, to(order[stage])))
            yield
            for copy in sent:
                copy.wait_recv()

    def rows_chain():
        half = width // 2
        part_ref = held["rows_part"]
        state = []
        for part in range(2):
            state.append([part_ref, list(inner_first), (pl.ds(part * half, half),)])
        orders = (inner, inner[::-1])
        for stage in range(len(inner)):
            sent = []
            for part in range(2):
                current, dims, columns = state[part]
                mask = orders[part][stage]
                where = dims.index(mask)
                away = (slice(None),) * where + (1 - bit(member, mask),)
                away += (slice(None),) * (len(dims) - 1 - where)
                sent.append(
                    copies.start(
                        current.at[away + (slice(None),) + columns],
                        held[f"rows{part}_{stage}"],
                        to((TENSOR, mask)),
                    )
                )
            yield
            for part in range(2):
                sent[part].wait_recv()
                current, dims, columns = state[part]
                mask = orders[part][stage]
                where = dims.index(mask)
                landing = held[f"rows{part}_{stage}"]
                for tile in tiles(len(dims) - 1):
                    kept = tile[:where] + (bit(member, mask),) + tile[where:]
                    kept += (slice(None),) + columns
                    if stage < len(inner) - 1:
                        add(landing, tile + (slice(None),), current, kept)
                    else:
                        held["grad_rows"][:, part * half : (part + 1) * half] = wide(
                            landing[...]
                        ) + wide(current[kept])
                state[part] = [landing, dims[:where] + dims[where + 1 :], ()]

    def small_chain(pairs):
        for stage, move in enumerate(every):
            sent = []
            for first, name, _ in pairs:
                source = first if stage == 0 else held[f"{name}{stage - 1}"]
                sent.append(copies.start(source, held[f"{name}{stage}"], to(move)))
            yield
            for copy, (first, name, result) in zip(sent, pairs):
                copy.wait_recv()
                source = first if stage == 0 else held[f"{name}{stage - 1}"]
                value = held[f"{name}{stage}"][...] + source[...]
                if stage == len(every) - 1:
                    result[...] = value
                else:
                    held[f"{name}{stage}"][...] = value

    chains = {
        "out": out_chain(),
        "early": small_chain([(held["early_sum"], "early", early_out)]),
        "rows": rows_chain(),
        "square": square_chain(),
        "late": small_chain(
            [(held["late"], "late", late_out), (held["heads_sum"], "heads", heads_out)]
        ),
    }
    for part in range(PARTS):
        chains[f"h{part}"] = hidden_chain(part)
    live = list(chains)

    def go(*wanted):
        for name in wanted:
            if name in live:
                if next(chains[name], True):
                    live.remove(name)

    own_copy.wait()
    for copy in weight_copies:
        copy.wait()
    lanes = lax.broadcasted_iota(jnp.int32, (rows, wide_span), 1)

    def attend(block):
        at = pl.ds(pl.multiple_of(block * rows, rows), rows)
        query = q_ref[at, :]
        grad = grad_mixed[block]
        grad_q = jnp.zeros((rows, wide_span), F32)
        for head in range(heads):
            chosen = head_mask(lanes, head, offset)
            log_total = l_ref[at, head : head + 1]
            high = low(log_total)
            rest = log_total - wide(high)
            middle = low(rest)
            last = low(rest - wide(middle))
            fill = jnp.where(lanes == extra, 1.0, 0.0)
            fill = jnp.where(lanes == extra + 1, -wide(high), fill)
            fill = jnp.where(lanes == extra + 2, -wide(middle), fill)
            fill = jnp.where(lanes == extra + 3, -wide(last), fill)
            left = jnp.where(chosen, query, low(fill))
            upstream = jnp.where(chosen, grad, jnp.zeros_like(grad))
            probs = jnp.exp(dot_nt(k_ref[...], left))
            grad_probs = dot_nt(v_ref[...], upstream)
            centred = jnp.sum(probs * grad_probs, axis=0, keepdims=True)
            grad_scores = low(probs * (grad_probs - centred))
            sum_k[...] += dot_nn(grad_scores, left)
            sum_v[...] += dot_nn(low(probs), upstream)
            out = dot_tn(grad_scores, k_ref[...]) * scale
            grad_q = jnp.where(chosen, out, grad_q)
        grads[0, at, :] = low(grad_q)

    def block(index):
        count = members // 2

        @pl.loop(index * count, (index + 1) * count)
        def _(j):
            @pl.when(j > 0)
            def _():
                datt_copy(j).wait_recv()

            attend(xor_member(j))

    def compute_outs():
        unit_rows = span // 4
        out_part = held["out_part"]
        for index in range(members):
            full = dot_tn(att_ref[:, index * wide_span : (index + 1) * wide_span], branch_ref[...])
            inset = window(index, span, wide_span)[1]
            for quarter_index in range(4):
                at = index * 4 + quarter_index
                where = tuple((at * 16 // (members * 4)) // step % 2 for step in (8, 4, 2, 1))
                inner_row = (at * unit_rows) % out_part.shape[4]
                out_part[where + (slice(inner_row, inner_row + unit_rows), slice(None))] = low(
                    full[inset + quarter_index * unit_rows : inset + (quarter_index + 1) * unit_rows]
                )
        early = held["early_sum"]
        early[...] = jnp.zeros_like(early)
        for index, row in enumerate(early_refs):
            early[index : index + 1, :] = row[...].reshape(1, width)
        early[6 : 6 + hidden_bias_ref.shape[0], :] = hidden_bias_ref[...]

    def finish_attention():
        keep = (lanes >= offset) & (lanes < offset + span)

        @pl.loop(0, members)
        def _(block):
            at = pl.ds(pl.multiple_of(block * rows, rows), rows)
            grads[1, at, :] = low(jnp.where(keep, sum_k[at, :], 0.0))
            grads[2, at, :] = low(sum_v[at, :])

    def compute_rows():
        @pl.loop(0, members)
        def _(block):
            at = pl.ds(pl.multiple_of(block * rows, rows), rows)
            part = dot_nt(grads[0, at, :], weight_ref[0])
            part += dot_nt(grads[1, at, :], weight_ref[1])
            part += dot_nt(grads[2, at, :], weight_ref[2])
            held["rows_part"][slot(block) + (slice(None), slice(None))] = low(part)

    def compute_square():
        four = held["square"].shape[3]

        @pl.loop(0, 3)
        def _(which):
            turned_rows = held["turned"]
            turned_rows[...] = dot_tn(grads[which], normed_ref[...])
            for tile in tiles(2):
                at = pl.multiple_of(offset + (tile[0] * 2 + tile[1]) * four, 16)
                held["square"][(which,) + tile] = low(turned_rows[pl.ds(at, four), :])

        heads_sum = held["heads_sum"]
        heads_sum[...] = jnp.zeros_like(heads_sum)
        heads_sum[0, member] = jnp.sum(wide(grads[0]), axis=0, keepdims=True)
        heads_sum[1, member] = jnp.sum(wide(grads[2]), axis=0, keepdims=True)

    def compute_norm():
        while "rows" in live:
            go("rows")
        gain = norm_ref[0:1, :]
        gain_sum = jnp.zeros((1, width), F32)
        shift_sum = jnp.zeros((1, width), F32)
        step = rows // 2
        for start in range(0, rows, step):
            at = pl.ds(start, step)
            grad = held["grad_rows"][at, :]
            values = wide(blocks_ref[at, :])
            centre = values - jnp.mean(values, axis=-1, keepdims=True)
            spread = jnp.mean(centre * centre, axis=-1, keepdims=True)
            factor = lax.rsqrt(spread + EPSILON)
            unit = centre * factor
            scaled = grad * gain
            pulled = scaled - jnp.mean(scaled, axis=-1, keepdims=True)
            pulled = pulled - unit * jnp.mean(scaled * unit, axis=-1, keepdims=True)
            blocks_out[at, :] = middle_ref[at, :] + factor * pulled
            gain_sum += jnp.sum(grad * unit, axis=0, keepdims=True)
            shift_sum += jnp.sum(grad, axis=0, keepdims=True)
        late = held["late"]
        late[...] = jnp.zeros_like(late)
        late[0:1, :] = gain_sum
        late[1:2, :] = shift_sum

    for token in sum(BACK_PROGRAM, ()):
        if token.startswith("*block"):
            block(int(token[6:]))
            if token == "*block1":
                finish_attention()
        elif token == "*outs":
            compute_outs()
        elif token == "*rows":
            compute_rows()
        elif token == "*square":
            compute_square()
        elif token == "*norm":
            compute_norm()
        else:
            go(token)
    while live:
        go(*list(live))
    finals = []
    sources = [held["square_full"].at[which] for which in range(3)] + [held["out_full"]]
    sources += [held["whole"].at[which] for which in range(2)]
    targets = (query_out, key_out, value_out, out_out, down_out, up_out)
    for index, (source, target) in enumerate(zip(sources, targets)):
        copy = pltpu.make_async_copy(source, target, here.at[index])
        copy.start()
        finals.append(copy)
    for copy in finals:
        copy.wait()
    for j in range(1, members):
        datt_copy(j).wait_send()
    copies.drain()


def back(
    heads,
    members,
    tensor_size,
    dp_size,
    span,
    quarter,
    queries,
    keys,
    values,
    logs,
    datt,
    normed,
    w_q,
    w_k,
    w_v,
    grad_down,
    grad_up,
    attended,
    grad_branch,
    blocks,
    norm,
    middle,
    hidden_bias,
    early,
):
    rows, width = blocks.shape
    wide_span = queries.shape[1]
    shapes = back_shapes(members, rows, width, wide_span, span, tensor_size, dp_size, quarter)
    names = list(shapes)
    outer, inner = len(bits_of(tensor_size)), len(bits_of(members))
    every = outer + len(bits_of(dp_size))
    number = members + PARTS * (outer + 1 + 1 + 2 + len(bits_of(dp_size))) + every + 8
    number += 2 + every + 3 * (inner + 2) + 2 * inner + 3 * every
    vmem = pl.BlockSpec(memory_space=pltpu.VMEM)
    away = pl.BlockSpec(memory_space=pl.ANY)

    def shape_of(name):
        return jax.ShapeDtypeStruct(*shapes[name])

    def part_of(name):
        shape, kind = shapes[name]
        return jax.ShapeDtypeStruct(shape[1:], kind)

    return pl.pallas_call(
        functools.partial(back_kernel, heads, members, tensor_size, dp_size, names, number),
        out_shape=(
            jax.ShapeDtypeStruct((rows, width), F32),
            part_of("square_full"),
            part_of("square_full"),
            part_of("square_full"),
            shape_of("out_full"),
            part_of("whole"),
            part_of("whole"),
            jax.ShapeDtypeStruct((16, width), F32),
            shape_of("late"),
            shape_of("heads_sum"),
        ),
        in_specs=[vmem] * 6 + [away] * 3 + [vmem] * 14,
        out_specs=(vmem,) + (away,) * 6 + (vmem,) * 3,
        scratch_shapes=[pltpu.VMEM(*shapes[name]) for name in names]
        + [
            pltpu.SemaphoreType.DMA((number,)),
            pltpu.SemaphoreType.DMA((number,)),
            pltpu.SemaphoreType.DMA((6,)),
        ],
        compiler_params=pltpu.CompilerParams(
            vmem_limit_bytes=60 << 20, collective_id=1, has_side_effects=True
        ),
        cost_estimate=pl.CostEstimate(
            flops=40_000_000_000, bytes_accessed=40_000_000, transcendentals=3_000_000
        ),
    )(
        queries,
        keys,
        values,
        logs,
        datt,
        normed,
        w_q,
        w_k,
        w_v,
        grad_down,
        grad_up,
        attended,
        grad_branch,
        blocks,
        norm,
        middle,
        hidden_bias,
        *early,
    )


def vectors_kernel(
    span,
    early_ref,
    late_ref,
    heads_ref,
    query_ref,
    value_ref,
    out_ref,
    gain1_ref,
    shift1_ref,
    gain2_ref,
    shift2_ref,
    down_ref,
    gates_ref,
):
    width = out_ref.shape[0]
    members, wide_span = heads_ref.shape[1], heads_ref.shape[3]
    for which, target in ((0, query_ref), (1, value_ref)):
        pieces = []
        for index in range(members):
            inset = window(index, span, wide_span)[1]
            if index * span < width:
                pieces.append(heads_ref[which, index, :, inset : inset + span])
        target[...] = jnp.concatenate(pieces, axis=1).reshape(width)
    rows = ((early_ref, 0, out_ref), (late_ref, 0, gain1_ref), (late_ref, 1, shift1_ref))
    rows += ((early_ref, 1, gain2_ref), (early_ref, 2, shift2_ref), (early_ref, 3, down_ref))
    for source, row, target in rows:
        target[...] = source[row : row + 1, :].reshape(width)
    gates_ref[...] = early_ref[4:6, :]


def vectors(span, width, early, late, head_sums):
    line = jax.ShapeDtypeStruct((width,), F32)
    return pl.pallas_call(
        functools.partial(vectors_kernel, span),
        out_shape=(line,) * 8 + (jax.ShapeDtypeStruct((2, width), F32),),
        compiler_params=pltpu.CompilerParams(vmem_limit_bytes=4 << 20),
    )(early, late, head_sums)


def local(
    blocks,
    counts,
    cotangent,
    w_query,
    w_key,
    w_value,
    w_out,
    b_query,
    b_value,
    b_out,
    norm1_gain,
    norm1_bias,
    norm2_gain,
    norm2_bias,
    gate_logits,
    w_up,
    b_up,
    w_down,
    b_down,
):
    rows, width = blocks.shape
    tensor_size = lax.axis_size(TENSOR)
    dp_size = lax.axis_size(DP)
    t_pos = lax.axis_index(TENSOR)
    d_pos = lax.axis_index(DP)
    members = SEQ // rows
    member = t_pos % members
    per_head = -(-HEADS // members)
    span = per_head * HEAD_DIM
    ring = 4
    line = tensor_size // ring
    z_pos = t_pos // line
    x_pos = t_pos % line
    core = d_pos % 2
    side = (d_pos // 2) % 2
    shard = w_up.shape[1]
    quarter = shard // 4
    hidden_total = shard * tensor_size
    dp_rest = [(DP, mask) for mask in bits_of(dp_size)[2:]]
    member_masks = bits_of(members)
    tensor_rest = [(TENSOR, mask) for mask in bits_of(tensor_size)[len(member_masks):]]

    def z_shift(value, step):
        pairs = [
            (i, ((i // line + step) % ring) * line + i % line) for i in range(tensor_size)
        ]
        return lax.ppermute(value, TENSOR, pairs)

    def x_shift(value, step):
        pairs = [
            (i, (i // line) * line + (i % line + step) % line) for i in range(tensor_size)
        ]
        return lax.ppermute(value, TENSOR, pairs)

    gain_one = wide(norm1_gain)
    shift_one = wide(norm1_bias)
    gain_two = wide(norm2_gain)
    shift_two = wide(norm2_bias)
    logits_gate = wide(gate_logits)
    inputs = wide(blocks)

    doc_counts = pick(counts, t_pos // members)
    slot_ids = member ^ jnp.arange(members, dtype=jnp.int32)
    own_pos = member * rows + jnp.arange(rows, dtype=jnp.int32)
    visual = own_pos >= TEXT_SLOTS

    wide_span = -(-(span + 4) // 128) * 128
    reach = window(members - 1, span, wide_span)[0] + wide_span

    def reached(array, axis=-1):
        if reach == width:
            return array
        pads = [(0, 0)] * array.ndim
        pads[axis] = (0, reach - width)
        return jnp.pad(array, pads)

    w_q, w_k, w_v = reached(w_query), reached(w_key), reached(w_value)
    bias = reached(wide(jnp.stack([b_query, b_value], 0)))
    halves = (2, 2, quarter, width)
    piece = jnp.stack(
        [pick(w_up.T.reshape(halves), core), pick(w_down.reshape(halves), core)], 0
    )
    queries, keys, values, logs, normed_all, attended, cot_all, up_t, down, biases = front(
        per_head,
        members,
        tensor_size,
        blocks,
        jnp.stack([gain_one, shift_one], 0),
        w_q,
        w_k,
        w_v,
        bias,
        jnp.broadcast_to(doc_counts[:, None], (2, 128)),
        cotangent,
        piece,
        wide(b_up)[None, :],
    )
    normed_all = normed_all.reshape(SEQ, width)
    cot_all = cot_all.reshape(2 * rows, width)
    up_t = up_t.reshape(-1, width)
    down = down.reshape(-1, width)
    reached_out = reached(w_out, 0)
    starts = [window(index, span, wide_span)[0] for index in range(members)]
    out_rows = jnp.concatenate([reached_out[at : at + wide_span] for at in starts], 0)

    branch = dot_nn(attended, out_rows) + wide(b_out)
    gate = jax.nn.sigmoid(
        jnp.where(visual[:, None], logits_gate[1][None, :], logits_gate[0][None, :])
    )
    middle = inputs + gate * branch
    second = low(normalize(middle, gain_two, shift_two))
    second_all = jnp.concatenate([second, flip(second, DP, 1)], 0)

    pre = dot_nt(second_all, up_t) + biases
    hidden = low(gelu_exact(pre))
    grad_down = low(dot_tn(hidden, cot_all))
    spread = dot_nt(cot_all, down)
    dpre = low(gelu_grad(pre, spread))
    grad_second = dot_nn(dpre[:rows], up_t) + flip(dot_nn(dpre[rows:], up_t), DP, 1)
    lowered = dot_nn(hidden[:rows], down) + flip(dot_nn(hidden[rows:], down), DP, 1)
    grad_up = low(dot_tn(dpre, second_all))
    grad_up_bias = jnp.sum(wide(dpre), axis=0)
    joined = low(middle + lowered + wide(b_down))

    upstream = wide(cotangent)
    pull_two = jax.vjp(normalize, middle, gain_two, shift_two)[1]
    grad_middle_norm, grad_gain_two, grad_shift_two = pull_two(grad_second)
    grad_middle = upstream + grad_middle_norm
    grad_branch = low(gate * grad_middle)
    gate_term = grad_middle * branch * gate * (1.0 - gate)
    grad_gate = [
        jnp.sum(jnp.where(visual[:, None], 0.0, gate_term), axis=0),
        jnp.sum(jnp.where(visual[:, None], gate_term, 0.0), axis=0),
    ]
    grad_out_bias = jnp.sum(wide(grad_branch), axis=0)
    grad_attended = low(dot_nt(grad_branch, out_rows))
    bias_sum = grad_up_bias.reshape(tensor_size, 1, 2 * quarter)
    both = jnp.arange(2, dtype=jnp.int32)[None, :, None]
    bias_sum = jnp.where(both == core, bias_sum, 0.0).reshape(hidden_total // width, width)
    early = [grad_out_bias, grad_gain_two, grad_shift_two, jnp.sum(upstream, axis=0)] + grad_gate
    hidden_shape = (2,) * len(bits_of(tensor_size)) + (2, quarter, width)
    grad_blocks, *squares, outs, down_sum, up_sum, early, late, head_sums = back(
        per_head,
        members,
        tensor_size,
        dp_size,
        span,
        quarter,
        queries,
        keys,
        values,
        logs,
        grad_attended,
        normed_all,
        w_q,
        w_k,
        w_v,
        grad_down.reshape(hidden_shape),
        grad_up.reshape(hidden_shape),
        attended,
        grad_branch,
        blocks,
        jnp.stack([gain_one, shift_one], 0),
        grad_middle,
        bias_sum,
        early,
    )
    outs = outs.reshape(members * span, width)[:width]
    query_bias, value_bias, out_bias, gain1, shift1, gain2, shift2, down_bias, gates = vectors(
        span, width, early, late, head_sums
    )
    bias_out = lax.dynamic_slice_in_dim(
        early[6 : 6 + hidden_total // width].reshape(hidden_total), t_pos * shard, shard, 0
    )

    def turned_over(value, size):
        identity = low(jnp.eye(size, dtype=F32))
        return dot_tn(value, identity)

    flipped = [
        turned_over(square.reshape(members * span, width)[:width], width) for square in squares
    ]
    return (
        joined,
        grad_blocks,
        flipped[0],
        flipped[1],
        flipped[2],
        wide(outs),
        query_bias,
        value_bias,
        out_bias,
        gain1,
        shift1,
        gain2,
        shift2,
        gates,
        turned_over(up_sum.reshape(shard, width), shard),
        bias_out,
        wide(down_sum.reshape(shard, width)),
        down_bias,
    )


def solution(mesh):
    rows = P((DP, TENSOR), None)
    in_specs = (rows, P(DP, None), rows) + (P(),) * 12 + (
        P(None, TENSOR),
        P(TENSOR),
        P(TENSOR, None),
        P(),
    )
    out_specs = (rows, rows) + (P(),) * 12 + (
        P(None, TENSOR),
        P(TENSOR),
        P(TENSOR, None),
        P(),
    )
    return jax.shard_map(local, mesh=mesh, in_specs=in_specs, out_specs=out_specs, check_vma=False)
```
